16 devices in a mesh: outer: 4 (over z, y), inner: 4 (over x, core).
Axes of the slice: x: 2, y: 2, z: 2, core: 2. Of those that a mesh axis runs over, the one named last changes fastest.
Arguments:
- g_emb: float32 [16, 4096, 768], P(('outer', 'inner'))
- g_qkv: float32 [16, 2, 768, 2304], P(('outer', 'inner'))
- g_o: float32 [16, 2, 768, 768], P(('outer', 'inner'))
- g_w1: float32 [16, 2, 768, 3072], P(('outer', 'inner'))
- g_w2: float32 [16, 2, 3072, 768], P(('outer', 'inner'))
- g_bqkv: float32 [16, 2, 2304], P(('outer', 'inner'))
- g_b1: float32 [16, 2, 3072], P(('outer', 'inner'))
- g_dvec: float32 [16, 2, 6, 768], P(('outer', 'inner'))
- m: float32 [17321472], P(('outer', 'inner'))
- v: float32 [17321472], P(('outer', 'inner'))
- w: float32 [17321472], P(('outer', 'inner'))
- lr: float32 [], replicated
- beta1: float32 [], replicated
- beta2: float32 [], replicated
- eps: float32 [], replicated
- step: int32 [], replicated
Outputs:
- output 1: float32 [17321472], P(('outer', 'inner'))
- output 2: float32 [17321472], P(('outer', 'inner'))
- output 3: float32 [17321472], P(('outer', 'inner'))
- output 4: bfloat16 [4096, 768], replicated
- output 5: bfloat16 [2, 768, 2304], replicated
- output 6: bfloat16 [2, 768, 768], replicated
- output 7: bfloat16 [2, 768, 3072], replicated
- output 8: bfloat16 [2, 3072, 768], replicated
- output 9: bfloat16 [2, 2304], replicated
- output 10: bfloat16 [2, 3072], replicated
- output 11: bfloat16 [2, 6, 768], replicated
All inputs are finite; a program needn't handle non-finite values.
Results may differ from the reference program's by a relative error of at most 0.001.
Values are sent between devices in bfloat16 or wider.
A program may use at most 1 GiB of HBM per device.

```python
import math
import jax
import jax.numpy as jnp

DEVICES = 16
D = 768
FF = 3072
LAYERS = 2
EMB_ROWS = 4096

SHAPES = (
    (EMB_ROWS, D),
    (LAYERS, D, 3 * D),
    (LAYERS, D, D),
    (LAYERS, D, FF),
    (LAYERS, FF, D),
    (LAYERS, 3 * D),
    (LAYERS, FF),
    (LAYERS, 6, D),
)
SIZES = tuple(math.prod(s) for s in SHAPES)
PSI = sum(SIZES)
NAMES = ("g_emb", "g_qkv", "g_o", "g_w1", "g_w2", "g_bqkv", "g_b1", "g_dvec")


def draw_grad(key, shape):
    k1, k2 = jax.random.split(key)
    common = jax.random.normal(k1, shape, jnp.float32)
    own = jax.random.normal(k2, (DEVICES,) + shape, jnp.float32)
    return common[None] + 4.0 * own


def setup_inputs(seed: int = 0) -> dict:
    ks = jax.random.split(jax.random.key(seed), 16)
    out = {}
    for i in range(8):
        out[NAMES[i]] = draw_grad(ks[i], SHAPES[i])
    out["m"] = jax.random.normal(ks[8], (PSI,), jnp.float32)
    out["v"] = jax.random.uniform(ks[9], (PSI,), jnp.float32, 1.0, 4.0)
    out["w"] = jax.random.normal(ks[10], (PSI,), jnp.float32)
    out["lr"] = jax.random.uniform(ks[11], (), jnp.float32, 0.12, 0.2)
    out["beta1"] = jax.random.uniform(ks[12], (), jnp.float32, 0.5, 0.7)
    out["beta2"] = jax.random.uniform(ks[13], (), jnp.float32, 0.7, 0.9)
    out["eps"] = jax.random.uniform(ks[14], (), jnp.float32, 0.1, 1.5)
    out["step"] = jax.random.randint(ks[15], (), 1, 6, jnp.int32)
    return out


def reference(g_emb, g_qkv, g_o, g_w1, g_w2, g_bqkv, g_b1, g_dvec, m, v, w, lr, beta1, beta2, eps, step):
    grads = (g_emb, g_qkv, g_o, g_w1, g_w2, g_bqkv, g_b1, g_dvec)
    g = jnp.concatenate([jnp.sum(x, axis=0).reshape(-1) for x in grads]) / DEVICES
    t = step.astype(jnp.float32)
    m_new = beta1 * m + (1.0 - beta1) * g
    v_new = beta2 * v + (1.0 - beta2) * (g * g)
    m_hat = m_new / (1.0 - beta1 ** t)
    v_hat = v_new / (1.0 - beta2 ** t)
    w_new = w - lr * m_hat / (jnp.sqrt(v_hat) + eps)
    flat = w_new.astype(jnp.bfloat16)
    wb = []
    start = 0
    for i in range(8):
        wb.append(flat[start:start + SIZES[i]].reshape(SHAPES[i]))
        start = start + SIZES[i]
    return (m_new, v_new, w_new, wb[0], wb[1], wb[2], wb[3], wb[4], wb[5], wb[6], wb[7])
```

```python
import functools
import math

import jax
import jax.numpy as jnp
from jax import lax
from jax.experimental import pallas as pl
from jax.experimental.pallas import tpu as pltpu
from jax.sharding import PartitionSpec as P

AXES = ("outer", "inner")
MESH = pl.DeviceIdType.MESH
ANY = pl.BlockSpec(memory_space=pl.ANY)
LANES = 128
TILE = 16
VMEM_LIMIT = 63 * 1024 * 1024
BF = jnp.bfloat16
F32 = jnp.float32

ORDER = ((1, 1), (1, 0), (0, 1), (0, 0))


class Plan:
    def __init__(self, shapes, p):
        self.p = p
        self.sizes = [math.prod(s) for s in shapes]
        self.total = sum(self.sizes)
        self.shard = self.total // p
        tile = TILE * LANES
        g = math.gcd(self.shard, tile)
        self.num, self.den = self.shard // g, tile // g
        tiles = -(-(self.shard + tile - g) // tile)
        self.unit = -(-tiles // 3) * TILE
        self.window = 3 * self.unit
        self.rows = self.first(p - 1) * TILE + self.window
        self.big = []
        start = 0
        for s, n in zip(shapes, self.sizes):
            if s[-2] % TILE == 0:
                self.big.append((n // s[-1], s[-1] // LANES, start // LANES))
                start += n
        self.small_row = start // LANES
        self.small_size = self.total - start

    def first(self, r):
        if isinstance(r, int):
            return r * self.num // self.den
        return lax.div(r * self.num, self.den)

    def chunks(self, target):
        out = []
        for k, (rows, nj, flat) in enumerate(self.big):
            step = max(c for c in range(TILE, rows + 1, TILE) if rows % c == 0 and c * nj <= target)
            for r in range(0, rows, step):
                out.append((k, r, step, nj, flat + r * nj))
        return out


def group_rows(rows, nj):
    best = TILE
    for c in (16, 32, 64):
        if rows % c == 0 and c * nj <= 384:
            best = c
    return best


def flatten_kernel(plan, work, depth, *refs):
    n = len(plan.big)
    xs, small, f_ref, outs, ins = refs[:n], refs[n], refs[n + 1], refs[n + 2], refs[n + 3:2 * n + 3]
    in_sem, out_sem, small_sem = refs[2 * n + 3:]

    tail = pltpu.make_async_copy(small, f_ref.at[pl.ds(plan.small_row, small.shape[0])], small_sem)
    tail.start()

    def load(i):
        k, r, rows, nj, _ = work[i]
        return pltpu.make_async_copy(xs[k].at[pl.ds(r, rows)], ins[k].at[i % depth], in_sem.at[i % depth])

    def store(i):
        k, r, rows, nj, flat = work[i]
        return pltpu.make_async_copy(
            outs.at[i % depth, pl.ds(0, rows * nj)], f_ref.at[pl.ds(flat, rows * nj)], out_sem.at[i % depth]
        )

    for i in range(min(depth, len(work))):
        load(i).start()
    for i, (k, r, rows, nj, flat) in enumerate(work):
        slot = i % depth
        load(i).wait()
        if i >= depth:
            store(i - depth).wait()
        step = group_rows(rows, nj)

        def body(g, _, k=k, slot=slot, nj=nj, step=step):
            for h in range(0, step, 8):
                src = pl.multiple_of(g * step + h, 8)
                dst = pl.multiple_of(src * nj, 8)
                for j in range(nj):
                    outs[slot, pl.ds(dst + j, 8, stride=nj), :] = ins[k][slot, pl.ds(src, 8), j * LANES:(j + 1) * LANES]
            return 0

        lax.fori_loop(0, rows // step, body, 0)
        store(i).start()
        if i + depth < len(work):
            load(i + depth).start()
    for i in range(max(0, len(work) - depth), len(work)):
        store(i).wait()
    tail.wait()


def flatten(plan, grads):
    n = len(plan.big)
    depth = 4
    work = plan.chunks(3456)
    xs = [x.reshape(rows, nj * LANES) for x, (rows, nj, _) in zip(grads, plan.big)]
    small = jnp.concatenate([x.reshape(-1) for x in grads[n:]])
    pad = (plan.rows - plan.small_row) * LANES - plan.small_size
    small = jnp.pad(small, (0, pad)).reshape(-1, LANES)
    step = {w[0]: w[2] for w in work}
    size = max(w[2] * w[3] for w in work)
    return pl.pallas_call(
        functools.partial(flatten_kernel, plan, work, depth),
        out_shape=jax.ShapeDtypeStruct((plan.rows, LANES), F32),
        in_specs=[ANY] * (n + 1),
        out_specs=ANY,
        scratch_shapes=[pltpu.VMEM((depth, size, LANES), F32)]
        + [pltpu.VMEM((depth, step[k], plan.big[k][1] * LANES), F32) for k in range(n)]
        + [pltpu.SemaphoreType.DMA((depth,)), pltpu.SemaphoreType.DMA((depth,)), pltpu.SemaphoreType.DMA],
        compiler_params=pltpu.CompilerParams(vmem_limit_bytes=VMEM_LIMIT),
        name="flatten",
    )(*xs, small)


class Place:
    def __init__(self):
        o, i = lax.axis_index("outer"), lax.axis_index("inner")
        self.bits = [lax.div(o, 2), lax.rem(o, 2), lax.div(i, 2)]
        self.core = lax.rem(i, 2)

    def flipped(self, d):
        b = list(self.bits)
        b[d] = 1 - b[d]
        return (b[0] * 2 + b[1], b[2] * 2 + self.core)

    def partner(self):
        return (self.bits[0] * 2 + self.bits[1], self.bits[2] * 2 + 1 - self.core)

    def owner(self, dims, e, core):
        b = list(self.bits)
        for d, flip in zip(dims, e):
            if flip:
                b[d] = 1 - b[d]
        return b[0] * 8 + b[1] * 4 + b[2] * 2 + core


def dims_of(k):
    return (k, (k + 1) % 3, (k + 2) % 3)


def meet(place):
    barrier = pltpu.get_barrier_semaphore()
    peers = [place.partner()] + [place.flipped(d) for d in range(3)]
    for peer in peers:
        pl.semaphore_signal(barrier, inc=1, device_id=peer, device_id_type=MESH)
    pl.semaphore_wait(barrier, len(peers))


def remote(src, dst, send, recv, dev):
    return pltpu.make_async_remote_copy(
        src_ref=src, dst_ref=dst, send_sem=send, recv_sem=recv, device_id=dev, device_id_type=MESH
    )


def rs_kernel(plan, f_ref, g_ref, late_ref, early, r1, r2, r3, own, oth, *sems):
    (own_sem, oth_sem, out_sem, d_send, d_recv, s1_send, s1_recv, s2_send, s2_recv, s3_send, s3_recv) = sems
    u = plan.unit
    place = Place()
    partner = place.partner()
    units = [(k, (1,) + e) for e in ORDER for k in range(3)]
    units += [(k, (0,) + e) for e in ORDER for k in range(3)]

    def source(n, core):
        k, e = units[n]
        row = plan.first(place.owner(dims_of(k), e, core)) * TILE + k * u
        return f_ref.at[pl.ds(pl.multiple_of(row, TILE), u)]

    def exchange(n):
        dst = early.at[n] if n < 12 else late_ref.at[n - 12]
        return remote(source(n, 1 - place.core), dst, d_send.at[n], d_recv.at[n], partner)

    def load(n):
        return pltpu.make_async_copy(source(n, place.core), own.at[n % 2], own_sem.at[n % 2])

    def fetch(n):
        return pltpu.make_async_copy(late_ref.at[n], oth.at[n % 2], oth_sem.at[n % 2])

    def add(dst, *srcs):
        step = 48

        def body(i, _):
            rows = pl.ds(pl.multiple_of(i * step, 16), step)
            total = dst[rows, :]
            for s in srcs:
                total = total + s[rows, :]
            dst[rows, :] = total
            return 0

        lax.fori_loop(0, u // step, body, 0)

    load(0).start()
    load(1).start()
    meet(place)
    for n in range(24):
        exchange(n).start()

    first, second, third = [], [], []
    for n in range(12):
        k = units[n][0]
        load(n).wait()
        exchange(n).wait_recv()
        add(early.at[n], own.at[n % 2])
        load(n + 2).start()
        copy = remote(early.at[n], r1.at[n], s1_send.at[n], s1_recv.at[n], place.flipped(dims_of(k)[0]))
        copy.start()
        first.append(copy)

    for n in range(2):
        exchange(12 + n).wait_recv()
        fetch(n).start()
    for n in range(12):
        k = units[n][0]
        load(12 + n).wait()
        fetch(n).wait()
        first[n].wait_recv()
        add(r1.at[n], own.at[n % 2], oth.at[n % 2])
        if n + 2 < 12:
            load(14 + n).start()
            exchange(14 + n).wait_recv()
            fetch(n + 2).start()
        if n < 6:
            copy = remote(r1.at[n], r2.at[n], s2_send.at[n], s2_recv.at[n], place.flipped(dims_of(k)[1]))
            copy.start()
            second.append(copy)

    for n in range(6):
        second[n].wait_recv()
        add(r1.at[6 + n], r2.at[n])
        if n < 3:
            copy = remote(r1.at[6 + n], r3.at[n], s3_send.at[n], s3_recv.at[n], place.flipped(dims_of(n)[2]))
            copy.start()
            third.append(copy)
    outs = []
    for k in range(3):
        third[k].wait_recv()
        add(r1.at[9 + k], r3.at[k])
        out = pltpu.make_async_copy(r1.at[9 + k], g_ref.at[pl.ds(k * u, u)], out_sem.at[k])
        out.start()
        outs.append(out)
    for out in outs:
        out.wait()
    for n in range(24):
        exchange(n).wait_send()
    for copy in first + second + third:
        copy.wait_send()


def reduce_scatter(plan, f):
    u = plan.unit
    dma = pltpu.SemaphoreType.DMA
    g, _ = pl.pallas_call(
        functools.partial(rs_kernel, plan),
        out_shape=(
            jax.ShapeDtypeStruct((plan.window, LANES), F32),
            jax.ShapeDtypeStruct((12, u, LANES), F32),
        ),
        in_specs=[ANY],
        out_specs=(ANY, ANY),
        scratch_shapes=[pltpu.VMEM((n, u, LANES), F32) for n in (12, 12, 6, 3, 2, 2)]
        + [dma((n,)) for n in (2, 2, 3, 24, 24, 12, 12, 6, 6, 3, 3)],
        compiler_params=pltpu.CompilerParams(
            collective_id=0, has_side_effects=True, vmem_limit_bytes=VMEM_LIMIT
        ),
        name="reduce_scatter",
    )(f)
    return g


def ag_kernel(plan, win, w_ref, own_sem, s_send, s_recv, d_send, d_recv):
    u = plan.unit
    place = Place()
    partner = place.partner()

    def where(k, e):
        row = place.owner(dims_of(k), e, place.core) * plan.window + k * u
        return w_ref.at[pl.ds(pl.multiple_of(row, TILE), u)]

    slot = {(1, 0, 0): 0, (0, 1, 0): 1, (1, 1, 0): 2, (0, 0, 1): 3, (1, 0, 1): 4, (0, 1, 1): 5, (1, 1, 1): 6}

    def src(k, e):
        return win.at[pl.ds(k * u, u)] if e == (0, 0, 0) else where(k, e)

    def send(k, e, n):
        there = list(e)
        there[n] = 1
        s = slot[tuple(there)] * 3 + k
        return remote(src(k, e), where(k, e), s_send.at[s], s_recv.at[s], place.flipped(dims_of(k)[n]))

    def arrival(k, e):
        s = slot[e] * 3 + k
        return remote(where(k, e), where(k, e), s_send.at[s], s_recv.at[s], place.flipped(0))

    def share(k, e):
        s = (slot[e] + 1 if e != (0, 0, 0) else 0) * 3 + k
        return remote(src(k, e), where(k, e), d_send.at[s], d_recv.at[s], partner)

    def shared(k, e):
        s = (slot[e] + 1 if e != (0, 0, 0) else 0) * 3 + k
        row = place.owner(dims_of(k), e, 1 - place.core) * plan.window + k * u
        dst = w_ref.at[pl.ds(pl.multiple_of(row, TILE), u)]
        return remote(dst, dst, d_send.at[s], d_recv.at[s], partner)

    me = place.owner(dims_of(0), (0, 0, 0), place.core) * plan.window
    keep = pltpu.make_async_copy(win, w_ref.at[pl.ds(pl.multiple_of(me, TILE), plan.window)], own_sem)
    meet(place)
    sent = []

    def go(copy):
        copy.start()
        sent.append(copy)

    for n in range(3):
        for k in range(3):
            go(send(k, (0, 0, 0), n))
    keep.start()
    for k in range(3):
        go(share(k, (0, 0, 0)))
    for e in ((1, 0, 0), (0, 1, 0), (0, 0, 1), (1, 1, 0), (1, 0, 1), (0, 1, 1), (1, 1, 1)):
        for k in range(3):
            arrival(k, e).wait_recv()
            for n in range(1, 3):
                if not any(e[n:]):
                    go(send(k, e, n))
            go(share(k, e))
    keep.wait()
    for e in [(0, 0, 0)] + list(slot):
        for k in range(3):
            shared(k, e).wait_recv()
    for copy in sent:
        copy.wait_send()


def all_gather(plan, win):
    dma = pltpu.SemaphoreType.DMA
    return pl.pallas_call(
        functools.partial(ag_kernel, plan),
        out_shape=jax.ShapeDtypeStruct((plan.p * plan.window, LANES), BF),
        in_specs=[pl.BlockSpec(memory_space=pltpu.VMEM)],
        out_specs=ANY,
        scratch_shapes=[dma, dma((21,)), dma((21,)), dma((24,)), dma((24,))],
        compiler_params=pltpu.CompilerParams(collective_id=1, has_side_effects=True),
        name="all_gather",
    )(win)


def restore_kernel(plan, work, depth, w_ref, *refs):
    n = len(plan.big)
    outs, small = refs[:n], refs[n]
    ins, wide, stage = refs[n + 1], refs[n + 2], refs[n + 3:2 * n + 3]
    heads, tails, in_sem, out_sem, edge_sem, small_sem = refs[2 * n + 3:]
    p = plan.p

    def at(tile):
        r = max(r for r in range(p) if plan.first(r) <= tile)
        return r, r * plan.window + (tile - plan.first(r)) * TILE

    def pieces(i):
        _, _, rows, nj, flat = work[i]
        a, b = flat // TILE, (flat + rows * nj) // TILE
        cuts = [a] + [plan.first(r) for r in range(p) if a < plan.first(r) < b] + [b]
        return [(at(lo)[1], (lo - a) * TILE, (hi - lo) * TILE) for lo, hi in zip(cuts, cuts[1:])]

    def loads(i):
        s = i % depth
        return [
            pltpu.make_async_copy(w_ref.at[pl.ds(src, size)], ins.at[s, pl.ds(dst, size)], in_sem.at[s, m])
            for m, (src, dst, size) in enumerate(pieces(i))
        ]

    def store(i):
        k, r, rows, nj, flat = work[i]
        s = i % depth
        return pltpu.make_async_copy(stage[k].at[s], outs[k].at[pl.ds(r, rows)], out_sem.at[s])

    last = plan.first(p - 1)
    off = plan.small_row // TILE - last
    small_copy = pltpu.make_async_copy(
        w_ref.at[pl.ds((p - 1) * plan.window + off * TILE, small.shape[0])], ins.at[depth, pl.ds(0, small.shape[0])],
        small_sem,
    )
    small_copy.start()
    edges = []
    for r in range(1, p):
        t = plan.first(r)
        before = (r - 1) * plan.window + (t - plan.first(r - 1)) * TILE
        edges.append(pltpu.make_async_copy(w_ref.at[pl.ds(r * plan.window, TILE)], heads.at[r], edge_sem.at[0, r]))
        edges.append(pltpu.make_async_copy(w_ref.at[pl.ds(before, TILE)], tails.at[r], edge_sem.at[1, r]))
    for i in range(depth):
        for c in loads(i):
            c.start()
    for c in edges:
        c.start()
    for c in edges:
        c.wait()
    where = lax.broadcasted_iota(jnp.int32, (TILE, LANES), 0) * LANES + lax.broadcasted_iota(jnp.int32, (TILE, LANES), 1)
    for r in range(1, p):
        cut = r * plan.shard - plan.first(r) * TILE * LANES
        merged = jnp.where(where < cut, tails[r].astype(F32), heads[r].astype(F32))
        heads[r] = merged.astype(BF)
    small_copy.wait()
    small_out = pltpu.make_async_copy(ins.at[depth, pl.ds(0, small.shape[0])], small, small_sem)
    small_out.start()

    for i, (k, r, rows, nj, flat) in enumerate(work):
        s = i % depth
        for c in loads(i):
            c.wait()
        a, b = flat // TILE, (flat + rows * nj) // TILE
        for d in range(1, p):
            t = plan.first(d)
            if a <= t < b:
                ins[s, pl.ds((t - a) * TILE, TILE), :] = heads[d]
        if i >= depth:
            store(i - depth).wait()
        step = group_rows(rows, nj)

        def widen(g, _, s=s, size=step * nj):
            rs = pl.ds(pl.multiple_of(g * size, TILE), size)
            wide[rs, :] = ins[s, rs, :].astype(F32)
            return 0

        lax.fori_loop(0, rows // step, widen, 0)

        def body(g, _, k=k, s=s, nj=nj, step=step):
            for h in range(0, step, TILE):
                dst = pl.multiple_of(g * step + h, TILE)
                src = pl.multiple_of(dst * nj, TILE)
                for j in range(nj):
                    x = wide[pl.ds(src + j, TILE, stride=nj), :]
                    stage[k][s, pl.ds(dst, TILE), j * LANES:(j + 1) * LANES] = x.astype(BF)
            return 0

        lax.fori_loop(0, rows // step, body, 0)
        store(i).start()
        if i + depth < len(work):
            for c in loads(i + depth):
                c.start()
    for i in range(len(work) - depth, len(work)):
        store(i).wait()
    small_out.wait()


def restore(plan, wide, shapes):
    n = len(plan.big)
    depth = 3
    work = plan.chunks(3456)
    step = {w[0]: w[2] for w in work}
    size = max(w[2] * w[3] for w in work)
    small_rows = -(-plan.small_size // (LANES * TILE)) * TILE
    dma = pltpu.SemaphoreType.DMA
    outs = pl.pallas_call(
        functools.partial(restore_kernel, plan, work, depth),
        out_shape=[jax.ShapeDtypeStruct((rows, nj * LANES), BF) for rows, nj, _ in plan.big]
        + [jax.ShapeDtypeStruct((small_rows, LANES), BF)],
        in_specs=[ANY],
        out_specs=[ANY] * (n + 1),
        scratch_shapes=[pltpu.VMEM((depth + 1, size, LANES), BF), pltpu.VMEM((size, LANES), F32)]
        + [pltpu.VMEM((depth, step[k], plan.big[k][1] * LANES), BF) for k in range(n)]
        + [pltpu.VMEM((plan.p, TILE, LANES), BF), pltpu.VMEM((plan.p, TILE, LANES), BF)]
        + [dma((depth, 3)), dma((depth,)), dma((2, plan.p)), dma],
        compiler_params=pltpu.CompilerParams(vmem_limit_bytes=VMEM_LIMIT),
        name="restore",
    )(wide)
    flat = outs[n].reshape(-1)
    result = [x.reshape(s) for x, s in zip(outs[:n], shapes)]
    start = 0
    for s in shapes[n:]:
        size = math.prod(s)
        result.append(flat[start:start + size].reshape(s))
        start += size
    return tuple(result)


def adam_update(g, m, v, w, lr, beta1, beta2, eps, step):
    t = step.astype(jnp.float32)
    m_new = beta1 * m + (1.0 - beta1) * g
    v_new = beta2 * v + (1.0 - beta2) * (g * g)
    m_hat = m_new / (1.0 - beta1 ** t)
    v_hat = v_new / (1.0 - beta2 ** t)
    w_new = w - lr * m_hat / (jnp.sqrt(v_hat) + eps)
    return m_new, v_new, w_new


def solution(mesh):
    p = mesh.shape["outer"] * mesh.shape["inner"]

    def body(g_emb, g_qkv, g_o, g_w1, g_w2, g_bqkv, g_b1, g_dvec, m, v, w, lr, beta1, beta2, eps, step):
        grads = (g_emb, g_qkv, g_o, g_w1, g_w2, g_bqkv, g_b1, g_dvec)
        shapes = tuple(x.shape[1:] for x in grads)
        plan = Plan(shapes, p)
        local = flatten(plan, grads)
        total = reduce_scatter(plan, local).reshape(-1)
        r = lax.axis_index(AXES)
        offset = r * plan.shard - plan.first(r) * TILE * LANES
        g = lax.dynamic_slice(total, (offset,), (plan.shard,)) / p
        m_new, v_new, w_new = adam_update(g, m, v, w, lr, beta1, beta2, eps, step)
        win = jnp.zeros((plan.window * LANES,), BF)
        win = lax.dynamic_update_slice(win, w_new.astype(BF), (offset,))
        wb = all_gather(plan, win.reshape(plan.window, LANES))
        return (m_new, v_new, w_new) + restore(plan, wb, shapes)

    g3 = P(AXES, None, None)
    g4 = P(AXES, None, None, None)
    flat = P(AXES)
    rep = P()
    in_specs = (g3, g4, g4, g4, g4, g3, g3, g4, flat, flat, flat, rep, rep, rep, rep, rep)
    out_specs = (flat, flat, flat, rep, rep, rep, rep, rep, rep, rep, rep)
    return jax.shard_map(body, mesh=mesh, in_specs=in_specs, out_specs=out_specs, check_vma=False)
```

```python
import functools
import math

import jax
import jax.numpy as jnp
from jax import lax
from jax.experimental import pallas as pl
from jax.experimental.pallas import tpu as pltpu
from jax.sharding import PartitionSpec as P

AXES = ("outer", "inner")
MESH = pl.DeviceIdType.MESH
ANY = pl.BlockSpec(memory_space=pl.ANY)
LANES = 128
TILE = 16
VMEM_LIMIT = 63 * 1024 * 1024
BF = jnp.bfloat16
F32 = jnp.float32

ORDER = ((1, 1), (1, 0), (0, 1), (0, 0))


class Plan:
    def __init__(self, shapes, p):
        self.p = p
        self.sizes = [math.prod(s) for s in shapes]
        self.total = sum(self.sizes)
        self.shard = self.total // p
        self.big = []
        start = 0
        for s, n in zip(shapes, self.sizes):
            if s[-2] % TILE == 0:
                self.big.append((n // LANES, s[-1] // LANES, start // LANES))
                start += n
        self.small_row = start // LANES
        self.small_size = self.total - start
        self.starts, need = [], 0
        for r in range(p):
            self.starts.append(self.group(r * self.shard // LANES)[0])
            low, size = self.group(((r + 1) * self.shard - 1) // LANES)
            need = max(need, low + size - self.starts[r])
        self.unit = -(-need // (3 * 48)) * 48
        self.window = 3 * self.unit
        self.small_rows = self.starts[p - 1] + self.window - self.small_row

    def group(self, row):
        for n, nj, flat in self.big:
            if flat <= row < flat + n:
                size = 8 * nj
                return flat + (row - flat) // size * size, size
        return self.small_row + (row - self.small_row) // TILE * TILE, TILE

    def pieces(self, lo, hi):
        spans = [(flat, flat + n) for n, _, flat in self.big]
        spans.append((self.small_row, self.small_row + self.small_rows))
        out = []
        for k, (a, b) in enumerate(spans):
            x, y = max(a, lo), min(b, hi)
            if x < y:
                out.append((k, x - a, y - x, x - lo))
        return out

    def start(self, r):
        row = jnp.int32(self.starts[0])
        for i in range(1, self.p):
            row = jnp.where(r == i, jnp.int32(self.starts[i]), row)
        return row

    def segments(self, first):
        out = []
        for n, nj, flat in self.big:
            lo = jnp.maximum(first, flat)
            hi = jnp.minimum(first + self.window, flat + n)
            out.append((nj, lo - first, lax.div(jnp.maximum(hi - lo, 0), 8 * nj)))
        lo = jnp.maximum(first, self.small_row)
        hi = first + self.window
        out.append((1, lo - first, lax.div(jnp.maximum(hi - lo, 0), TILE)))
        return out


def as_stored(x, nj):
    return x.reshape(-1, 8, nj, LANES).transpose(0, 2, 1, 3).reshape(-1, LANES)


def from_stored(x, nj, shape):
    return x.reshape(-1, nj, 8, LANES).transpose(0, 2, 1, 3).reshape(shape)


class Place:
    def __init__(self):
        o, i = lax.axis_index("outer"), lax.axis_index("inner")
        self.bits = [lax.div(o, 2), lax.rem(o, 2), lax.div(i, 2)]
        self.core = lax.rem(i, 2)

    def flipped(self, d):
        b = list(self.bits)
        b[d] = 1 - b[d]
        return (b[0] * 2 + b[1], b[2] * 2 + self.core)

    def partner(self):
        return (self.bits[0] * 2 + self.bits[1], self.bits[2] * 2 + 1 - self.core)

    def neighbour(self, k, n):
        d = lax.rem(k + n, 3)
        b = [jnp.where(d == i, 1 - x, x) for i, x in enumerate(self.bits)]
        return (b[0] * 2 + b[1], b[2] * 2 + self.core)

    def block(self, n, core):
        k = lax.rem(n, 3)
        a = lax.div(n, 3)
        e = [1 - lax.div(a, 4), 1 - lax.rem(lax.div(a, 2), 2), 1 - lax.rem(a, 2)]
        r = core
        for d, weight in enumerate((8, 4, 2)):
            j = lax.rem(d - k + 3, 3)
            flip = jnp.where(j == 0, e[0], jnp.where(j == 1, e[1], e[2]))
            r = r + weight * (self.bits[d] + flip - 2 * self.bits[d] * flip)
        return r, k

    def owner(self, dims, e, core):
        b = list(self.bits)
        for d, flip in zip(dims, e):
            if flip:
                b[d] = 1 - b[d]
        return b[0] * 8 + b[1] * 4 + b[2] * 2 + core


def dims_of(k):
    return (k, (k + 1) % 3, (k + 2) % 3)


def meet(place):
    barrier = pltpu.get_barrier_semaphore()
    peers = [place.partner()] + [place.flipped(d) for d in range(3)]
    for peer in peers:
        pl.semaphore_signal(barrier, inc=1, device_id=peer, device_id_type=MESH)
    pl.semaphore_wait(barrier, len(peers))


def remote(src, dst, send, recv, dev):
    return pltpu.make_async_remote_copy(
        src_ref=src, dst_ref=dst, send_sem=send, recv_sem=recv, device_id=dev, device_id_type=MESH
    )


def rs_kernel(plan, *refs):
    n_in = len(plan.big) + 1
    xs, g_ref, late_ref = refs[:n_in], refs[n_in], refs[n_in + 1]
    early, r1, r2, r3, own, oth, flat = refs[n_in + 2:n_in + 9]
    (own_sem, oth_sem, out_sem, d_send, d_recv, s1_send, s1_recv, s2_send, s2_recv, s3_send, s3_recv) = refs[n_in + 9:]
    u = plan.unit
    place = Place()
    partner = place.partner()

    def pick(n, core, issue):
        r, k = place.block(n, core)
        for k0 in range(3):

            @pl.when(k == k0)
            def _(k0=k0):
                for r0 in range(plan.p):

                    @pl.when(r == r0)
                    def _(r0=r0):
                        lo = plan.starts[r0] + k0 * u
                        for t, row, size, at in plan.pieces(lo, lo + u):
                            issue(xs[t].at[pl.ds(row, size)], at, size)

    def exchange(i, _):
        def early_out(src, at, size):
            remote(src, early.at[i, pl.ds(at, size)], d_send.at[i], d_recv.at[i], partner).start()

        pick(i, 1 - place.core, early_out)
        return 0

    def exchange_late(i, _):
        def late_out(src, at, size):
            remote(src, late_ref.at[i, pl.ds(at, size)], d_send.at[12 + i], d_recv.at[12 + i], partner).start()

        pick(12 + i, 1 - place.core, late_out)
        return 0

    def arrived(i):
        return remote(early.at[i], early.at[i], d_send.at[i], d_recv.at[i], partner)

    def arrived_late(i):
        return remote(late_ref.at[i], late_ref.at[i], d_send.at[12 + i], d_recv.at[12 + i], partner)

    def load(i):
        slot = lax.rem(i, 2)

        def issue(src, at, size):
            pltpu.make_async_copy(src, own.at[slot, pl.ds(at, size)], own_sem.at[slot]).start()

        pick(i, place.core, issue)

    def loaded(i):
        slot = lax.rem(i, 2)
        return pltpu.make_async_copy(late_ref.at[0], own.at[slot], own_sem.at[slot])

    def fetch(i):
        slot = lax.rem(i, 2)
        return pltpu.make_async_copy(late_ref.at[i], oth.at[slot], oth_sem.at[slot])

    def hop(stage, i):
        src, dst, send, recv = (
            (early, r1, s1_send, s1_recv), (r1, r2, s2_send, s2_recv)
        )[stage]
        return remote(src.at[i], dst.at[i], send.at[i], recv.at[i], place.neighbour(lax.rem(i, 3), stage))

    def last_hop(k):
        return remote(r1.at[6 + k], r3.at[k], s3_send.at[k], s3_recv.at[k], place.flipped(dims_of(k)[2]))

    def add(dst, *srcs):
        step = 48

        def body(i, _):
            rows = pl.ds(pl.multiple_of(i * step, 16), step)
            total = dst[rows, :]
            for s in srcs:
                total = total + s[rows, :]
            dst[rows, :] = total
            return 0

        lax.fori_loop(0, u // step, body, 0)

    def preload(i, _):
        load(i)
        return 0

    meet(place)
    lax.fori_loop(0, 12, exchange, 0)
    lax.fori_loop(0, 2, preload, 0)
    lax.fori_loop(0, 12, exchange_late, 0)

    def first(i, _):
        slot = lax.rem(i, 2)
        loaded(i).wait()
        arrived(i).wait_recv()
        add(early.at[i], own.at[slot])
        hop(0, i).start()
        load(i + 2)
        return 0

    lax.fori_loop(0, 12, first, 0)

    for i in range(2):
        arrived_late(i).wait_recv()
        fetch(i).start()

    def second(i, _):
        slot = lax.rem(i, 2)
        loaded(i).wait()
        fetch(i).wait()
        hop(0, i).wait_recv()
        add(r1.at[i], own.at[slot], oth.at[slot])

        @pl.when(i < 6)
        def _():
            hop(1, i).start()

        @pl.when(i < 10)
        def _():
            load(i + 14)
            arrived_late(i + 2).wait_recv()
            fetch(i + 2).start()

        return 0

    lax.fori_loop(0, 12, second, 0)

    for i in range(6):
        hop(1, i).wait_recv()
        add(r1.at[6 + i], r2.at[i])
        if i < 3:
            last_hop(i).start()
    for k in range(3):
        last_hop(k).wait_recv()
        add(r1.at[9 + k], r3.at[k])
    first_row = plan.start(place.owner(dims_of(0), (0, 0, 0), place.core))
    stored = r1.at[pl.ds(9, 3)].reshape(3 * u, LANES)
    for nj, row, groups in plan.segments(first_row):

        def sort(i, _, nj=nj, row=row):
            size = 8 * nj if nj > 1 else TILE
            base = pl.multiple_of(row + i * size, TILE)
            if nj == 1:
                flat[pl.ds(base, TILE), :] = stored[pl.ds(base, TILE), :]
            else:
                for j in range(nj):
                    flat[pl.ds(base + j, 8, stride=nj), :] = stored[pl.ds(base + j * 8, 8), :]
            return 0

        lax.fori_loop(0, groups, sort, 0)
    out = pltpu.make_async_copy(flat, g_ref, out_sem)
    out.start()

    def sent(i, _):
        arrived(i).wait_send()
        arrived_late(i).wait_send()
        hop(0, i).wait_send()
        return 0

    lax.fori_loop(0, 12, sent, 0)
    for i in range(6):
        hop(1, i).wait_send()
    for k in range(3):
        last_hop(k).wait_send()
    out.wait()


def reduce_scatter(plan, xs):
    u = plan.unit
    dma = pltpu.SemaphoreType.DMA
    g, _ = pl.pallas_call(
        functools.partial(rs_kernel, plan),
        out_shape=(
            jax.ShapeDtypeStruct((plan.window, LANES), F32),
            jax.ShapeDtypeStruct((12, u, LANES), F32),
        ),
        in_specs=[ANY] * len(xs),
        out_specs=(ANY, ANY),
        scratch_shapes=[pltpu.VMEM((n, u, LANES), F32) for n in (12, 12, 6, 3, 2, 2)]
        + [pltpu.VMEM((plan.window, LANES), F32)]
        + [dma((2,)), dma((2,)), dma] + [dma((n,)) for n in (24, 24, 12, 12, 6, 6, 3, 3)],
        compiler_params=pltpu.CompilerParams(
            collective_id=0, has_side_effects=True, vmem_limit_bytes=VMEM_LIMIT
        ),
        name="reduce_scatter",
    )(*xs)
    return g


def ag_kernel(plan, values, w_ref, win, own_sem, s_send, s_recv, d_send, d_recv):
    u = plan.unit
    place = Place()
    partner = place.partner()

    for nj, row, groups in plan.segments(plan.start(place.owner(dims_of(0), (0, 0, 0), place.core))):

        def sort(i, _, nj=nj, row=row):
            size = 8 * nj if nj > 1 else TILE
            base = pl.multiple_of(row + i * size, TILE)
            if nj == 1:
                win[pl.ds(base, TILE), :] = values[pl.ds(base, TILE), :].astype(BF)
            else:
                for j in range(0, nj, 2):
                    pair = [values[pl.ds(base + j + h, 8, stride=nj), :] for h in range(2)]
                    win[pl.ds(base + j * 8, TILE), :] = jnp.concatenate(pair, axis=0).astype(BF)
            return 0

        lax.fori_loop(0, groups, sort, 0)

    def where(k, e):
        row = place.owner(dims_of(k), e, place.core) * plan.window + k * u
        return w_ref.at[pl.ds(pl.multiple_of(row, TILE), u)]

    slot = {(1, 0, 0): 0, (0, 1, 0): 1, (1, 1, 0): 2, (0, 0, 1): 3, (1, 0, 1): 4, (0, 1, 1): 5, (1, 1, 1): 6}

    def src(k, e):
        return win.at[pl.ds(k * u, u)] if e == (0, 0, 0) else where(k, e)

    def send(k, e, n):
        there = list(e)
        there[n] = 1
        s = slot[tuple(there)] * 3 + k
        return remote(src(k, e), where(k, e), s_send.at[s], s_recv.at[s], place.flipped(dims_of(k)[n]))

    def arrival(k, e):
        s = slot[e] * 3 + k
        return remote(where(k, e), where(k, e), s_send.at[s], s_recv.at[s], place.flipped(0))

    def share(k, e):
        s = (slot[e] + 1 if e != (0, 0, 0) else 0) * 3 + k
        return remote(src(k, e), where(k, e), d_send.at[s], d_recv.at[s], partner)

    def shared(k, e):
        s = (slot[e] + 1 if e != (0, 0, 0) else 0) * 3 + k
        row = place.owner(dims_of(k), e, 1 - place.core) * plan.window + k * u
        dst = w_ref.at[pl.ds(pl.multiple_of(row, TILE), u)]
        return remote(dst, dst, d_send.at[s], d_recv.at[s], partner)

    me = place.owner(dims_of(0), (0, 0, 0), place.core) * plan.window
    keep = pltpu.make_async_copy(win, w_ref.at[pl.ds(pl.multiple_of(me, TILE), plan.window)], own_sem)
    meet(place)
    sent = []

    def go(copy):
        copy.start()
        sent.append(copy)

    for n in range(3):
        for k in range(3):
            go(send(k, (0, 0, 0), n))
    keep.start()
    for k in range(3):
        go(share(k, (0, 0, 0)))
    for e in ((1, 0, 0), (0, 1, 0), (0, 0, 1), (1, 1, 0), (1, 0, 1), (0, 1, 1), (1, 1, 1)):
        for k in range(3):
            arrival(k, e).wait_recv()
            for n in range(1, 3):
                if not any(e[n:]):
                    go(send(k, e, n))
            go(share(k, e))
    keep.wait()
    for e in [(0, 0, 0)] + list(slot):
        for k in range(3):
            shared(k, e).wait_recv()
    for copy in sent:
        copy.wait_send()


def all_gather(plan, win):
    dma = pltpu.SemaphoreType.DMA
    return pl.pallas_call(
        functools.partial(ag_kernel, plan),
        out_shape=jax.ShapeDtypeStruct((plan.p * plan.window, LANES), BF),
        in_specs=[pl.BlockSpec(memory_space=pltpu.VMEM)],
        out_specs=ANY,
        scratch_shapes=[pltpu.VMEM((plan.window, LANES), BF), dma, dma((21,)), dma((21,)), dma((24,)), dma((24,))],
        compiler_params=pltpu.CompilerParams(collective_id=1, has_side_effects=True, vmem_limit_bytes=16 * 1024 * 1024),
        name="all_gather",
    )(win)


def restore_kernel(plan, work, depth, w_ref, *refs):
    n = len(plan.big) + 1
    outs = refs[:n]
    buf, heads, tails, in_sem, out_sem, edge_sem = refs[n:]
    p, ahead = plan.p, depth // 2

    def parts(i):
        _, _, rows, flat = work[i]
        cuts = [flat] + [s for s in plan.starts[1:] if flat < s < flat + rows] + [flat + rows]
        out = []
        for lo, hi in zip(cuts, cuts[1:]):
            r = max(r for r in range(p) if plan.starts[r] <= lo)
            out.append((r * plan.window + lo - plan.starts[r], lo - flat, hi - lo))
        return out

    def loads(i):
        s = i % depth
        return [
            pltpu.make_async_copy(w_ref.at[pl.ds(src, size)], buf.at[s, pl.ds(dst, size)], in_sem.at[s, m])
            for m, (src, dst, size) in enumerate(parts(i))
        ]

    def store(i):
        k, row, rows, _ = work[i]
        s = i % depth
        return pltpu.make_async_copy(buf.at[s, pl.ds(0, rows)], outs[k].at[pl.ds(row, rows)], out_sem.at[s])

    edges, size = [], [0] * p
    for r in range(1, p):
        size[r] = plan.group(plan.starts[r])[1]
        before = (r - 1) * plan.window + plan.starts[r] - plan.starts[r - 1]
        for m, (ref, src) in enumerate(((heads, r * plan.window), (tails, before))):
            edges.append(
                pltpu.make_async_copy(w_ref.at[pl.ds(src, size[r])], ref.at[r, pl.ds(0, size[r])], edge_sem.at[m, r])
            )
    for c in edges:
        c.start()
    for i in range(ahead):
        for c in loads(i):
            c.start()
    for c in edges:
        c.wait()
    for r in range(1, p):
        nj = size[r] // 8
        shape = (size[r], LANES)
        row, lane = lax.broadcasted_iota(jnp.int32, shape, 0), lax.broadcasted_iota(jnp.int32, shape, 1)
        at = (lax.rem(row, 8) * nj + lax.div(row, 8)) * LANES + lane
        cut = r * plan.shard - plan.starts[r] * LANES
        rows = pl.ds(0, size[r])
        heads[r, rows, :] = jnp.where(at < cut, tails[r, rows, :].astype(F32), heads[r, rows, :].astype(F32)).astype(BF)

    for i, (k, row, rows, flat) in enumerate(work):
        s = i % depth
        for c in loads(i):
            c.wait()
        for r in range(1, p):
            if flat <= plan.starts[r] < flat + rows:
                buf[s, pl.ds(plan.starts[r] - flat, size[r]), :] = heads[r, pl.ds(0, size[r]), :]
        store(i).start()
        if i + ahead < len(work):
            if i + ahead >= depth:
                store(i + ahead - depth).wait()
            for c in loads(i + ahead):
                c.start()
    for i in range(max(0, len(work) - depth), len(work)):
        store(i).wait()


def restore(plan, gathered, shapes):
    n = len(plan.big)
    depth, top = 8, 192
    work = []
    for k, (rows, nj, flat) in enumerate(plan.big):
        step = max(c for c in range(8 * nj, 3457, 8 * nj) if rows % c == 0)
        work += [(k, r, step, flat + r) for r in range(0, rows, step)]
    small_rows = -(-plan.small_size // (LANES * TILE)) * TILE
    work.append((n, 0, small_rows, plan.small_row))
    dma = pltpu.SemaphoreType.DMA
    outs = pl.pallas_call(
        functools.partial(restore_kernel, plan, work, depth),
        out_shape=[jax.ShapeDtypeStruct((rows, LANES), BF) for rows, _, _ in plan.big]
        + [jax.ShapeDtypeStruct((small_rows, LANES), BF)],
        in_specs=[ANY],
        out_specs=[ANY] * (n + 1),
        scratch_shapes=[pltpu.VMEM((depth, max(w[2] for w in work), LANES), BF)]
        + [pltpu.VMEM((plan.p, top, LANES), BF)] * 2
        + [dma((depth, 3)), dma((depth,)), dma((2, plan.p))],
        compiler_params=pltpu.CompilerParams(vmem_limit_bytes=32 * 1024 * 1024),
        name="restore",
    )(gathered)
    flat = outs[n].reshape(-1)
    result = [from_stored(x, nj, s) for x, (_, nj, _), s in zip(outs, plan.big, shapes)]
    start = 0
    for s in shapes[n:]:
        size = math.prod(s)
        result.append(flat[start:start + size].reshape(s))
        start += size
    return tuple(result)


def adam_update(g, m, v, w, lr, beta1, beta2, eps, step):
    t = step.astype(jnp.float32)
    m_new = beta1 * m + (1.0 - beta1) * g
    v_new = beta2 * v + (1.0 - beta2) * (g * g)
    m_hat = m_new / (1.0 - beta1 ** t)
    v_hat = v_new / (1.0 - beta2 ** t)
    w_new = w - lr * m_hat / (jnp.sqrt(v_hat) + eps)
    return m_new, v_new, w_new


def solution(mesh):
    p = mesh.shape["outer"] * mesh.shape["inner"]

    def body(g_emb, g_qkv, g_o, g_w1, g_w2, g_bqkv, g_b1, g_dvec, m, v, w, lr, beta1, beta2, eps, step):
        grads = (g_emb, g_qkv, g_o, g_w1, g_w2, g_bqkv, g_b1, g_dvec)
        shapes = tuple(x.shape[1:] for x in grads)
        plan = Plan(shapes, p)
        n = len(plan.big)
        small = jnp.concatenate([x.reshape(-1) for x in grads[n:]])
        small = jnp.pad(small, (0, plan.small_rows * LANES - plan.small_size)).reshape(-1, LANES)
        stored = [as_stored(x, nj) for x, (_, nj, _) in zip(grads, plan.big)]
        total = reduce_scatter(plan, stored + [small]).reshape(-1)
        r = lax.axis_index(AXES)
        offset = r * plan.shard - plan.start(r) * LANES
        g = lax.dynamic_slice(total, (offset,), (plan.shard,)) / p
        m_new, v_new, w_new = adam_update(g, m, v, w, lr, beta1, beta2, eps, step)
        front = max(i * plan.shard - plan.starts[i] * LANES for i in range(p))
        back = plan.window * LANES - plan.shard
        win = lax.dynamic_slice(jnp.pad(w_new, (front, back)), (front - offset,), (plan.window * LANES,))
        wb = all_gather(plan, win.reshape(plan.window, LANES))
        return (m_new, v_new, w_new) + restore(plan, wb, shapes)

    g3 = P(AXES, None, None)
    g4 = P(AXES, None, None, None)
    flat = P(AXES)
    rep = P()
    in_specs = (g3, g4, g4, g4, g4, g3, g3, g4, flat, flat, flat, rep, rep, rep, rep, rep)
    out_specs = (flat, flat, flat, rep, rep, rep, rep, rep, rep, rep, rep)
    return jax.shard_map(body, mesh=mesh, in_specs=in_specs, out_specs=out_specs, check_vma=False)
```

```python
import functools
import math

import jax
import jax.numpy as jnp
from jax import lax
from jax.experimental import pallas as pl
from jax.experimental.pallas import tpu as pltpu
from jax.sharding import PartitionSpec as P

AXES = ("outer", "inner")
MESH = pl.DeviceIdType.MESH
ANY = pl.BlockSpec(memory_space=pl.ANY)
LANES = 128
TILE = 16
SPLIT = 4
DEEP = 4
LEAD = 12
BF = jnp.bfloat16
F32 = jnp.float32


class Plan:
    def __init__(self, shapes, p):
        self.p = p
        self.sizes = [math.prod(s) for s in shapes]
        self.total = sum(self.sizes)
        self.shard = self.total // p
        self.big = []
        start = 0
        for s, n in zip(shapes, self.sizes):
            if s[-2] % TILE == 0:
                self.big.append((n // LANES, s[-1] // LANES, start // LANES))
                start += n
        self.small_row = start // LANES
        self.small_size = self.total - start
        self.starts, need = [], 0
        for r in range(p):
            self.starts.append(self.group(r * self.shard // LANES)[0])
            low, size = self.group(((r + 1) * self.shard - 1) // LANES)
            need = max(need, low + size - self.starts[r])
        self.part = -(-need // (3 * SPLIT * TILE)) * TILE
        self.unit = SPLIT * self.part
        self.window = 3 * self.unit
        self.small_rows = self.starts[p - 1] + self.window - self.small_row

    def group(self, row):
        for n, nj, flat in self.big:
            if flat <= row < flat + n:
                size = 8 * nj
                return flat + (row - flat) // size * size, size
        return self.small_row + (row - self.small_row) // TILE * TILE, TILE

    def spans(self):
        spans = [(flat, flat + n) for n, _, flat in self.big]
        return spans + [(self.small_row, self.small_row + self.small_rows)]

    def crossing(self):
        out = {}
        for start in self.starts:
            for lo in range(start, start + self.window, self.part):
                cuts = []
                for t, (x, y) in enumerate(self.spans()):
                    x, y = max(x, lo), min(y, lo + self.part)
                    if x < y:
                        cuts.append((t, x - self.spans()[t][0], y - x, x - lo))
                if len(cuts) > 1:
                    out[lo] = cuts
        return out

    def start(self, r):
        row = jnp.int32(self.starts[0])
        for i in range(1, self.p):
            row = jnp.where(r == i, jnp.int32(self.starts[i]), row)
        return row

    def segments(self, first):
        out = []
        for n, nj, flat in self.big:
            lo = jnp.maximum(first, flat)
            hi = jnp.minimum(first + self.window, flat + n)
            out.append((nj, lo - first, lax.div(jnp.maximum(hi - lo, 0), 8 * nj)))
        return out

    def pairs(self):
        out, row = [], 0
        for n in self.sizes[len(self.big):]:
            out.append((row, n // (2 * LANES)))
            row += n // LANES
        return out


def as_stored(x, nj):
    return x.reshape(-1, 8, nj, LANES).transpose(0, 2, 1, 3).reshape(-1, LANES)


def from_stored(x, nj, shape):
    return x.reshape(-1, nj, 8, LANES).transpose(0, 2, 1, 3).reshape(shape)


class Place:
    def __init__(self):
        o, i = lax.axis_index("outer"), lax.axis_index("inner")
        self.bits = [lax.div(o, 2), lax.rem(o, 2), lax.div(i, 2)]
        self.core = lax.rem(i, 2)

    def flipped(self, d):
        b = list(self.bits)
        b[d] = 1 - b[d]
        return (b[0] * 2 + b[1], b[2] * 2 + self.core)

    def partner(self):
        return (self.bits[0] * 2 + self.bits[1], self.bits[2] * 2 + 1 - self.core)

    def neighbour(self, k, n):
        d = lax.rem(k + n, 3)
        b = [jnp.where(d == i, 1 - x, x) for i, x in enumerate(self.bits)]
        return (b[0] * 2 + b[1], b[2] * 2 + self.core)

    def part(self, i):
        a, s, k = lax.div(i, 3 * SPLIT), lax.rem(lax.div(i, 3), SPLIT), lax.rem(i, 3)
        return a, k, s, a * (3 * SPLIT) + k * SPLIT + s

    def block(self, a, k, core):
        e = [1 - lax.div(a, 4), 1 - lax.rem(lax.div(a, 2), 2), 1 - lax.rem(a, 2)]
        r = core
        for d, weight in enumerate((8, 4, 2)):
            j = lax.rem(d - k + 3, 3)
            flip = jnp.where(j == 0, e[0], jnp.where(j == 1, e[1], e[2]))
            r = r + weight * (self.bits[d] + flip - 2 * self.bits[d] * flip)
        return r

    def owner(self, dims, e, core):
        b = list(self.bits)
        for d, flip in zip(dims, e):
            if flip:
                b[d] = 1 - b[d]
        return b[0] * 8 + b[1] * 4 + b[2] * 2 + core


def dims_of(k):
    return (k, (k + 1) % 3, (k + 2) % 3)


def arrive(place):
    barrier = pltpu.get_barrier_semaphore()
    for peer in [place.partner()] + [place.flipped(d) for d in range(3)]:
        pl.semaphore_signal(barrier, inc=1, device_id=peer, device_id_type=MESH)


def meet():
    pl.semaphore_wait(pltpu.get_barrier_semaphore(), 4)


def remote(src, dst, send, recv, dev):
    return pltpu.make_async_remote_copy(
        src_ref=src, dst_ref=dst, send_sem=send, recv_sem=recv, device_id=dev, device_id_type=MESH
    )


def rs_kernel(plan, *refs):
    n_in = len(plan.big) + 1
    xs, flat, late_ref = refs[:n_in], refs[n_in], refs[n_in + 1]
    early, r1, r2, r3, own, oth = refs[n_in + 2:n_in + 8]
    own_sem, oth_sem, d_send, d_recv, s1_send, s1_recv, s2_send, s2_recv, s3_send, s3_recv = refs[n_in + 8:]
    part = plan.part
    wave = 3 * SPLIT
    early_n = 4 * wave
    place = Place()
    partner = place.partner()
    crossing = plan.crossing()

    def pick(i, core, issue):
        a, k, s, _ = place.part(i)
        row = plan.start(place.block(a, k, core)) + k * plan.unit + s * part
        for t, (lo, hi) in enumerate(plan.spans()):

            @pl.when((row >= lo) & (row <= hi - part))
            def _(t=t, lo=lo):
                issue(xs[t].at[pl.ds(pl.multiple_of(row - lo, TILE), part)], 0, part)

        for first, cuts in crossing.items():

            @pl.when(row == first)
            def _(cuts=cuts):
                for t, at, size, to in cuts:
                    issue(xs[t].at[pl.ds(at, size)], to, size)

    def swap(i):
        slot = place.part(i)[3]

        def issue(src, at, size):
            remote(src, early.at[slot, pl.ds(at, size)], d_send.at[slot], d_recv.at[slot], partner).start()

        pick(i, 1 - place.core, issue)

    def swap_late(i):
        slot = place.part(i)[3]

        def issue(src, at, size):
            remote(
                src, late_ref.at[slot, pl.ds(at, size)], d_send.at[early_n + slot], d_recv.at[early_n + slot], partner
            ).start()

        pick(early_n + i, 1 - place.core, issue)

    def swapped(slot):
        return remote(early.at[slot], early.at[slot], d_send.at[slot], d_recv.at[slot], partner)

    def swapped_late(slot):
        sems = d_send.at[early_n + slot], d_recv.at[early_n + slot]
        return remote(late_ref.at[slot], late_ref.at[slot], *sems, partner)

    def load(i):
        to = lax.rem(i, DEEP)

        def issue(src, at, size):
            pltpu.make_async_copy(src, own.at[to, pl.ds(at, size)], own_sem.at[to]).start()

        pick(i, place.core, issue)

    def loaded(i):
        to = lax.rem(i, DEEP)
        return pltpu.make_async_copy(late_ref.at[0], own.at[to], own_sem.at[to])

    def fetch(i):
        to = lax.rem(i, DEEP)
        return pltpu.make_async_copy(late_ref.at[place.part(i)[3]], oth.at[to], oth_sem.at[to])

    def hop(stage, k, slot):
        src, dst, send, recv, base = (
            (early, r1, s1_send, s1_recv, 0),
            (r1, r2, s2_send, s2_recv, 0),
            (r1, r3, s3_send, s3_recv, 2 * wave),
        )[stage]
        return remote(src.at[base + slot], dst.at[slot], send.at[slot], recv.at[slot], place.neighbour(k, stage))

    def add(dst, *srcs):
        step = 48

        def body(i, _):
            rows = pl.ds(pl.multiple_of(i * step, TILE), step)
            total = dst[rows, :]
            for s in srcs:
                total = total + s[rows, :]
            dst[rows, :] = total
            return 0

        lax.fori_loop(0, part // step, body, 0)

    def loop(count, f):
        def body(i, _):
            f(i)
            return 0

        lax.fori_loop(0, count, body, 0)

    arrive(place)
    loop(DEEP, load)
    meet()
    loop(LEAD, swap)

    def first(i):
        _, k, _, slot = place.part(i)

        @pl.when(i + LEAD < early_n)
        def _():
            swap(i + LEAD)

        @pl.when(i + LEAD >= early_n)
        def _():
            swap_late(i + LEAD - early_n)

        loaded(i).wait()
        swapped(slot).wait_recv()
        add(early.at[slot], own.at[lax.rem(i, DEEP)])
        hop(0, k, slot).start()
        load(i + DEEP)

    loop(early_n, first)

    def prefetch(i):
        swapped_late(place.part(i)[3]).wait_recv()
        fetch(i).start()

    loop(DEEP, prefetch)

    def second(i):
        _, k, _, slot = place.part(i)

        @pl.when(i + LEAD < early_n)
        def _():
            swap_late(i + LEAD)

        to = lax.rem(i, DEEP)
        loaded(i).wait()
        fetch(i).wait()
        hop(0, k, slot).wait_recv()
        add(r1.at[slot], own.at[to], oth.at[to])

        @pl.when(i < 2 * wave)
        def _():
            hop(1, k, slot).start()

        @pl.when(i + DEEP < early_n)
        def _():
            load(early_n + i + DEEP)
            prefetch(i + DEEP)

    loop(early_n, second)

    def third(i):
        _, k, _, slot = place.part(i)
        hop(1, k, slot).wait_recv()
        add(r1.at[2 * wave + slot], r2.at[slot])

        @pl.when(i < wave)
        def _():
            hop(2, k, slot).start()

    loop(2 * wave, third)

    def fourth(i):
        _, k, _, slot = place.part(i)
        hop(2, k, slot).wait_recv()
        add(r1.at[3 * wave + slot], r3.at[slot])

    loop(wave, fourth)

    me = place.owner(dims_of(0), (0, 0, 0), place.core)
    stored = r1.at[pl.ds(3 * wave, wave)].reshape(plan.window, LANES)
    for nj, row, groups in plan.segments(plan.start(me)):

        def sort(i, nj=nj, row=row):
            base = pl.multiple_of(row + i * 8 * nj, TILE)
            for j in range(nj):
                flat[pl.ds(base + j, 8, stride=nj), :] = stored[pl.ds(base + j * 8, 8), :]

        loop(groups, sort)

    @pl.when(me == plan.p - 1)
    def _():
        base = plan.small_row - plan.starts[plan.p - 1]
        for row, nj in plan.pairs():
            for layer in range(2):
                at = base + row + layer * nj
                flat[pl.ds(at, nj), :] = stored[pl.ds(base + row + layer, nj, stride=2), :]

    def sent(i):
        _, k, _, slot = place.part(i)
        swapped(slot).wait_send()
        swapped_late(slot).wait_send()
        hop(0, k, slot).wait_send()

        @pl.when(i < 2 * wave)
        def _():
            hop(1, k, slot).wait_send()

        @pl.when(i < wave)
        def _():
            hop(2, k, slot).wait_send()

    loop(early_n, sent)


def reduce_scatter(plan, xs):
    dma = pltpu.SemaphoreType.DMA
    wave = 3 * SPLIT
    slots = [4 * wave, 4 * wave, 2 * wave, wave, DEEP, DEEP]
    used = (sum(slots) * plan.part * LANES * 4 >> 20) + 2
    g, _ = pl.pallas_call(
        functools.partial(rs_kernel, plan),
        out_shape=(
            pltpu.VMEM((plan.window, LANES), F32),
            jax.ShapeDtypeStruct((4 * wave, plan.part, LANES), F32),
        ),
        in_specs=[ANY] * len(xs),
        out_specs=(pl.BlockSpec(memory_space=pltpu.VMEM), ANY),
        scratch_shapes=[pltpu.VMEM((n, plan.part, LANES), F32) for n in slots]
        + [dma((DEEP,)), dma((DEEP,))]
        + [dma((n * wave,)) for n in (8, 8, 4, 4, 2, 2, 1, 1)],
        compiler_params=pltpu.CompilerParams(
            collective_id=0, has_side_effects=True, vmem_limit_bytes=used << 20
        ),
        name="reduce_scatter",
    )(*xs)
    return g


def ag_kernel(plan, values, *refs):
    w_refs, (win, tiny, s_send, s_recv, d_send, d_recv) = refs[:3], refs[3:]
    part, unit = plan.part, plan.unit
    place = Place()
    partner = place.partner()
    here = (0, 0, 0)
    me = place.owner(dims_of(0), here, place.core)
    arrive(place)

    for nj, row, groups in plan.segments(plan.start(me)):

        def sort(i, _, nj=nj, row=row):
            base = pl.multiple_of(row + i * 8 * nj, TILE)
            for j in range(0, nj, 2):
                pair = [values[pl.ds(base + j + h, 8, stride=nj), :] for h in range(2)]
                win[pl.ds(base + j * 8, TILE), :] = jnp.concatenate(pair, axis=0).astype(BF)
            return 0

        lax.fori_loop(0, groups, sort, 0)

    @pl.when(me == plan.p - 1)
    def _():
        base = plan.small_row - plan.starts[plan.p - 1]
        tiny[...] = jnp.zeros_like(tiny)
        for row, nj in plan.pairs():
            for layer in range(2):
                tiny[pl.ds(row + layer, nj, stride=2), :] = values[pl.ds(base + row + layer * nj, nj), :]
        win[pl.ds(base, tiny.shape[0]), :] = tiny[...].astype(BF)

    def rows_of(k, e, s, core):
        row = place.owner(dims_of(k), e, core) * unit + s * part
        return w_refs[k].at[pl.ds(pl.multiple_of(row, TILE), part)]

    slot = {here: 0, (1, 0, 0): 1, (0, 1, 0): 2, (0, 0, 1): 3, (1, 1, 0): 4, (1, 0, 1): 5, (0, 1, 1): 6, (1, 1, 1): 7}

    def index(k, e, s):
        return (slot[e] * 3 + k) * SPLIT + s

    def src(k, e, s):
        return win.at[pl.ds(k * plan.unit + s * part, part)] if e == here else rows_of(k, e, s, place.core)

    sent = []

    def send(k, e, s, n):
        there = list(e)
        there[n] = 1
        i = index(k, tuple(there), s)
        copy = remote(
            src(k, e, s), rows_of(k, e, s, place.core), s_send.at[i], s_recv.at[i], place.flipped(dims_of(k)[n])
        )
        copy.start()
        sent.append(copy)

    def share(k, e, s):
        i = index(k, e, s)
        copy = remote(src(k, e, s), rows_of(k, e, s, place.core), d_send.at[i], d_recv.at[i], partner)
        copy.start()
        sent.append(copy)

    def arrival(k, e, s):
        i, dst = index(k, e, s), rows_of(k, e, s, place.core)
        return remote(dst, dst, s_send.at[i], s_recv.at[i], partner)

    def shared(k, e, s):
        i, dst = index(k, e, s), rows_of(k, e, s, 1 - place.core)
        return remote(dst, dst, d_send.at[i], d_recv.at[i], partner)

    meet()
    for n in range(3):
        for s in range(SPLIT):
            for k in range(3):
                send(k, here, s, n)
    for s in range(SPLIT):
        for k in range(3):
            share(k, here, s)
    rows = 3 * TILE
    for k in range(3):

        def keep(i, _, k=k):
            at = pl.multiple_of(i * rows, rows)
            w_refs[k][pl.ds(pl.multiple_of(me * unit + at, TILE), rows), :] = win[pl.ds(k * unit + at, rows), :]
            return 0

        lax.fori_loop(0, unit // rows, keep, 0)
    for e in list(slot)[1:]:
        for s in range(SPLIT):
            for k in range(3):
                arrival(k, e, s).wait_recv()
                for n in range(1, 3):
                    if not any(e[n:]):
                        send(k, e, s, n)
                share(k, e, s)
    for e in slot:
        for s in range(SPLIT):
            for k in range(3):
                shared(k, e, s).wait_recv()
    for copy in sent:
        copy.wait_send()

    for r in range(1, plan.p):
        size = plan.group(plan.starts[r])[1]
        nj, shape = size // 8, (size, LANES)
        row, lane = lax.broadcasted_iota(jnp.int32, shape, 0), lax.broadcasted_iota(jnp.int32, shape, 1)
        at = (lax.rem(row, 8) * nj + lax.div(row, 8)) * LANES + lane
        cut = r * plan.shard - plan.starts[r] * LANES
        gap = plan.starts[r] - plan.starts[r - 1] - 2 * unit
        before = w_refs[2][pl.ds((r - 1) * unit + gap, size), :]
        rows = pl.ds(r * unit, size)
        w_refs[0][rows, :] = jnp.where(at < cut, before.astype(F32), w_refs[0][rows, :].astype(F32)).astype(BF)


def all_gather(plan, win):
    dma = pltpu.SemaphoreType.DMA
    n = 8 * 3 * SPLIT
    return pl.pallas_call(
        functools.partial(ag_kernel, plan),
        out_shape=[pltpu.VMEM((plan.p * plan.unit, LANES), BF)] * 3,
        in_specs=[pl.BlockSpec(memory_space=pltpu.VMEM)],
        out_specs=[pl.BlockSpec(memory_space=pltpu.VMEM)] * 3,
        scratch_shapes=[pltpu.VMEM((plan.window, LANES), BF), pltpu.VMEM((small_rows(plan), LANES), F32)]
        + [dma((n,))] * 4,
        compiler_params=pltpu.CompilerParams(collective_id=1, has_side_effects=True, vmem_limit_bytes=8 << 20),
        name="all_gather",
    )(win)


def small_rows(plan):
    return -(-plan.small_size // (LANES * TILE)) * TILE


def restore_kernel(plan, *refs):
    w_refs, outs, out_sem = refs[:3], refs[3:-1], refs[-1]
    p = plan.p
    spans = plan.spans()[:-1] + [(plan.small_row, plan.small_row + small_rows(plan))]
    copies = []
    for r in range(p):
        lo = plan.starts[r]
        hi = plan.starts[r + 1] if r + 1 < p else spans[-1][1]
        for k in range(3):
            first = lo + k * plan.unit
            for t, (x, y) in enumerate(spans):
                x, y = max(x, first), min(y, hi, first + plan.unit)
                if x < y:
                    src = w_refs[k].at[pl.ds(r * plan.unit + x - first, y - x)]
                    dst = outs[t].at[pl.ds(x - spans[t][0], y - x)]
                    copies.append(pltpu.make_async_copy(src, dst, out_sem.at[len(copies)]))
    for c in copies:
        c.start()
    for c in copies:
        c.wait()


def restore(plan, gathered, shapes):
    n = len(plan.big)
    dma = pltpu.SemaphoreType.DMA
    outs = pl.pallas_call(
        functools.partial(restore_kernel, plan),
        out_shape=[jax.ShapeDtypeStruct((rows, LANES), BF) for rows, _, _ in plan.big]
        + [jax.ShapeDtypeStruct((small_rows(plan), LANES), BF)],
        in_specs=[ANY] * 3,
        out_specs=[ANY] * (n + 1),
        scratch_shapes=[dma((3 * plan.p + n + 1,))],
        compiler_params=pltpu.CompilerParams(vmem_limit_bytes=1 << 20),
        name="restore",
    )(*gathered)
    result = [from_stored(x, nj, s) for x, (_, nj, _), s in zip(outs, plan.big, shapes)]
    small = outs[n].reshape(-1, 2, LANES)
    for (row, nj), s in zip(plan.pairs(), shapes[n:]):
        result.append(small[row // 2:row // 2 + nj].transpose(1, 0, 2).reshape(s))
    return tuple(result)


def adam_update(g, m, v, w, lr, beta1, beta2, eps, step):
    t = step.astype(jnp.float32)
    m_new = beta1 * m + (1.0 - beta1) * g
    v_new = beta2 * v + (1.0 - beta2) * (g * g)
    m_hat = m_new / (1.0 - beta1 ** t)
    v_hat = v_new / (1.0 - beta2 ** t)
    w_new = w - lr * m_hat / (jnp.sqrt(v_hat) + eps)
    return m_new, v_new, w_new


def solution(mesh):
    p = mesh.shape["outer"] * mesh.shape["inner"]

    def body(g_emb, g_qkv, g_o, g_w1, g_w2, g_bqkv, g_b1, g_dvec, m, v, w, lr, beta1, beta2, eps, step):
        grads = (g_emb, g_qkv, g_o, g_w1, g_w2, g_bqkv, g_b1, g_dvec)
        shapes = tuple(x.shape[1:] for x in grads)
        plan = Plan(shapes, p)
        n = len(plan.big)
        stored = [as_stored(x, nj) for x, (_, nj, _) in zip(grads, plan.big)]
        small = jnp.concatenate([x.reshape(2, -1, LANES).transpose(1, 0, 2) for x in grads[n:]], axis=0)
        small = jnp.pad(small, ((0, plan.small_rows // 2 - small.shape[0]), (0, 0), (0, 0)))
        stored.append(small.reshape(-1, LANES))
        total = reduce_scatter(plan, stored).reshape(-1)
        r = lax.axis_index(AXES)
        offset = r * plan.shard - plan.start(r) * LANES
        g = lax.dynamic_slice(total, (offset,), (plan.shard,)) / p
        m_new, v_new, w_new = adam_update(g, m, v, w, lr, beta1, beta2, eps, step)
        front = max(i * plan.shard - plan.starts[i] * LANES for i in range(p))
        back = plan.window * LANES - plan.shard
        win = lax.dynamic_slice(jnp.pad(w_new, (front, back)), (front - offset,), (plan.window * LANES,))
        wb = all_gather(plan, win.reshape(plan.window, LANES))
        return (m_new, v_new, w_new) + restore(plan, wb, shapes)

    g3 = P(AXES, None, None)
    g4 = P(AXES, None, None, None)
    flat = P(AXES)
    rep = P()
    in_specs = (g3, g4, g4, g4, g4, g3, g3, g4, flat, flat, flat, rep, rep, rep, rep, rep)
    out_specs = (flat, flat, flat, rep, rep, rep, rep, rep, rep, rep, rep)
    return jax.shard_map(body, mesh=mesh, in_specs=in_specs, out_specs=out_specs, check_vma=False)
```

```python
import functools
import math

import jax
import jax.numpy as jnp
from jax import lax
from jax.experimental import pallas as pl
from jax.experimental.pallas import tpu as pltpu
from jax.sharding import PartitionSpec as P

AXES = ("outer", "inner")
MESH = pl.DeviceIdType.MESH
ANY = pl.BlockSpec(memory_space=pl.ANY)
LANES = 128
TILE = 16
SPLIT = 2
DEEP = 2
LEAD = 6
BF = jnp.bfloat16
F32 = jnp.float32


class Plan:
    def __init__(self, shapes, p):
        self.p = p
        self.sizes = [math.prod(s) for s in shapes]
        self.total = sum(self.sizes)
        self.shard = self.total // p
        self.big = []
        start = 0
        for s, n in zip(shapes, self.sizes):
            if s[-2] % TILE == 0:
                self.big.append((n // LANES, s[-1] // LANES, start // LANES))
                start += n
        self.small_row = start // LANES
        self.small_size = self.total - start
        self.starts, need = [], 0
        for r in range(p):
            self.starts.append(self.group(r * self.shard // LANES)[0])
            low, size = self.group(((r + 1) * self.shard - 1) // LANES)
            need = max(need, low + size - self.starts[r])
        self.part = -(-need // (3 * SPLIT * TILE)) * TILE
        self.unit = SPLIT * self.part
        self.window = 3 * self.unit
        self.small_rows = self.starts[p - 1] + self.window - self.small_row

    def group(self, row):
        for n, nj, flat in self.big:
            if flat <= row < flat + n:
                size = 8 * nj
                return flat + (row - flat) // size * size, size
        return self.small_row + (row - self.small_row) // TILE * TILE, TILE

    def spans(self):
        spans = [(flat, flat + n) for n, _, flat in self.big]
        return spans + [(self.small_row, self.small_row + self.small_rows)]

    def crossing(self):
        out = {}
        for start in self.starts:
            for lo in range(start, start + self.window, self.part):
                cuts = []
                for t, (x, y) in enumerate(self.spans()):
                    x, y = max(x, lo), min(y, lo + self.part)
                    if x < y:
                        cuts.append((t, x - self.spans()[t][0], y - x, x - lo))
                if len(cuts) > 1:
                    out[lo] = cuts
        return out

    def start(self, r):
        row = jnp.int32(self.starts[0])
        for i in range(1, self.p):
            row = jnp.where(r == i, jnp.int32(self.starts[i]), row)
        return row

    def segments(self, first):
        out = []
        for n, nj, flat in self.big:
            lo = jnp.maximum(first, flat)
            hi = jnp.minimum(first + self.window, flat + n)
            out.append((nj, lo - first, lax.div(jnp.maximum(hi - lo, 0), 8 * nj)))
        return out

    def pairs(self):
        flat, row, kept = [], 0, 0
        for n in self.sizes[len(self.big):]:
            flat.append((row, n // (2 * LANES)))
            row += n // LANES
        out = []
        for at, nj in flat[1:] + flat[:1]:
            out.append((at, kept, nj))
            kept += 2 * nj
        return out[-1:] + out[:-1]


def as_stored(x, nj):
    return x.reshape(-1, 8, nj, LANES).transpose(0, 2, 1, 3).reshape(-1, LANES)


def from_stored(x, nj, shape):
    return x.reshape(-1, nj, 8, LANES).transpose(0, 2, 1, 3).reshape(shape)


class Place:
    def __init__(self):
        o, i = lax.axis_index("outer"), lax.axis_index("inner")
        self.bits = [lax.div(o, 2), lax.rem(o, 2), lax.div(i, 2)]
        self.core = lax.rem(i, 2)

    def flipped(self, d):
        b = list(self.bits)
        b[d] = 1 - b[d]
        return (b[0] * 2 + b[1], b[2] * 2 + self.core)

    def partner(self):
        return (self.bits[0] * 2 + self.bits[1], self.bits[2] * 2 + 1 - self.core)

    def neighbour(self, k, n):
        d = lax.rem(k + n, 3)
        b = [jnp.where(d == i, 1 - x, x) for i, x in enumerate(self.bits)]
        return (b[0] * 2 + b[1], b[2] * 2 + self.core)

    def part(self, i):
        return lax.div(i, 3 * SPLIT), lax.rem(i, 3), lax.rem(i, 3 * SPLIT)

    def block(self, a, k, core):
        e = [1 - lax.div(a, 4), 1 - lax.rem(lax.div(a, 2), 2), 1 - lax.rem(a, 2)]
        r = core
        for d, weight in enumerate((8, 4, 2)):
            j = lax.rem(d - k + 3, 3)
            flip = jnp.where(j == 0, e[0], jnp.where(j == 1, e[1], e[2]))
            r = r + weight * (self.bits[d] + flip - 2 * self.bits[d] * flip)
        return r

    def owner(self, dims, e, core):
        b = list(self.bits)
        for d, flip in zip(dims, e):
            if flip:
                b[d] = 1 - b[d]
        return b[0] * 8 + b[1] * 4 + b[2] * 2 + core


def dims_of(k):
    return (k, (k + 1) % 3, (k + 2) % 3)


def arrive(place):
    barrier = pltpu.get_barrier_semaphore()
    for peer in [place.partner()] + [place.flipped(d) for d in range(3)]:
        pl.semaphore_signal(barrier, inc=1, device_id=peer, device_id_type=MESH)


def meet():
    pl.semaphore_wait(pltpu.get_barrier_semaphore(), 4)


def remote(src, dst, send, recv, dev):
    return pltpu.make_async_remote_copy(
        src_ref=src, dst_ref=dst, send_sem=send, recv_sem=recv, device_id=dev, device_id_type=MESH
    )


def rs_kernel(plan, *refs):
    n_big = len(plan.big)
    n_in = n_big + len(plan.pairs())
    flat, late_ref = refs[n_in:n_in + 2]
    early, r1, r2, r3, own, oth, small, odd = refs[n_in + 2:n_in + 10]
    own_sem, oth_sem, d_send, d_recv, s1_send, s1_recv, s2_send, s2_recv, s3_send, s3_recv, tiny_sem = refs[n_in + 10:]
    xs = refs[:n_big] + (small,)
    part = plan.part
    wave = 3 * SPLIT
    early_n = 4 * wave
    place = Place()
    partner = place.partner()
    crossing = plan.crossing()

    def pick(i, core, issue):
        a, k, at = place.part(i)
        row = plan.start(place.block(a, k, core)) + at * part
        for t, (lo, hi) in enumerate(plan.spans()):

            @pl.when((row >= lo) & (row <= hi - part))
            def _(t=t, lo=lo):
                issue(xs[t].at[pl.ds(pl.multiple_of(row - lo, TILE), part)], 0, part)

        for first, cuts in crossing.items():

            @pl.when(row == first)
            def _(cuts=cuts):
                for t, at, size, to in cuts:
                    issue(xs[t].at[pl.ds(at, size)], to, size)

    def swap(i):
        slot = i

        def issue(src, at, size):
            remote(src, early.at[slot, pl.ds(at, size)], d_send.at[slot], d_recv.at[slot], partner).start()

        pick(i, 1 - place.core, issue)

    def swap_late(i):
        slot = i

        def issue(src, at, size):
            remote(
                src, late_ref.at[slot, pl.ds(at, size)], d_send.at[early_n + slot], d_recv.at[early_n + slot], partner
            ).start()

        pick(early_n + i, 1 - place.core, issue)

    def swapped(slot):
        return remote(early.at[slot], early.at[slot], d_send.at[slot], d_recv.at[slot], partner)

    def swapped_late(slot):
        sems = d_send.at[early_n + slot], d_recv.at[early_n + slot]
        return remote(late_ref.at[slot], late_ref.at[slot], *sems, partner)

    def load(i):
        to = lax.rem(i, DEEP)

        def issue(src, at, size):
            pltpu.make_async_copy(src, own.at[to, pl.ds(at, size)], own_sem.at[to]).start()

        pick(i, place.core, issue)

    def loaded(i):
        to = lax.rem(i, DEEP)
        return pltpu.make_async_copy(late_ref.at[0], own.at[to], own_sem.at[to])

    def fetch(i):
        to = lax.rem(i, DEEP)
        return pltpu.make_async_copy(late_ref.at[i], oth.at[to], oth_sem.at[to])

    def hop(stage, k, slot):
        src, dst, send, recv, base = (
            (early, r1, s1_send, s1_recv, 0),
            (r1, r2, s2_send, s2_recv, 0),
            (r1, r3, s3_send, s3_recv, 2 * wave),
        )[stage]
        return remote(src.at[base + slot], dst.at[slot], send.at[slot], recv.at[slot], place.neighbour(k, stage))

    def add(dst, *srcs):
        step = 48

        def body(i, _):
            rows = pl.ds(pl.multiple_of(i * step, TILE), step)
            total = dst[rows, :]
            for s in srcs:
                total = total + s[rows, :]
            dst[rows, :] = total
            return 0

        lax.fori_loop(0, part // step, body, 0)

    def loop(count, f):
        def body(i, _):
            f(i)
            return 0

        lax.fori_loop(0, count, body, 0)

    arrive(place)
    copies = []
    for m, (x, (_, kept, nj)) in enumerate(zip(refs[n_big:n_in], plan.pairs())):
        dst = odd if m == 0 else small.at[pl.ds(kept, 2 * nj)]
        copies.append(pltpu.make_async_copy(x, dst, tiny_sem.at[m]))
        copies[-1].start()
    end = plan.small_size // LANES
    small[end:, :] = jnp.zeros((plan.small_rows - end, LANES), F32)
    for c in copies:
        c.wait()
    _, kept, nj = plan.pairs()[0]
    for j in range(nj):
        small[kept + 2 * j:kept + 2 * j + 2, :] = odd[:, j * LANES:(j + 1) * LANES]
    loop(DEEP, load)
    meet()
    loop(LEAD, swap)

    def first(i):
        k, slot = lax.rem(i, 3), i

        @pl.when(i + LEAD < early_n)
        def _():
            swap(i + LEAD)

        @pl.when(i + LEAD >= early_n)
        def _():
            swap_late(i + LEAD - early_n)

        loaded(i).wait()
        swapped(slot).wait_recv()
        add(early.at[slot], own.at[lax.rem(i, DEEP)])
        hop(0, k, slot).start()
        load(i + DEEP)

    loop(early_n, first)

    def prefetch(i):
        swapped_late(i).wait_recv()
        fetch(i).start()

    loop(DEEP, prefetch)

    def second(i):
        k, slot = lax.rem(i, 3), i

        @pl.when(i + LEAD < early_n)
        def _():
            swap_late(i + LEAD)

        to = lax.rem(i, DEEP)
        loaded(i).wait()
        fetch(i).wait()
        hop(0, k, slot).wait_recv()
        add(r1.at[slot], own.at[to], oth.at[to])

        @pl.when(i < 2 * wave)
        def _():
            hop(1, k, slot).start()

        @pl.when(i + DEEP < early_n)
        def _():
            load(early_n + i + DEEP)
            prefetch(i + DEEP)

    loop(early_n, second)

    def third(i):
        k, slot = lax.rem(i, 3), i
        hop(1, k, slot).wait_recv()
        add(r1.at[2 * wave + slot], r2.at[slot])

        @pl.when(i < wave)
        def _():
            hop(2, k, slot).start()

    loop(2 * wave, third)

    def fourth(i):
        k, slot = lax.rem(i, 3), i
        hop(2, k, slot).wait_recv()
        add(r1.at[3 * wave + slot], r3.at[slot])

    loop(wave, fourth)

    me = place.owner(dims_of(0), (0, 0, 0), place.core)
    stored = r1.at[pl.ds(3 * wave, wave)].reshape(plan.window, LANES)
    for nj, row, groups in plan.segments(plan.start(me)):

        def sort(i, nj=nj, row=row):
            base = pl.multiple_of(row + i * 8 * nj, TILE)
            for j in range(nj):
                flat[pl.ds(base + j, 8, stride=nj), :] = stored[pl.ds(base + j * 8, 8), :]

        loop(groups, sort)

    @pl.when(me == plan.p - 1)
    def _():
        base = plan.small_row - plan.starts[plan.p - 1]
        for row, kept, nj in plan.pairs():
            for layer in range(2):
                flat[pl.ds(base + row + layer * nj, nj), :] = stored[pl.ds(base + kept + layer, nj, stride=2), :]

    def sent(i):
        k, slot = lax.rem(i, 3), i
        swapped(slot).wait_send()
        swapped_late(slot).wait_send()
        hop(0, k, slot).wait_send()

        @pl.when(i < 2 * wave)
        def _():
            hop(1, k, slot).wait_send()

        @pl.when(i < wave)
        def _():
            hop(2, k, slot).wait_send()

    loop(early_n, sent)


def reduce_scatter(plan, xs):
    dma = pltpu.SemaphoreType.DMA
    wave = 3 * SPLIT
    slots = [4 * wave, 4 * wave, 2 * wave, wave, DEEP, DEEP]
    used = (sum(slots) * plan.part * LANES * 4 >> 20) + 2
    g, _ = pl.pallas_call(
        functools.partial(rs_kernel, plan),
        out_shape=(
            pltpu.VMEM((plan.window, LANES), F32),
            jax.ShapeDtypeStruct((4 * wave, plan.part, LANES), F32),
        ),
        in_specs=[ANY] * len(xs),
        out_specs=(pl.BlockSpec(memory_space=pltpu.VMEM), ANY),
        scratch_shapes=[pltpu.VMEM((n, plan.part, LANES), F32) for n in slots]
        + [pltpu.VMEM((plan.small_rows, LANES), F32), pltpu.VMEM(xs[len(plan.big)].shape, F32)]
        + [dma((DEEP,)), dma((DEEP,))]
        + [dma((n * wave,)) for n in (8, 8, 4, 4, 2, 2, 1, 1)]
        + [dma((len(plan.pairs()),))],
        compiler_params=pltpu.CompilerParams(
            collective_id=0, has_side_effects=True, vmem_limit_bytes=used << 20
        ),
        name="reduce_scatter",
    )(*xs)
    return g


def ag_kernel(plan, values, *refs):
    w_refs, (win, tiny, s_send, s_recv, d_send, d_recv) = refs[:3], refs[3:]
    part, unit = plan.part, plan.unit
    place = Place()
    partner = place.partner()
    here = (0, 0, 0)
    me = place.owner(dims_of(0), here, place.core)
    arrive(place)

    for nj, row, groups in plan.segments(plan.start(me)):

        def sort(i, _, nj=nj, row=row):
            base = pl.multiple_of(row + i * 8 * nj, TILE)
            for j in range(0, nj, 2):
                pair = [values[pl.ds(base + j + h, 8, stride=nj), :] for h in range(2)]
                win[pl.ds(base + j * 8, TILE), :] = jnp.concatenate(pair, axis=0).astype(BF)
            return 0

        lax.fori_loop(0, groups, sort, 0)

    @pl.when(me == plan.p - 1)
    def _():
        base = plan.small_row - plan.starts[plan.p - 1]
        tiny[...] = jnp.zeros_like(tiny)
        for row, kept, nj in plan.pairs():
            for layer in range(2):
                tiny[pl.ds(kept + layer, nj, stride=2), :] = values[pl.ds(base + row + layer * nj, nj), :]
        win[pl.ds(base, tiny.shape[0]), :] = tiny[...].astype(BF)

    def rows_of(k, e, s, core):
        row = place.owner(dims_of(k), e, core) * unit + s * part
        return w_refs[k].at[pl.ds(pl.multiple_of(row, TILE), part)]

    slot = {here: 0, (1, 0, 0): 1, (0, 1, 0): 2, (0, 0, 1): 3, (1, 1, 0): 4, (1, 0, 1): 5, (0, 1, 1): 6, (1, 1, 1): 7}

    def index(k, e, s):
        return (slot[e] * 3 + k) * SPLIT + s

    def src(k, e, s):
        return win.at[pl.ds((3 * s + k) * part, part)] if e == here else rows_of(k, e, s, place.core)

    sent = []

    def send(k, e, s, n):
        there = list(e)
        there[n] = 1
        i = index(k, tuple(there), s)
        copy = remote(
            src(k, e, s), rows_of(k, e, s, place.core), s_send.at[i], s_recv.at[i], place.flipped(dims_of(k)[n])
        )
        copy.start()
        sent.append(copy)

    def share(k, e, s):
        i = index(k, e, s)
        copy = remote(src(k, e, s), rows_of(k, e, s, place.core), d_send.at[i], d_recv.at[i], partner)
        copy.start()
        sent.append(copy)

    def arrival(k, e, s):
        i, dst = index(k, e, s), rows_of(k, e, s, place.core)
        return remote(dst, dst, s_send.at[i], s_recv.at[i], partner)

    def shared(k, e, s):
        i, dst = index(k, e, s), rows_of(k, e, s, 1 - place.core)
        return remote(dst, dst, d_send.at[i], d_recv.at[i], partner)

    meet()
    for n in range(3):
        for s in range(SPLIT):
            for k in range(3):
                send(k, here, s, n)
    for s in range(SPLIT):
        for k in range(3):
            share(k, here, s)
    rows = 3 * TILE
    for s in range(SPLIT):
        for k in range(3):

            def keep(i, _, k=k, s=s):
                at = pl.multiple_of(i * rows, rows)
                to = pl.ds(pl.multiple_of(me * unit + s * part + at, TILE), rows)
                w_refs[k][to, :] = win[pl.ds((3 * s + k) * part + at, rows), :]
                return 0

            lax.fori_loop(0, part // rows, keep, 0)
    for e in list(slot)[1:]:
        for s in range(SPLIT):
            for k in range(3):
                arrival(k, e, s).wait_recv()
                for n in range(1, 3):
                    if not any(e[n:]):
                        send(k, e, s, n)
                share(k, e, s)
    for e in slot:
        for s in range(SPLIT):
            for k in range(3):
                shared(k, e, s).wait_recv()
    for copy in sent:
        copy.wait_send()

    for r in range(1, plan.p):
        size = plan.group(plan.starts[r])[1]
        nj, shape = size // 8, (size, LANES)
        row, lane = lax.broadcasted_iota(jnp.int32, shape, 0), lax.broadcasted_iota(jnp.int32, shape, 1)
        at = (lax.rem(row, 8) * nj + lax.div(row, 8)) * LANES + lane
        cut = r * plan.shard - plan.starts[r] * LANES
        gap = plan.starts[r] - plan.starts[r - 1] - plan.window
        before = w_refs[2][pl.ds(r * unit + gap, size), :]
        rows = pl.ds(r * unit, size)
        w_refs[0][rows, :] = jnp.where(at < cut, before.astype(F32), w_refs[0][rows, :].astype(F32)).astype(BF)


def all_gather(plan, win):
    dma = pltpu.SemaphoreType.DMA
    n = 8 * 3 * SPLIT
    return pl.pallas_call(
        functools.partial(ag_kernel, plan),
        out_shape=[pltpu.VMEM((plan.p * plan.unit, LANES), BF)] * 3,
        in_specs=[pl.BlockSpec(memory_space=pltpu.VMEM)],
        out_specs=[pl.BlockSpec(memory_space=pltpu.VMEM)] * 3,
        scratch_shapes=[pltpu.VMEM((plan.window, LANES), BF), pltpu.VMEM((small_rows(plan), LANES), F32)]
        + [dma((n,))] * 4,
        compiler_params=pltpu.CompilerParams(collective_id=1, has_side_effects=True, vmem_limit_bytes=8 << 20),
        name="all_gather",
    )(win)


def small_rows(plan):
    return -(-plan.small_size // (LANES * TILE)) * TILE


def restore_kernel(plan, *refs):
    w_refs, outs, out_sem = refs[:3], refs[3:-1], refs[-1]
    p, part = plan.p, plan.part
    copies = []

    def copy(r, x, y, dst):
        for n in range(x // part, -(-y // part)):
            lo, hi = max(x, n * part), min(y, (n + 1) * part)
            src = w_refs[n % 3].at[pl.ds(r * plan.unit + n // 3 * part + lo - n * part, hi - lo)]
            copies.append(pltpu.make_async_copy(src, dst(lo - x, hi - lo), out_sem.at[len(copies)]))

    for r in range(p):
        lo = plan.starts[r]
        hi = plan.starts[r + 1] if r + 1 < p else plan.small_row
        for t, (a, b) in enumerate(plan.spans()[:-1]):
            x, y = max(a, lo), min(b, hi)
            if x < y:
                copy(r, x - lo, y - lo, lambda at, size, t=t, x=x, a=a: outs[t].at[pl.ds(x - a + at, size)])
    base = plan.small_row - plan.starts[p - 1]
    for out, (_, kept, nj) in zip(outs[len(plan.big):], plan.pairs()):
        copy(p - 1, base + kept, base + kept + out.shape[0], lambda at, size, out=out: out.at[pl.ds(at, size)])
    for c in copies:
        c.start()
    for c in copies:
        c.wait()


def restore(plan, gathered, shapes):
    n = len(plan.big)
    dma = pltpu.SemaphoreType.DMA
    outs = pl.pallas_call(
        functools.partial(restore_kernel, plan),
        out_shape=[jax.ShapeDtypeStruct((rows, LANES), BF) for rows, _, _ in plan.big]
        + [jax.ShapeDtypeStruct((2 * nj if m else -(-2 * nj // TILE) * TILE, LANES), BF)
           for m, (_, _, nj) in enumerate(plan.pairs())],
        in_specs=[ANY] * 3,
        out_specs=[ANY] * len(shapes),
        scratch_shapes=[dma((3 * SPLIT * plan.p + 3 * n,))],
        compiler_params=pltpu.CompilerParams(vmem_limit_bytes=1 << 20),
        name="restore",
    )(*gathered)
    result = [from_stored(x, nj, s) for x, (_, nj, _), s in zip(outs, plan.big, shapes)]
    for x, (_, _, nj), s in zip(outs[n:], plan.pairs(), shapes[n:]):
        result.append(x[:2 * nj].reshape(nj, 2, LANES).transpose(1, 0, 2).reshape(s))
    return tuple(result)


def adam_update(g, m, v, w, lr, beta1, beta2, eps, step):
    t = step.astype(jnp.float32)
    m_new = beta1 * m + (1.0 - beta1) * g
    v_new = beta2 * v + (1.0 - beta2) * (g * g)
    m_hat = m_new / (1.0 - beta1 ** t)
    v_hat = v_new / (1.0 - beta2 ** t)
    w_new = w - lr * m_hat / (jnp.sqrt(v_hat) + eps)
    return m_new, v_new, w_new


def solution(mesh):
    p = mesh.shape["outer"] * mesh.shape["inner"]

    def body(g_emb, g_qkv, g_o, g_w1, g_w2, g_bqkv, g_b1, g_dvec, m, v, w, lr, beta1, beta2, eps, step):
        grads = (g_emb, g_qkv, g_o, g_w1, g_w2, g_bqkv, g_b1, g_dvec)
        shapes = tuple(x.shape[1:] for x in grads)
        plan = Plan(shapes, p)
        n = len(plan.big)
        stored = [as_stored(x, nj) for x, (_, nj, _) in zip(grads, plan.big)]
        stored.append(grads[n].reshape(shapes[n]))
        stored += [x.reshape(2, -1, LANES).transpose(1, 0, 2).reshape(-1, LANES) for x in grads[n + 1:]]
        total = reduce_scatter(plan, stored).reshape(-1)
        r = lax.axis_index(AXES)
        offset = r * plan.shard - plan.start(r) * LANES
        g = lax.dynamic_slice(total, (offset,), (plan.shard,)) / p
        m_new, v_new, w_new = adam_update(g, m, v, w, lr, beta1, beta2, eps, step)
        front = max(i * plan.shard - plan.starts[i] * LANES for i in range(p))
        back = plan.window * LANES - plan.shard
        win = lax.dynamic_slice(jnp.pad(w_new, (front, back)), (front - offset,), (plan.window * LANES,))
        wb = all_gather(plan, win.reshape(plan.window, LANES))
        return (m_new, v_new, w_new) + restore(plan, wb, shapes)

    g3 = P(AXES, None, None)
    g4 = P(AXES, None, None, None)
    flat = P(AXES)
    rep = P()
    in_specs = (g3, g4, g4, g4, g4, g3, g3, g4, flat, flat, flat, rep, rep, rep, rep, rep)
    out_specs = (flat, flat, flat, rep, rep, rep, rep, rep, rep, rep, rep)
    return jax.shard_map(body, mesh=mesh, in_specs=in_specs, out_specs=out_specs, check_vma=False)
```

```python
import functools
import math

import jax
import jax.numpy as jnp
from jax import lax
from jax.experimental import pallas as pl
from jax.experimental.pallas import tpu as pltpu
from jax.sharding import PartitionSpec as P

AXES = ("outer", "inner")
MESH = pl.DeviceIdType.MESH
ANY = pl.BlockSpec(memory_space=pl.ANY)
LANES = 128
TILE = 16
SPLIT = 4
HALVES = 2
DEEP = 4
LEAD = 12
BF = jnp.bfloat16
F32 = jnp.float32


class Plan:
    def __init__(self, shapes, p):
        self.p = p
        self.sizes = [math.prod(s) for s in shapes]
        self.total = sum(self.sizes)
        self.shard = self.total // p
        self.big = []
        start = 0
        for s, n in zip(shapes, self.sizes):
            if s[-2] % TILE == 0:
                self.big.append((n // LANES, s[-1] // LANES, start // LANES))
                start += n
        self.small_row = start // LANES
        self.small_size = self.total - start
        self.starts, need = [], 0
        for r in range(p):
            self.starts.append(self.group(r * self.shard // LANES)[0])
            low, size = self.group(((r + 1) * self.shard - 1) // LANES)
            need = max(need, low + size - self.starts[r])
        self.part = -(-need // (3 * SPLIT * TILE)) * TILE
        self.unit = SPLIT * self.part
        self.window = 3 * self.unit
        self.piece = self.unit // HALVES
        self.small_rows = self.starts[p - 1] + self.window - self.small_row

    def group(self, row):
        for n, nj, flat in self.big:
            if flat <= row < flat + n:
                size = 8 * nj
                return flat + (row - flat) // size * size, size
        return self.small_row + (row - self.small_row) // TILE * TILE, TILE

    def spans(self):
        spans = [(flat, flat + n) for n, _, flat in self.big]
        return spans + [(self.small_row, self.small_row + self.small_rows)]

    def crossing(self):
        out = {}
        for start in self.starts:
            for lo in range(start, start + self.window, self.part):
                cuts = []
                for t, (x, y) in enumerate(self.spans()):
                    x, y = max(x, lo), min(y, lo + self.part)
                    if x < y:
                        cuts.append((t, x - self.spans()[t][0], y - x, x - lo))
                if len(cuts) > 1:
                    out[lo] = cuts
        return out

    def start(self, r):
        row = jnp.int32(self.starts[0])
        for i in range(1, self.p):
            row = jnp.where(r == i, jnp.int32(self.starts[i]), row)
        return row

    def segments(self, first):
        out = []
        for n, nj, flat in self.big:
            lo = jnp.maximum(first, flat)
            hi = jnp.minimum(first + self.window, flat + n)
            out.append((nj, lo - first, lax.div(jnp.maximum(hi - lo, 0), 8 * nj)))
        return out

    def sort(self, first, lo, hi, spill, move):
        for nj, row, groups in self.segments(first):
            size = 8 * nj
            more = size - 1 if spill else 0
            done, todo = [
                jnp.minimum(groups, lax.div(jnp.maximum(x - row, 0) + more, size)) if x else 0 for x in (lo, hi)
            ]

            def body(i, _, nj=nj, row=row, done=done, size=size):
                move(nj, pl.multiple_of(row + (done + i) * size, TILE))
                return 0

            lax.fori_loop(0, todo - done, body, 0)

    def pairs(self):
        flat, row, kept = [], 0, 0
        for n in self.sizes[len(self.big):]:
            flat.append((row, n // (2 * LANES)))
            row += n // LANES
        out = []
        for at, nj in flat[1:] + flat[:1]:
            out.append((at, kept, nj))
            kept += 2 * nj
        return out[-1:] + out[:-1]


def as_stored(x, nj):
    return x.reshape(-1, 8, nj, LANES).transpose(0, 2, 1, 3).reshape(-1, LANES)


def from_stored(x, nj, shape):
    return x.reshape(-1, nj, 8, LANES).transpose(0, 2, 1, 3).reshape(shape)


class Place:
    def __init__(self):
        o, i = lax.axis_index("outer"), lax.axis_index("inner")
        self.bits = [lax.div(o, 2), lax.rem(o, 2), lax.div(i, 2)]
        self.core = lax.rem(i, 2)

    def flipped(self, d):
        b = list(self.bits)
        b[d] = 1 - b[d]
        return (b[0] * 2 + b[1], b[2] * 2 + self.core)

    def partner(self):
        return (self.bits[0] * 2 + self.bits[1], self.bits[2] * 2 + 1 - self.core)

    def neighbour(self, k, n):
        d = lax.rem(k + n, 3)
        b = [jnp.where(d == i, 1 - x, x) for i, x in enumerate(self.bits)]
        return (b[0] * 2 + b[1], b[2] * 2 + self.core)

    def part(self, i):
        return lax.div(i, 3 * SPLIT), lax.rem(i, 3), lax.rem(i, 3 * SPLIT)

    def block(self, a, k, core):
        e = [1 - lax.div(a, 4), 1 - lax.rem(lax.div(a, 2), 2), 1 - lax.rem(a, 2)]
        r = core
        for d, weight in enumerate((8, 4, 2)):
            j = lax.rem(d - k + 3, 3)
            flip = jnp.where(j == 0, e[0], jnp.where(j == 1, e[1], e[2]))
            r = r + weight * (self.bits[d] + flip - 2 * self.bits[d] * flip)
        return r

    def owner(self, dims, e, core):
        b = list(self.bits)
        for d, flip in zip(dims, e):
            if flip:
                b[d] = 1 - b[d]
        return b[0] * 8 + b[1] * 4 + b[2] * 2 + core


def dims_of(k):
    return (k, (k + 1) % 3, (k + 2) % 3)


def arrive(place):
    barrier = pltpu.get_barrier_semaphore()
    for peer in [place.partner()] + [place.flipped(d) for d in range(3)]:
        pl.semaphore_signal(barrier, inc=1, device_id=peer, device_id_type=MESH)


def meet():
    pl.semaphore_wait(pltpu.get_barrier_semaphore(), 4)


def remote(src, dst, send, recv, dev):
    return pltpu.make_async_remote_copy(
        src_ref=src, dst_ref=dst, send_sem=send, recv_sem=recv, device_id=dev, device_id_type=MESH
    )


def rs_kernel(plan, *refs):
    n_big = len(plan.big)
    n_in = n_big + len(plan.pairs())
    flat, late_ref = refs[n_in:n_in + 2]
    early, r1, r2, r3, own, oth, small, odd = refs[n_in + 2:n_in + 10]
    own_sem, oth_sem, d_send, d_recv, s1_send, s1_recv, s2_send, s2_recv, s3_send, s3_recv, tiny_sem = refs[n_in + 10:]
    xs = refs[:n_big] + (small,)
    part = plan.part
    wave = 3 * SPLIT
    early_n = 4 * wave
    place = Place()
    partner = place.partner()
    crossing = plan.crossing()

    def pick(i, core, issue):
        a, k, at = place.part(i)
        row = plan.start(place.block(a, k, core)) + at * part
        for t, (lo, hi) in enumerate(plan.spans()):

            @pl.when((row >= lo) & (row <= hi - part))
            def _(t=t, lo=lo):
                issue(xs[t].at[pl.ds(pl.multiple_of(row - lo, TILE), part)], 0, part)

        for first, cuts in crossing.items():

            @pl.when(row == first)
            def _(cuts=cuts):
                for t, at, size, to in cuts:
                    issue(xs[t].at[pl.ds(at, size)], to, size)

    def swap(i):
        slot = i

        def issue(src, at, size):
            remote(src, early.at[slot, pl.ds(at, size)], d_send.at[slot], d_recv.at[slot], partner).start()

        pick(i, 1 - place.core, issue)

    def swap_late(i):
        slot = i

        def issue(src, at, size):
            remote(
                src, late_ref.at[slot, pl.ds(at, size)], d_send.at[early_n + slot], d_recv.at[early_n + slot], partner
            ).start()

        pick(early_n + i, 1 - place.core, issue)

    def swapped(slot):
        return remote(early.at[slot], early.at[slot], d_send.at[slot], d_recv.at[slot], partner)

    def swapped_late(slot):
        sems = d_send.at[early_n + slot], d_recv.at[early_n + slot]
        return remote(late_ref.at[slot], late_ref.at[slot], *sems, partner)

    def load(i):
        to = lax.rem(i, DEEP)

        def issue(src, at, size):
            pltpu.make_async_copy(src, own.at[to, pl.ds(at, size)], own_sem.at[to]).start()

        pick(i, place.core, issue)

    def loaded(i):
        to = lax.rem(i, DEEP)
        return pltpu.make_async_copy(late_ref.at[0], own.at[to], own_sem.at[to])

    def fetch(i):
        to = lax.rem(i, DEEP)
        return pltpu.make_async_copy(late_ref.at[i], oth.at[to], oth_sem.at[to])

    def hop(stage, k, slot):
        src, dst, send, recv, base = (
            (early, r1, s1_send, s1_recv, 0),
            (r1, r2, s2_send, s2_recv, 0),
            (r1, r3, s3_send, s3_recv, 2 * wave),
        )[stage]
        return remote(src.at[base + slot], dst.at[slot], send.at[slot], recv.at[slot], place.neighbour(k, stage))

    def add(dst, *srcs):
        step = 48

        def body(i, _):
            rows = pl.ds(pl.multiple_of(i * step, TILE), step)
            total = dst[rows, :]
            for s in srcs:
                total = total + s[rows, :]
            dst[rows, :] = total
            return 0

        lax.fori_loop(0, part // step, body, 0)

    def loop(count, f):
        def body(i, _):
            f(i)
            return 0

        lax.fori_loop(0, count, body, 0)

    arrive(place)
    copies = []
    for m, (x, (_, kept, nj)) in enumerate(zip(refs[n_big:n_in], plan.pairs())):
        dst = odd if m == 0 else small.at[pl.ds(kept, 2 * nj)]
        copies.append(pltpu.make_async_copy(x, dst, tiny_sem.at[m]))
        copies[-1].start()
    end = plan.small_size // LANES
    small[end:, :] = jnp.zeros((plan.small_rows - end, LANES), F32)
    for c in copies:
        c.wait()
    _, kept, nj = plan.pairs()[0]
    for j in range(nj):
        small[kept + 2 * j:kept + 2 * j + 2, :] = odd[:, j * LANES:(j + 1) * LANES]
    loop(DEEP, load)
    meet()
    loop(LEAD, swap)

    def first(i):
        k, slot = lax.rem(i, 3), i

        @pl.when(i + LEAD < early_n)
        def _():
            swap(i + LEAD)

        @pl.when(i + LEAD >= early_n)
        def _():
            swap_late(i + LEAD - early_n)

        loaded(i).wait()
        swapped(slot).wait_recv()
        add(early.at[slot], own.at[lax.rem(i, DEEP)])
        hop(0, k, slot).start()
        load(i + DEEP)

    loop(early_n, first)

    def prefetch(i):
        swapped_late(i).wait_recv()
        fetch(i).start()

    loop(DEEP, prefetch)

    def second(i):
        k, slot = lax.rem(i, 3), i

        @pl.when(i + LEAD < early_n)
        def _():
            swap_late(i + LEAD)

        to = lax.rem(i, DEEP)
        loaded(i).wait()
        fetch(i).wait()
        hop(0, k, slot).wait_recv()
        add(r1.at[slot], own.at[to], oth.at[to])

        @pl.when(i < 2 * wave)
        def _():
            hop(1, k, slot).start()

        @pl.when(i + DEEP < early_n)
        def _():
            load(early_n + i + DEEP)
            prefetch(i + DEEP)

    loop(early_n, second)

    def third(i):
        k, slot = lax.rem(i, 3), i
        hop(1, k, slot).wait_recv()
        add(r1.at[2 * wave + slot], r2.at[slot])

        @pl.when(i < wave)
        def _():
            hop(2, k, slot).start()

    loop(2 * wave, third)

    me = place.owner(dims_of(0), (0, 0, 0), place.core)
    first_row = plan.start(me)
    stored = r1.at[pl.ds(3 * wave, wave)].reshape(plan.window, LANES)

    def move(nj, base):
        for j in range(nj):
            flat[pl.ds(base + j, 8, stride=nj), :] = stored[pl.ds(base + j * 8, 8), :]

    for s in range(SPLIT):

        def fourth(j, s=s):
            slot = 3 * s + j
            hop(2, j, slot).wait_recv()
            add(r1.at[3 * wave + slot], r3.at[slot])

        loop(3, fourth)
        plan.sort(first_row, 3 * s * part, 3 * (s + 1) * part, False, move)

    @pl.when(me == plan.p - 1)
    def _():
        base = plan.small_row - plan.starts[plan.p - 1]
        for row, kept, nj in plan.pairs():
            for layer in range(2):
                flat[pl.ds(base + row + layer * nj, nj), :] = stored[pl.ds(base + kept + layer, nj, stride=2), :]

    def sent(i):
        k, slot = lax.rem(i, 3), i
        swapped(slot).wait_send()
        swapped_late(slot).wait_send()
        hop(0, k, slot).wait_send()

        @pl.when(i < 2 * wave)
        def _():
            hop(1, k, slot).wait_send()

        @pl.when(i < wave)
        def _():
            hop(2, k, slot).wait_send()

    loop(early_n, sent)


def reduce_scatter(plan, xs):
    dma = pltpu.SemaphoreType.DMA
    wave = 3 * SPLIT
    slots = [4 * wave, 4 * wave, 2 * wave, wave, DEEP, DEEP]
    used = (sum(slots) * plan.part * LANES * 4 >> 20) + 2
    g, _ = pl.pallas_call(
        functools.partial(rs_kernel, plan),
        out_shape=(
            pltpu.VMEM((plan.window, LANES), F32),
            jax.ShapeDtypeStruct((4 * wave, plan.part, LANES), F32),
        ),
        in_specs=[ANY] * len(xs),
        out_specs=(pl.BlockSpec(memory_space=pltpu.VMEM), ANY),
        scratch_shapes=[pltpu.VMEM((n, plan.part, LANES), F32) for n in slots]
        + [pltpu.VMEM((plan.small_rows, LANES), F32), pltpu.VMEM(xs[len(plan.big)].shape, F32)]
        + [dma((DEEP,)), dma((DEEP,))]
        + [dma((n * wave,)) for n in (8, 8, 4, 4, 2, 2, 1, 1)]
        + [dma((len(plan.pairs()),))],
        compiler_params=pltpu.CompilerParams(
            collective_id=0, has_side_effects=True, vmem_limit_bytes=used << 20
        ),
        name="reduce_scatter",
    )(*xs)
    return g


def ag_kernel(plan, values, *refs):
    w_refs, (win, tiny, s_send, s_recv, d_send, d_recv) = refs[:3], refs[3:]
    part, unit = plan.piece, plan.unit
    place = Place()
    partner = place.partner()
    here = (0, 0, 0)
    me = place.owner(dims_of(0), here, place.core)
    arrive(place)

    first_row = plan.start(me)

    def move(nj, base):
        for j in range(0, nj, 2):
            pair = [values[pl.ds(base + j + h, 8, stride=nj), :] for h in range(2)]
            win[pl.ds(base + j * 8, TILE), :] = jnp.concatenate(pair, axis=0).astype(BF)

    @pl.when(me == plan.p - 1)
    def _():
        base = plan.small_row - plan.starts[plan.p - 1]
        tiny[...] = jnp.zeros_like(tiny)
        for row, kept, nj in plan.pairs():
            for layer in range(2):
                tiny[pl.ds(kept + layer, nj, stride=2), :] = values[pl.ds(base + row + layer * nj, nj), :]
        win[pl.ds(base, tiny.shape[0]), :] = tiny[...].astype(BF)

    def rows_of(k, e, s, core):
        row = place.owner(dims_of(k), e, core) * unit + s * part
        return w_refs[k].at[pl.ds(pl.multiple_of(row, TILE), part)]

    slot = {here: 0, (1, 0, 0): 1, (0, 1, 0): 2, (0, 0, 1): 3, (1, 1, 0): 4, (1, 0, 1): 5, (0, 1, 1): 6, (1, 1, 1): 7}

    def index(k, e, s):
        return (slot[e] * 3 + k) * HALVES + s

    def src(k, e, s):
        return win.at[pl.ds((3 * s + k) * part, part)] if e == here else rows_of(k, e, s, place.core)

    sent = []

    def send(k, e, s, n):
        there = list(e)
        there[n] = 1
        i = index(k, tuple(there), s)
        copy = remote(
            src(k, e, s), rows_of(k, e, s, place.core), s_send.at[i], s_recv.at[i], place.flipped(dims_of(k)[n])
        )
        copy.start()
        sent.append(copy)

    def share(k, e, s):
        i = index(k, e, s)
        copy = remote(src(k, e, s), rows_of(k, e, s, place.core), d_send.at[i], d_recv.at[i], partner)
        copy.start()
        sent.append(copy)

    def arrival(k, e, s):
        i, dst = index(k, e, s), rows_of(k, e, s, place.core)
        return remote(dst, dst, s_send.at[i], s_recv.at[i], partner)

    def shared(k, e, s):
        i, dst = index(k, e, s), rows_of(k, e, s, 1 - place.core)
        return remote(dst, dst, d_send.at[i], d_recv.at[i], partner)

    for s in range(HALVES):
        plan.sort(first_row, 3 * s * part, 3 * (s + 1) * part, True, move)
        if s == 0:
            meet()
        for n in range(3):
            for k in range(3):
                send(k, here, s, n)
    for s in range(HALVES):
        for k in range(3):
            share(k, here, s)
    rows = 3 * TILE
    for s in range(HALVES):
        for k in range(3):

            def keep(i, _, k=k, s=s):
                at = pl.multiple_of(i * rows, rows)
                to = pl.ds(pl.multiple_of(me * unit + s * part + at, TILE), rows)
                w_refs[k][to, :] = win[pl.ds((3 * s + k) * part + at, rows), :]
                return 0

            lax.fori_loop(0, part // rows, keep, 0)
    for e in list(slot)[1:]:
        for s in range(HALVES):
            for k in range(3):
                arrival(k, e, s).wait_recv()
                for n in range(1, 3):
                    if not any(e[n:]):
                        send(k, e, s, n)
                share(k, e, s)
    for e in slot:
        for s in range(HALVES):
            for k in range(3):
                shared(k, e, s).wait_recv()
    for copy in sent:
        copy.wait_send()

    for r in range(1, plan.p):
        size = plan.group(plan.starts[r])[1]
        nj, shape = size // 8, (size, LANES)
        row, lane = lax.broadcasted_iota(jnp.int32, shape, 0), lax.broadcasted_iota(jnp.int32, shape, 1)
        at = (lax.rem(row, 8) * nj + lax.div(row, 8)) * LANES + lane
        cut = r * plan.shard - plan.starts[r] * LANES
        gap = plan.starts[r] - plan.starts[r - 1] - plan.window
        before = w_refs[2][pl.ds(r * unit + gap, size), :]
        rows = pl.ds(r * unit, size)
        w_refs[0][rows, :] = jnp.where(at < cut, before.astype(F32), w_refs[0][rows, :].astype(F32)).astype(BF)


def all_gather(plan, win):
    dma = pltpu.SemaphoreType.DMA
    n = 8 * 3 * HALVES
    return pl.pallas_call(
        functools.partial(ag_kernel, plan),
        out_shape=[pltpu.VMEM((plan.p * plan.unit, LANES), BF)] * 3,
        in_specs=[pl.BlockSpec(memory_space=pltpu.VMEM)],
        out_specs=[pl.BlockSpec(memory_space=pltpu.VMEM)] * 3,
        scratch_shapes=[pltpu.VMEM((plan.window, LANES), BF), pltpu.VMEM((small_rows(plan), LANES), F32)]
        + [dma((n,))] * 4,
        compiler_params=pltpu.CompilerParams(collective_id=1, has_side_effects=True, vmem_limit_bytes=8 << 20),
        name="all_gather",
    )(win)


def small_rows(plan):
    return -(-plan.small_size // (LANES * TILE)) * TILE


def restore_kernel(plan, *refs):
    w_refs, outs, out_sem = refs[:3], refs[3:-1], refs[-1]
    p, part = plan.p, plan.piece
    copies = []

    def copy(r, x, y, dst):
        for n in range(x // part, -(-y // part)):
            lo, hi = max(x, n * part), min(y, (n + 1) * part)
            src = w_refs[n % 3].at[pl.ds(r * plan.unit + n // 3 * part + lo - n * part, hi - lo)]
            copies.append(pltpu.make_async_copy(src, dst(lo - x, hi - lo), out_sem.at[len(copies)]))

    for r in range(p):
        lo = plan.starts[r]
        hi = plan.starts[r + 1] if r + 1 < p else plan.small_row
        for t, (a, b) in enumerate(plan.spans()[:-1]):
            x, y = max(a, lo), min(b, hi)
            if x < y:
                copy(r, x - lo, y - lo, lambda at, size, t=t, x=x, a=a: outs[t].at[pl.ds(x - a + at, size)])
    base = plan.small_row - plan.starts[p - 1]
    for out, (_, kept, nj) in zip(outs[len(plan.big):], plan.pairs()):
        copy(p - 1, base + kept, base + kept + out.shape[0], lambda at, size, out=out: out.at[pl.ds(at, size)])
    for c in copies:
        c.start()
    for c in copies:
        c.wait()


def restore(plan, gathered, shapes):
    n = len(plan.big)
    dma = pltpu.SemaphoreType.DMA
    outs = pl.pallas_call(
        functools.partial(restore_kernel, plan),
        out_shape=[jax.ShapeDtypeStruct((rows, LANES), BF) for rows, _, _ in plan.big]
        + [jax.ShapeDtypeStruct((2 * nj if m else -(-2 * nj // TILE) * TILE, LANES), BF)
           for m, (_, _, nj) in enumerate(plan.pairs())],
        in_specs=[ANY] * 3,
        out_specs=[ANY] * len(shapes),
        scratch_shapes=[dma((3 * HALVES * plan.p + 3 * n,))],
        compiler_params=pltpu.CompilerParams(vmem_limit_bytes=1 << 20),
        name="restore",
    )(*gathered)
    result = [from_stored(x, nj, s) for x, (_, nj, _), s in zip(outs, plan.big, shapes)]
    for x, (_, _, nj), s in zip(outs[n:], plan.pairs(), shapes[n:]):
        result.append(x[:2 * nj].reshape(nj, 2, LANES).transpose(1, 0, 2).reshape(s))
    return tuple(result)


def adam_update(g, m, v, w, lr, beta1, beta2, eps, step):
    t = step.astype(jnp.float32)
    m_new = beta1 * m + (1.0 - beta1) * g
    v_new = beta2 * v + (1.0 - beta2) * (g * g)
    m_hat = m_new * (1.0 / (1.0 - beta1 ** t))
    v_hat = v_new * (1.0 / (1.0 - beta2 ** t))
    w_new = w - lr * m_hat / (jnp.sqrt(v_hat) + eps)
    return m_new, v_new, w_new


def solution(mesh):
    p = mesh.shape["outer"] * mesh.shape["inner"]

    def body(g_emb, g_qkv, g_o, g_w1, g_w2, g_bqkv, g_b1, g_dvec, m, v, w, lr, beta1, beta2, eps, step):
        grads = (g_emb, g_qkv, g_o, g_w1, g_w2, g_bqkv, g_b1, g_dvec)
        shapes = tuple(x.shape[1:] for x in grads)
        plan = Plan(shapes, p)
        n = len(plan.big)
        stored = [as_stored(x, nj) for x, (_, nj, _) in zip(grads, plan.big)]
        stored.append(grads[n].reshape(shapes[n]))
        stored += [x.reshape(2, -1, LANES).transpose(1, 0, 2).reshape(-1, LANES) for x in grads[n + 1:]]
        total = reduce_scatter(plan, stored).reshape(-1)
        r = lax.axis_index(AXES)
        offset = r * plan.shard - plan.start(r) * LANES
        g = lax.dynamic_slice(total, (offset,), (plan.shard,)) / p
        m_new, v_new, w_new = adam_update(g, m, v, w, lr, beta1, beta2, eps, step)
        front = max(i * plan.shard - plan.starts[i] * LANES for i in range(p))
        back = plan.window * LANES - plan.shard
        win = lax.dynamic_slice(jnp.pad(w_new, (front, back)), (front - offset,), (plan.window * LANES,))
        wb = all_gather(plan, win.reshape(plan.window, LANES))
        return (m_new, v_new, w_new) + restore(plan, wb, shapes)

    g3 = P(AXES, None, None)
    g4 = P(AXES, None, None, None)
    flat = P(AXES)
    rep = P()
    in_specs = (g3, g4, g4, g4, g4, g3, g3, g4, flat, flat, flat, rep, rep, rep, rep, rep)
    out_specs = (flat, flat, flat, rep, rep, rep, rep, rep, rep, rep, rep)
    return jax.shard_map(body, mesh=mesh, in_specs=in_specs, out_specs=out_specs, check_vma=False)
```

```python
import functools
import math

import jax
import jax.numpy as jnp
from jax import lax
from jax.experimental import pallas as pl
from jax.experimental.pallas import tpu as pltpu
from jax.sharding import PartitionSpec as P

AXES = ("outer", "inner")
MESH = pl.DeviceIdType.MESH
ANY = pl.BlockSpec(memory_space=pl.ANY)
LANES = 128
TILE = 16
SPLIT = 4
HALVES = 2
DEEP = 2
PAD = 128
BLOCK = 133
LEAD = 12
BF = jnp.bfloat16
F32 = jnp.float32


class Plan:
    def __init__(self, shapes, p):
        self.p = p
        self.sizes = [math.prod(s) for s in shapes]
        self.total = sum(self.sizes)
        self.shard = self.total // p
        self.big = []
        start = 0
        for s, n in zip(shapes, self.sizes):
            if s[-2] % TILE == 0:
                self.big.append((n // LANES, s[-1] // LANES, start // LANES))
                start += n
        self.small_row = start // LANES
        self.small_size = self.total - start
        self.starts, need = [], 0
        for r in range(p):
            self.starts.append(self.group(r * self.shard // LANES)[0])
            low, size = self.group(((r + 1) * self.shard - 1) // LANES)
            need = max(need, low + size - self.starts[r])
        self.part = -(-need // (3 * SPLIT * TILE)) * TILE
        self.unit = SPLIT * self.part
        self.window = 3 * self.unit
        self.piece = self.unit // HALVES
        self.small_rows = self.starts[p - 1] + self.window - self.small_row

    def group(self, row):
        for n, nj, flat in self.big:
            if flat <= row < flat + n:
                size = 8 * nj
                return flat + (row - flat) // size * size, size
        return self.small_row + (row - self.small_row) // TILE * TILE, TILE

    def spans(self):
        spans = [(flat, flat + n) for n, _, flat in self.big]
        return spans + [(self.small_row, self.small_row + self.small_rows)]

    def crossing(self):
        out = {}
        for start in self.starts:
            for lo in range(start, start + self.window, self.part):
                cuts = []
                for t, (x, y) in enumerate(self.spans()):
                    x, y = max(x, lo), min(y, lo + self.part)
                    if x < y:
                        cuts.append((t, x - self.spans()[t][0], y - x, x - lo))
                if len(cuts) > 1:
                    out[lo] = cuts
        return out

    def start(self, r):
        row = jnp.int32(self.starts[0])
        for i in range(1, self.p):
            row = jnp.where(r == i, jnp.int32(self.starts[i]), row)
        return row

    def segments(self, first):
        out = []
        for n, nj, flat in self.big:
            lo = jnp.maximum(first, flat)
            hi = jnp.minimum(first + self.window, flat + n)
            out.append((nj, lo - first, lax.div(jnp.maximum(hi - lo, 0), 8 * nj)))
        return out

    def shift(self, r, first):
        offset = r * self.shard - first * LANES
        return lax.div(offset, LANES), lax.rem(offset, LANES)

    def sort(self, first, lo, hi, spill, move):
        for nj, row, groups in self.segments(first):
            size = 8 * nj
            more = size - 1 if spill else 0
            done, todo = [
                jnp.minimum(groups, lax.div(jnp.maximum(x - row, 0) + more, size)) if x else 0 for x in (lo, hi)
            ]

            def body(i, _, nj=nj, row=row, done=done, size=size):
                move(nj, pl.multiple_of(row + (done + i) * size, TILE))
                return 0

            lax.fori_loop(0, todo - done, body, 0)

    def pairs(self):
        flat, row, kept = [], 0, 0
        for n in self.sizes[len(self.big):]:
            flat.append((row, n // (2 * LANES)))
            row += n // LANES
        out = []
        for at, nj in flat[1:] + flat[:1]:
            out.append((at, kept, nj))
            kept += 2 * nj
        return out[-1:] + out[:-1]


def as_stored(x, nj):
    return x.reshape(-1, 8, nj, LANES).transpose(0, 2, 1, 3).reshape(-1, LANES)


def from_stored(x, nj, shape):
    return x.reshape(-1, nj, 8, LANES).transpose(0, 2, 1, 3).reshape(shape)


class Place:
    def __init__(self):
        o, i = lax.axis_index("outer"), lax.axis_index("inner")
        self.bits = [lax.div(o, 2), lax.rem(o, 2), lax.div(i, 2)]
        self.core = lax.rem(i, 2)

    def flipped(self, d):
        b = list(self.bits)
        b[d] = 1 - b[d]
        return (b[0] * 2 + b[1], b[2] * 2 + self.core)

    def partner(self):
        return (self.bits[0] * 2 + self.bits[1], self.bits[2] * 2 + 1 - self.core)

    def neighbour(self, k, n):
        d = lax.rem(k + n, 3)
        b = [jnp.where(d == i, 1 - x, x) for i, x in enumerate(self.bits)]
        return (b[0] * 2 + b[1], b[2] * 2 + self.core)

    def part(self, i):
        return lax.div(i, 3 * SPLIT), lax.rem(i, 3), lax.rem(i, 3 * SPLIT)

    def block(self, a, k, core):
        e = [1 - lax.div(a, 4), 1 - lax.rem(lax.div(a, 2), 2), 1 - lax.rem(a, 2)]
        r = core
        for d, weight in enumerate((8, 4, 2)):
            j = lax.rem(d - k + 3, 3)
            flip = jnp.where(j == 0, e[0], jnp.where(j == 1, e[1], e[2]))
            r = r + weight * (self.bits[d] + flip - 2 * self.bits[d] * flip)
        return r

    def owner(self, dims, e, core):
        b = list(self.bits)
        for d, flip in zip(dims, e):
            if flip:
                b[d] = 1 - b[d]
        return b[0] * 8 + b[1] * 4 + b[2] * 2 + core


def dims_of(k):
    return (k, (k + 1) % 3, (k + 2) % 3)


def arrive(place):
    barrier = pltpu.get_barrier_semaphore()
    for peer in [place.partner()] + [place.flipped(d) for d in range(3)]:
        pl.semaphore_signal(barrier, inc=1, device_id=peer, device_id_type=MESH)


def meet():
    pl.semaphore_wait(pltpu.get_barrier_semaphore(), 4)


def remote(src, dst, send, recv, dev):
    return pltpu.make_async_remote_copy(
        src_ref=src, dst_ref=dst, send_sem=send, recv_sem=recv, device_id=dev, device_id_type=MESH
    )


def rs_kernel(plan, *refs):
    n_big = len(plan.big)
    n_in = n_big + len(plan.pairs())
    flat, late_ref = refs[n_in:n_in + 2]
    early, r1, r2, own, oth, small, odd = refs[n_in + 2:n_in + 9]
    own_sem, oth_sem, d_send, d_recv, s1_send, s1_recv, s2_send, s2_recv, s3_send, s3_recv, tiny_sem, free = refs[
        n_in + 9:
    ]
    r3 = early
    xs = refs[:n_big] + (small,)
    part = plan.part
    wave = 3 * SPLIT
    early_n = 4 * wave
    place = Place()
    partner = place.partner()
    crossing = plan.crossing()

    def pick(i, core, issue):
        a, k, at = place.part(i)
        row = plan.start(place.block(a, k, core)) + at * part
        for t, (lo, hi) in enumerate(plan.spans()):

            @pl.when((row >= lo) & (row <= hi - part))
            def _(t=t, lo=lo):
                issue(xs[t].at[pl.ds(pl.multiple_of(row - lo, TILE), part)], 0, part)

        for first, cuts in crossing.items():

            @pl.when(row == first)
            def _(cuts=cuts):
                for t, at, size, to in cuts:
                    issue(xs[t].at[pl.ds(at, size)], to, size)

    def swap(i):
        slot = i

        def issue(src, at, size):
            remote(src, early.at[slot, pl.ds(at, size)], d_send.at[slot], d_recv.at[slot], partner).start()

        pick(i, 1 - place.core, issue)

    def swap_late(i):
        slot = i

        def issue(src, at, size):
            remote(
                src, late_ref.at[slot, pl.ds(at, size)], d_send.at[early_n + slot], d_recv.at[early_n + slot], partner
            ).start()

        pick(early_n + i, 1 - place.core, issue)

    def swapped(slot):
        return remote(early.at[slot], early.at[slot], d_send.at[slot], d_recv.at[slot], partner)

    def swapped_late(slot):
        sems = d_send.at[early_n + slot], d_recv.at[early_n + slot]
        return remote(late_ref.at[slot], late_ref.at[slot], *sems, partner)

    def load(i):
        to = lax.rem(i, DEEP)

        def issue(src, at, size):
            pltpu.make_async_copy(src, own.at[to, pl.ds(at, size)], own_sem.at[to]).start()

        pick(i, place.core, issue)

    def loaded(i):
        to = lax.rem(i, DEEP)
        return pltpu.make_async_copy(late_ref.at[0], own.at[to], own_sem.at[to])

    def fetch(i):
        to = lax.rem(i, DEEP)
        return pltpu.make_async_copy(late_ref.at[i], oth.at[to], oth_sem.at[to])

    def hop(stage, k, slot):
        src, dst, send, recv, base = (
            (early, r1, s1_send, s1_recv, 0),
            (r1, r2, s2_send, s2_recv, 0),
            (r1, r3, s3_send, s3_recv, 2 * wave),
        )[stage]
        return remote(src.at[base + slot], dst.at[slot], send.at[slot], recv.at[slot], place.neighbour(k, stage))

    def add(dst, *srcs):
        step = 48

        def body(i, _):
            rows = pl.ds(pl.multiple_of(i * step, TILE), step)
            total = dst[rows, :]
            for s in srcs:
                total = total + s[rows, :]
            dst[rows, :] = total
            return 0

        lax.fori_loop(0, part // step, body, 0)

    def loop(count, f):
        def body(i, _):
            f(i)
            return 0

        lax.fori_loop(0, count, body, 0)

    arrive(place)
    copies = []
    for m, (x, (_, kept, nj)) in enumerate(zip(refs[n_big:n_in], plan.pairs())):
        dst = odd if m == 0 else small.at[pl.ds(kept, 2 * nj)]
        copies.append(pltpu.make_async_copy(x, dst, tiny_sem.at[m]))
        copies[-1].start()
    end = plan.small_size // LANES
    small[end:, :] = jnp.zeros((plan.small_rows - end, LANES), F32)
    for c in copies:
        c.wait()
    _, kept, nj = plan.pairs()[0]
    for j in range(nj):
        small[kept + 2 * j:kept + 2 * j + 2, :] = odd[:, j * LANES:(j + 1) * LANES]
    loop(DEEP, load)
    meet()
    loop(LEAD, swap)

    def first(i):
        k, slot = lax.rem(i, 3), i

        @pl.when(i + LEAD < early_n)
        def _():
            swap(i + LEAD)

        @pl.when(i + LEAD >= early_n)
        def _():
            swap_late(i + LEAD - early_n)

        loaded(i).wait()
        swapped(slot).wait_recv()
        add(early.at[slot], own.at[lax.rem(i, DEEP)])
        hop(0, k, slot).start()
        load(i + DEEP)

    loop(early_n, first)

    def prefetch(i):
        swapped_late(i).wait_recv()
        fetch(i).start()

    loop(DEEP, prefetch)

    def second(i):
        k, slot = lax.rem(i, 3), i

        @pl.when(i + LEAD < early_n)
        def _():
            swap_late(i + LEAD)

        to = lax.rem(i, DEEP)
        loaded(i).wait()
        fetch(i).wait()
        hop(0, k, slot).wait_recv()
        add(r1.at[slot], own.at[to], oth.at[to])

        @pl.when(i < 2 * wave)
        def _():
            hop(1, k, slot).start()

        @pl.when(i + DEEP < early_n)
        def _():
            load(early_n + i + DEEP)
            prefetch(i + DEEP)

    loop(early_n, second)

    def gone(i):
        hop(0, lax.rem(i, 3), i).wait_send()

    loop(wave, gone)
    for d in range(3):
        pl.semaphore_signal(free, inc=1, device_id=place.flipped(d), device_id_type=MESH)
    pl.semaphore_wait(free, 3)

    def third(i):
        k, slot = lax.rem(i, 3), i
        hop(1, k, slot).wait_recv()
        add(r1.at[2 * wave + slot], r2.at[slot])

        @pl.when(i < wave)
        def _():
            hop(2, k, slot).start()

    loop(2 * wave, third)

    me = place.owner(dims_of(0), (0, 0, 0), place.core)
    first_row = plan.start(me)
    stored = r1.at[pl.ds(3 * wave, wave)].reshape(plan.window, LANES)

    def move(nj, base):
        for j in range(nj):
            flat[pl.ds(base + j, 8, stride=nj), :] = stored[pl.ds(base + j * 8, 8), :]

    for s in range(SPLIT):

        def fourth(j, s=s):
            slot = 3 * s + j
            hop(2, j, slot).wait_recv()
            add(r1.at[3 * wave + slot], r3.at[slot])

        loop(3, fourth)
        plan.sort(first_row, 3 * s * part, 3 * (s + 1) * part, False, move)

    @pl.when(me == plan.p - 1)
    def _():
        base = plan.small_row - plan.starts[plan.p - 1]
        for row, kept, nj in plan.pairs():
            for layer in range(2):
                flat[pl.ds(base + row + layer * nj, nj), :] = stored[pl.ds(base + kept + layer, nj, stride=2), :]

    def sent(i):
        k, slot = lax.rem(i, 3), i
        swapped(slot).wait_send()
        swapped_late(slot).wait_send()

        @pl.when(i >= wave)
        def _():
            hop(0, k, slot).wait_send()

        @pl.when(i < 2 * wave)
        def _():
            hop(1, k, slot).wait_send()

        @pl.when(i < wave)
        def _():
            hop(2, k, slot).wait_send()

    loop(early_n, sent)


def reduce_scatter(plan, xs):
    dma = pltpu.SemaphoreType.DMA
    wave = 3 * SPLIT
    slots = [4 * wave, 4 * wave, 2 * wave, DEEP, DEEP]
    used = sum(slots) * plan.part * LANES * 4 + (5 << 19)
    g, _ = pl.pallas_call(
        functools.partial(rs_kernel, plan),
        out_shape=(
            pltpu.VMEM((plan.window, LANES), F32),
            jax.ShapeDtypeStruct((4 * wave, plan.part, LANES), F32),
        ),
        in_specs=[ANY] * len(xs),
        out_specs=(pl.BlockSpec(memory_space=pltpu.VMEM), ANY),
        scratch_shapes=[pltpu.VMEM((n, plan.part, LANES), F32) for n in slots]
        + [pltpu.VMEM((plan.small_rows, LANES), F32), pltpu.VMEM(xs[len(plan.big)].shape, F32)]
        + [dma((DEEP,)), dma((DEEP,))]
        + [dma((n * wave,)) for n in (8, 8, 4, 4, 2, 2, 1, 1)]
        + [dma((len(plan.pairs()),)), pltpu.SemaphoreType.REGULAR],
        compiler_params=pltpu.CompilerParams(
            collective_id=0, has_side_effects=True, vmem_limit_bytes=used
        ),
        name="reduce_scatter",
    )(*xs)
    return g


def ag_kernel(plan, values, *refs):
    w_refs, (win, tiny, s_send, s_recv, d_send, d_recv) = refs[:3], refs[3:]
    part, unit = plan.piece, plan.unit
    place = Place()
    partner = place.partner()
    here = (0, 0, 0)
    me = place.owner(dims_of(0), here, place.core)
    arrive(place)

    first_row = plan.start(me)
    down, right = plan.shift(me, first_row)

    def value(row, n, stride=1):
        at = row - down + PAD
        lane = lax.broadcasted_iota(jnp.int32, (n, LANES), 1)
        if stride == 1:
            here, before = values[pl.ds(at, n), :], values[pl.ds(at - 1, n), :]
        else:
            here, before = values[pl.ds(at, n, stride=stride), :], values[pl.ds(at - 1, n, stride=stride), :]
        return jnp.where(lane >= right, here, before)

    def move(nj, base):
        for j in range(0, nj, 2):
            pair = [value(base + j + h, 8, nj) for h in range(2)]
            win[pl.ds(base + j * 8, TILE), :] = jnp.concatenate(pair, axis=0).astype(BF)

    @pl.when(me == plan.p - 1)
    def _():
        base = plan.small_row - plan.starts[plan.p - 1]
        tiny[...] = jnp.zeros_like(tiny)
        for row, kept, nj in plan.pairs():
            for layer in range(2):
                tiny[pl.ds(kept + layer, nj, stride=2), :] = value(base + row + layer * nj, nj)
        win[pl.ds(base, tiny.shape[0]), :] = tiny[...].astype(BF)

    def rows_of(k, e, s, core):
        row = place.owner(dims_of(k), e, core) * unit + s * part
        return w_refs[k].at[pl.ds(pl.multiple_of(row, TILE), part)]

    slot = {here: 0, (1, 0, 0): 1, (0, 1, 0): 2, (0, 0, 1): 3, (1, 1, 0): 4, (1, 0, 1): 5, (0, 1, 1): 6, (1, 1, 1): 7}

    def index(k, e, s):
        return (slot[e] * 3 + k) * HALVES + s

    def src(k, e, s):
        return win.at[pl.ds((3 * s + k) * part, part)] if e == here else rows_of(k, e, s, place.core)

    sent = []

    def send(k, e, s, n):
        there = list(e)
        there[n] = 1
        i = index(k, tuple(there), s)
        copy = remote(
            src(k, e, s), rows_of(k, e, s, place.core), s_send.at[i], s_recv.at[i], place.flipped(dims_of(k)[n])
        )
        copy.start()
        sent.append(copy)

    def share(k, e, s):
        i = index(k, e, s)
        copy = remote(src(k, e, s), rows_of(k, e, s, place.core), d_send.at[i], d_recv.at[i], partner)
        copy.start()
        sent.append(copy)

    def arrival(k, e, s):
        i, dst = index(k, e, s), rows_of(k, e, s, place.core)
        return remote(dst, dst, s_send.at[i], s_recv.at[i], partner)

    def shared(k, e, s):
        i, dst = index(k, e, s), rows_of(k, e, s, 1 - place.core)
        return remote(dst, dst, d_send.at[i], d_recv.at[i], partner)

    for s in range(HALVES):
        plan.sort(first_row, 3 * s * part, 3 * (s + 1) * part, True, move)
        if s == 0:
            meet()
        for n in range(3):
            for k in range(3):
                send(k, here, s, n)
    for s in range(HALVES):
        for k in range(3):
            share(k, here, s)
    rows = 3 * TILE
    for s in range(HALVES):
        for k in range(3):

            def keep(i, _, k=k, s=s):
                at = pl.multiple_of(i * rows, rows)
                to = pl.ds(pl.multiple_of(me * unit + s * part + at, TILE), rows)
                w_refs[k][to, :] = win[pl.ds((3 * s + k) * part + at, rows), :]
                return 0

            lax.fori_loop(0, part // rows, keep, 0)
    for e in list(slot)[1:]:
        for s in range(HALVES):
            for k in range(3):
                arrival(k, e, s).wait_recv()
                for n in range(1, 3):
                    if not any(e[n:]):
                        send(k, e, s, n)
                share(k, e, s)
    for e in slot:
        for s in range(HALVES):
            for k in range(3):
                shared(k, e, s).wait_recv()
    for copy in sent:
        copy.wait_send()

    for r in range(1, plan.p):
        size = plan.group(plan.starts[r])[1]
        nj, shape = size // 8, (size, LANES)
        row, lane = lax.broadcasted_iota(jnp.int32, shape, 0), lax.broadcasted_iota(jnp.int32, shape, 1)
        at = (lax.rem(row, 8) * nj + lax.div(row, 8)) * LANES + lane
        cut = r * plan.shard - plan.starts[r] * LANES
        gap = plan.starts[r] - plan.starts[r - 1] - plan.window
        before = w_refs[2][pl.ds(r * unit + gap, size), :]
        rows = pl.ds(r * unit, size)
        w_refs[0][rows, :] = jnp.where(at < cut, before.astype(F32), w_refs[0][rows, :].astype(F32)).astype(BF)


def all_gather(plan, win):
    dma = pltpu.SemaphoreType.DMA
    n = 8 * 3 * HALVES
    return pl.pallas_call(
        functools.partial(ag_kernel, plan),
        out_shape=[pltpu.VMEM((plan.p * plan.unit, LANES), BF)] * 3,
        in_specs=[pl.BlockSpec(memory_space=pltpu.VMEM)],
        out_specs=[pl.BlockSpec(memory_space=pltpu.VMEM)] * 3,
        scratch_shapes=[pltpu.VMEM((plan.window, LANES), BF), pltpu.VMEM((small_rows(plan), LANES), F32)]
        + [dma((n,))] * 4,
        compiler_params=pltpu.CompilerParams(collective_id=1, has_side_effects=True, vmem_limit_bytes=4 << 20),
        name="all_gather",
    )(win)


def small_rows(plan):
    return -(-plan.small_size // (LANES * TILE)) * TILE


def restore_kernel(plan, *refs):
    w_refs, outs, out_sem = refs[:3], refs[3:-1], refs[-1]
    p, part = plan.p, plan.piece
    copies = []

    def copy(r, x, y, dst):
        for n in range(x // part, -(-y // part)):
            lo, hi = max(x, n * part), min(y, (n + 1) * part)
            src = w_refs[n % 3].at[pl.ds(r * plan.unit + n // 3 * part + lo - n * part, hi - lo)]
            copies.append(pltpu.make_async_copy(src, dst(lo - x, hi - lo), out_sem.at[len(copies)]))

    for r in range(p):
        lo = plan.starts[r]
        hi = plan.starts[r + 1] if r + 1 < p else plan.small_row
        for t, (a, b) in enumerate(plan.spans()[:-1]):
            x, y = max(a, lo), min(b, hi)
            if x < y:
                copy(r, x - lo, y - lo, lambda at, size, t=t, x=x, a=a: outs[t].at[pl.ds(x - a + at, size)])
    base = plan.small_row - plan.starts[p - 1]
    for out, (_, kept, nj) in zip(outs[len(plan.big):], plan.pairs()):
        copy(p - 1, base + kept, base + kept + out.shape[0], lambda at, size, out=out: out.at[pl.ds(at, size)])
    for c in copies:
        c.start()
    for c in copies:
        c.wait()


def restore(plan, gathered, shapes):
    n = len(plan.big)
    dma = pltpu.SemaphoreType.DMA
    outs = pl.pallas_call(
        functools.partial(restore_kernel, plan),
        out_shape=[jax.ShapeDtypeStruct((rows, LANES), BF) for rows, _, _ in plan.big]
        + [jax.ShapeDtypeStruct((2 * nj if m else -(-2 * nj // TILE) * TILE, LANES), BF)
           for m, (_, _, nj) in enumerate(plan.pairs())],
        in_specs=[ANY] * 3,
        out_specs=[ANY] * len(shapes),
        scratch_shapes=[dma((3 * HALVES * plan.p + 3 * n,))],
        compiler_params=pltpu.CompilerParams(vmem_limit_bytes=4 << 20),
        name="restore",
    )(*gathered)
    result = [from_stored(x, nj, s) for x, (_, nj, _), s in zip(outs, plan.big, shapes)]
    for x, (_, _, nj), s in zip(outs[n:], plan.pairs(), shapes[n:]):
        result.append(x[:2 * nj].reshape(nj, 2, LANES).transpose(1, 0, 2).reshape(s))
    return tuple(result)


def update_kernel(plan, table, g, m, v, w, m_out, v_out, w_out, z):
    step = pl.program_id(0)
    me = lax.axis_index("outer") * 4 + lax.axis_index("inner")
    down, right = plan.shift(me, plan.start(me))
    lane = lax.broadcasted_iota(jnp.int32, (8, LANES), 1)
    left = lax.rem(LANES - right, LANES)
    beta1, gain1, beta2, gain2, scale1, scale2, lr, eps = [table[8 * n:8 * n + 8, :] for n in range(8)]
    size = 8 * LANES
    last = -(-plan.shard // size) - 1
    unroll = 7

    def body(i, _):
        for t in range(unroll):
            b = jnp.minimum(i * unroll + t, last - step * BLOCK)
            row = (step * BLOCK + b) * 8
            x0, x1 = g[pl.ds(row + down, 8), :], g[pl.ds(row + down + 1, 8), :]
            grad = pltpu.roll(jnp.where(lane >= right, x0, x1), left, 1) * (1.0 / plan.p)
            at = pl.ds(pl.multiple_of(b * size, size), size)
            m_new = beta1 * m[at].reshape(8, LANES) + gain1 * grad
            v_new = beta2 * v[at].reshape(8, LANES) + gain2 * (grad * grad)
            m_hat = m_new * scale1
            v_hat = v_new * scale2
            w_new = w[at].reshape(8, LANES) - lr * m_hat / (jnp.sqrt(v_hat) + eps)
            m_out[at] = m_new.reshape(size)
            v_out[at] = v_new.reshape(size)
            w_out[at] = w_new.reshape(size)
            z[pl.ds(pl.multiple_of(row + PAD, 8), 8), :] = pltpu.roll(w_new, right, 1)
        return 0

    lax.fori_loop(0, BLOCK // unroll, body, 0)


def update(plan, table, g, m, v, w):
    flat = jax.ShapeDtypeStruct((plan.shard,), F32)
    part = pl.BlockSpec((BLOCK * 8 * LANES,), lambda i: (i,))
    whole = pl.BlockSpec(memory_space=pltpu.VMEM)
    return pl.pallas_call(
        functools.partial(update_kernel, plan),
        grid=(pl.cdiv(plan.shard, BLOCK * 8 * LANES),),
        out_shape=(flat, flat, flat, pltpu.VMEM((plan.window + 2 * PAD, LANES), F32)),
        in_specs=[whole, whole, part, part, part],
        out_specs=(part, part, part, whole),
        compiler_params=pltpu.CompilerParams(vmem_limit_bytes=8 << 20),
        name="update",
    )(table, g, m, v, w)


def solution(mesh):
    p = mesh.shape["outer"] * mesh.shape["inner"]

    def body(g_emb, g_qkv, g_o, g_w1, g_w2, g_bqkv, g_b1, g_dvec, m, v, w, lr, beta1, beta2, eps, step):
        grads = (g_emb, g_qkv, g_o, g_w1, g_w2, g_bqkv, g_b1, g_dvec)
        shapes = tuple(x.shape[1:] for x in grads)
        plan = Plan(shapes, p)
        n = len(plan.big)
        stored = [as_stored(x, nj) for x, (_, nj, _) in zip(grads, plan.big)]
        stored.append(grads[n].reshape(shapes[n]))
        stored += [x.reshape(2, -1, LANES).transpose(1, 0, 2).reshape(-1, LANES) for x in grads[n + 1:]]
        t = step.astype(F32)
        scale1, scale2 = 1.0 / (1.0 - beta1 ** t), 1.0 / (1.0 - beta2 ** t)
        table = jnp.stack([beta1, 1.0 - beta1, beta2, 1.0 - beta2, scale1, scale2, lr, eps])
        table = jnp.broadcast_to(table[:, None, None], (8, 8, LANES)).reshape(64, LANES)
        total = reduce_scatter(plan, stored)
        m_new, v_new, w_new, values = update(plan, table, total, m, v, w)
        wb = all_gather(plan, values)
        return (m_new, v_new, w_new) + restore(plan, wb, shapes)

    g3 = P(AXES, None, None)
    g4 = P(AXES, None, None, None)
    flat = P(AXES)
    rep = P()
    in_specs = (g3, g4, g4, g4, g4, g3, g3, g4, flat, flat, flat, rep, rep, rep, rep, rep)
    out_specs = (flat, flat, flat, rep, rep, rep, rep, rep, rep, rep, rep)
    return jax.shard_map(body, mesh=mesh, in_specs=in_specs, out_specs=out_specs, check_vma=False)
```

```python
import functools
import math

import jax
import jax.numpy as jnp
from jax import lax
from jax.experimental import pallas as pl
from jax.experimental.pallas import tpu as pltpu
from jax.sharding import PartitionSpec as P

AXES = ("outer", "inner")
MESH = pl.DeviceIdType.MESH
ANY = pl.BlockSpec(memory_space=pl.ANY)
LANES = 128
TILE = 16
SPLIT = 4
HALVES = 2
DEEP = 4
LEAD = 12
BF = jnp.bfloat16
F32 = jnp.float32


class Plan:
    def __init__(self, shapes, p):
        self.p = p
        self.sizes = [math.prod(s) for s in shapes]
        self.total = sum(self.sizes)
        self.shard = self.total // p
        self.big = []
        start = 0
        for s, n in zip(shapes, self.sizes):
            if s[-2] % TILE == 0:
                self.big.append((n // LANES, s[-1] // LANES, start // LANES))
                start += n
        self.small_row = start // LANES
        self.small_size = self.total - start
        self.starts, need = [], 0
        for r in range(p):
            self.starts.append(self.group(r * self.shard // LANES)[0])
            low, size = self.group(((r + 1) * self.shard - 1) // LANES)
            need = max(need, low + size - self.starts[r])
        step = 3 * HALVES * 3 * TILE
        self.window = -(-need // step) * step
        self.unit = self.window // 3
        self.piece = self.unit // HALVES
        own = [b - a for a, b in zip(self.starts, self.starts[1:] + [self.total // LANES])]
        self.part = -(-max(own) // (3 * SPLIT * 8)) * 8
        self.sums = 3 * SPLIT * self.part
        self.edge = max(8 * nj for _, nj, _ in self.big)
        self.small_rows = self.starts[p - 1] + self.sums - self.small_row

    def group(self, row):
        for n, nj, flat in self.big:
            if flat <= row < flat + n:
                size = 8 * nj
                return flat + (row - flat) // size * size, size
        return self.small_row + (row - self.small_row) // TILE * TILE, TILE

    def spans(self):
        spans = [(flat, flat + n) for n, _, flat in self.big]
        return spans + [(self.small_row, self.small_row + self.small_rows)]

    def crossing(self):
        out = {}
        for start in self.starts:
            for lo in range(start, start + self.sums, self.part):
                cuts = []
                for t, (x, y) in enumerate(self.spans()):
                    x, y = max(x, lo), min(y, lo + self.part)
                    if x < y:
                        cuts.append((t, x - self.spans()[t][0], y - x, x - lo))
                if len(cuts) > 1:
                    out[lo] = cuts
        return out

    def start(self, r):
        row = jnp.int32(self.starts[0])
        for i in range(1, self.p):
            row = jnp.where(r == i, jnp.int32(self.starts[i]), row)
        return row

    def segments(self, first):
        out = []
        for n, nj, flat in self.big:
            lo = jnp.maximum(first, flat)
            hi = jnp.minimum(first + self.window, flat + n)
            out.append((nj, lo - first, lax.div(jnp.maximum(hi - lo, 0), 8 * nj)))
        return out

    def sort(self, first, lo, hi, spill, move):
        for nj, row, groups in self.segments(first):
            size = 8 * nj
            more = size - 1 if spill else 0
            done, todo = [
                jnp.minimum(groups, lax.div(jnp.maximum(x - row, 0) + more, size)) if x else 0 for x in (lo, hi)
            ]

            def body(i, _, nj=nj, row=row, done=done, size=size):
                move(nj, pl.multiple_of(row + (done + i) * size, TILE))
                return 0

            lax.fori_loop(0, todo - done, body, 0)

    def pairs(self):
        flat, row, kept = [], 0, 0
        for n in self.sizes[len(self.big):]:
            flat.append((row, n // (2 * LANES)))
            row += n // LANES
        out = []
        for at, nj in flat[1:] + flat[:1]:
            out.append((at, kept, nj))
            kept += 2 * nj
        return out[-1:] + out[:-1]


def as_stored(x, nj):
    return x.reshape(-1, 8, nj, LANES).transpose(0, 2, 1, 3).reshape(-1, LANES)


def from_stored(x, nj, shape):
    return x.reshape(-1, nj, 8, LANES).transpose(0, 2, 1, 3).reshape(shape)


class Place:
    def __init__(self):
        o, i = lax.axis_index("outer"), lax.axis_index("inner")
        self.bits = [lax.div(o, 2), lax.rem(o, 2), lax.div(i, 2)]
        self.core = lax.rem(i, 2)

    def flipped(self, d):
        b = list(self.bits)
        b[d] = 1 - b[d]
        return (b[0] * 2 + b[1], b[2] * 2 + self.core)

    def partner(self):
        return (self.bits[0] * 2 + self.bits[1], self.bits[2] * 2 + 1 - self.core)

    def neighbour(self, k, n):
        d = lax.rem(k + n, 3)
        b = [jnp.where(d == i, 1 - x, x) for i, x in enumerate(self.bits)]
        return (b[0] * 2 + b[1], b[2] * 2 + self.core)

    def part(self, i):
        return lax.div(i, 3 * SPLIT), lax.rem(i, 3), lax.rem(i, 3 * SPLIT)

    def block(self, a, k, core):
        e = [1 - lax.div(a, 4), 1 - lax.rem(lax.div(a, 2), 2), 1 - lax.rem(a, 2)]
        r = core
        for d, weight in enumerate((8, 4, 2)):
            j = lax.rem(d - k + 3, 3)
            flip = jnp.where(j == 0, e[0], jnp.where(j == 1, e[1], e[2]))
            r = r + weight * (self.bits[d] + flip - 2 * self.bits[d] * flip)
        return r

    def owner(self, dims, e, core):
        b = list(self.bits)
        for d, flip in zip(dims, e):
            if flip:
                b[d] = 1 - b[d]
        return b[0] * 8 + b[1] * 4 + b[2] * 2 + core


def dims_of(k):
    return (k, (k + 1) % 3, (k + 2) % 3)


def arrive(place, others=()):
    barrier = pltpu.get_barrier_semaphore()
    for peer in [place.partner()] + [place.flipped(d) for d in range(3)] + list(others):
        pl.semaphore_signal(barrier, inc=1, device_id=peer, device_id_type=MESH)


def meet(peers):
    pl.semaphore_wait(pltpu.get_barrier_semaphore(), peers)


def remote(src, dst, send, recv, dev):
    return pltpu.make_async_remote_copy(
        src_ref=src, dst_ref=dst, send_sem=send, recv_sem=recv, device_id=dev, device_id_type=MESH
    )


def rs_kernel(plan, *refs):
    n_big = len(plan.big)
    n_in = n_big + len(plan.pairs())
    flat, late_ref = refs[n_in:n_in + 2]
    early, r1, r2, r3, own, oth, small, odd, edge = refs[n_in + 2:n_in + 11]
    own_sem, oth_sem, d_send, d_recv, s1_send, s1_recv, s2_send, s2_recv, s3_send, s3_recv, tiny_sem, edge_sem = refs[
        n_in + 11:
    ]
    xs = refs[:n_big] + (small,)
    part = plan.part
    wave = 3 * SPLIT
    early_n = 4 * wave
    place = Place()
    partner = place.partner()
    crossing = plan.crossing()

    def pick(i, core, issue):
        a, k, at = place.part(i)
        row = plan.start(place.block(a, k, core)) + at * part
        for t, (lo, hi) in enumerate(plan.spans()):

            @pl.when((row >= lo) & (row <= hi - part))
            def _(t=t, lo=lo):
                issue(xs[t].at[pl.ds(pl.multiple_of(row - lo, 8), part)], 0, part)

        for first, cuts in crossing.items():

            @pl.when(row == first)
            def _(cuts=cuts):
                for t, at, size, to in cuts:
                    issue(xs[t].at[pl.ds(at, size)], to, size)

    def swap(i):
        slot = i

        def issue(src, at, size):
            remote(src, early.at[slot, pl.ds(at, size)], d_send.at[slot], d_recv.at[slot], partner).start()

        pick(i, 1 - place.core, issue)

    def swap_late(i):
        slot = i

        def issue(src, at, size):
            remote(
                src, late_ref.at[slot, pl.ds(at, size)], d_send.at[early_n + slot], d_recv.at[early_n + slot], partner
            ).start()

        pick(early_n + i, 1 - place.core, issue)

    def swapped(slot):
        return remote(early.at[slot], early.at[slot], d_send.at[slot], d_recv.at[slot], partner)

    def swapped_late(slot):
        sems = d_send.at[early_n + slot], d_recv.at[early_n + slot]
        return remote(late_ref.at[slot], late_ref.at[slot], *sems, partner)

    def load(i):
        to = lax.rem(i, DEEP)

        def issue(src, at, size):
            pltpu.make_async_copy(src, own.at[to, pl.ds(at, size)], own_sem.at[to]).start()

        pick(i, place.core, issue)

    def loaded(i):
        to = lax.rem(i, DEEP)
        return pltpu.make_async_copy(late_ref.at[0], own.at[to], own_sem.at[to])

    def fetch(i):
        to = lax.rem(i, DEEP)
        return pltpu.make_async_copy(late_ref.at[i], oth.at[to], oth_sem.at[to])

    def hop(stage, k, slot):
        src, dst, send, recv, base = (
            (early, r1, s1_send, s1_recv, 0),
            (r1, r2, s2_send, s2_recv, 0),
            (r1, r3, s3_send, s3_recv, 2 * wave),
        )[stage]
        return remote(src.at[base + slot], dst.at[slot], send.at[slot], recv.at[slot], place.neighbour(k, stage))

    def add(dst, *srcs):
        step = 48

        def some(rows):
            total = dst[rows, :]
            for s in srcs:
                total = total + s[rows, :]
            dst[rows, :] = total

        def body(i, _):
            some(pl.ds(pl.multiple_of(i * step, 8), step))
            return 0

        lax.fori_loop(0, part // step, body, 0)
        if part % step:
            some(pl.ds(part - part % step, part % step))

    def loop(count, f):
        def body(i, _):
            f(i)
            return 0

        lax.fori_loop(0, count, body, 0)

    me = place.owner(dims_of(0), (0, 0, 0), place.core)
    after = lax.rem(me + 1, plan.p)
    arrive(place, [(lax.div(after, 4), lax.rem(after, 4))])
    copies = []
    for m, (x, (_, kept, nj)) in enumerate(zip(refs[n_big:n_in], plan.pairs())):
        dst = odd if m == 0 else small.at[pl.ds(kept, 2 * nj)]
        copies.append(pltpu.make_async_copy(x, dst, tiny_sem.at[m]))
        copies[-1].start()
    end = plan.small_size // LANES
    small[end:, :] = jnp.zeros((plan.small_rows - end, LANES), F32)
    for c in copies:
        c.wait()
    _, kept, nj = plan.pairs()[0]
    for j in range(nj):
        small[kept + 2 * j:kept + 2 * j + 2, :] = odd[:, j * LANES:(j + 1) * LANES]
    loop(DEEP, load)
    meet(5)
    loop(LEAD, swap)

    def first(i):
        k, slot = lax.rem(i, 3), i

        @pl.when(i + LEAD < early_n)
        def _():
            swap(i + LEAD)

        @pl.when(i + LEAD >= early_n)
        def _():
            swap_late(i + LEAD - early_n)

        loaded(i).wait()
        swapped(slot).wait_recv()
        add(early.at[slot], own.at[lax.rem(i, DEEP)])
        hop(0, k, slot).start()
        load(i + DEEP)

    loop(early_n, first)

    def prefetch(i):
        swapped_late(i).wait_recv()
        fetch(i).start()

    loop(DEEP, prefetch)

    def second(i):
        k, slot = lax.rem(i, 3), i

        @pl.when(i + LEAD < early_n)
        def _():
            swap_late(i + LEAD)

        to = lax.rem(i, DEEP)
        loaded(i).wait()
        fetch(i).wait()
        hop(0, k, slot).wait_recv()
        add(r1.at[slot], own.at[to], oth.at[to])

        @pl.when(i < 2 * wave)
        def _():
            hop(1, k, slot).start()

        @pl.when(i + DEEP < early_n)
        def _():
            load(early_n + i + DEEP)
            prefetch(i + DEEP)

    loop(early_n, second)

    def third(i):
        k, slot = lax.rem(i, 3), i
        hop(1, k, slot).wait_recv()
        add(r1.at[2 * wave + slot], r2.at[slot])

        @pl.when(i < wave)
        def _():
            hop(2, k, slot).start()

    loop(2 * wave, third)

    first_row = plan.start(me)
    stored = r1.at[pl.ds(3 * wave, wave + 1)].reshape((wave + 1) * part, LANES)
    before = lax.rem(me + plan.p - 1, plan.p)
    passed = remote(
        r1.at[3 * wave, pl.ds(0, plan.edge)], edge, edge_sem.at[0], edge_sem.at[1],
        (lax.div(before, 4), lax.rem(before, 4)),
    )

    def move(nj, base):
        for j in range(nj):
            flat[pl.ds(base + j, 8, stride=nj), :] = stored[pl.ds(base + j * 8, 8), :]

    for s in range(SPLIT):

        def fourth(j, s=s):
            slot = 3 * s + j
            hop(2, j, slot).wait_recv()
            add(r1.at[3 * wave + slot], r3.at[slot])

        loop(3, fourth)
        if s == 0:
            passed.start()
        if s == SPLIT - 1:
            passed.wait_recv()
            gap = jnp.where(me == plan.p - 1, plan.sums, plan.start(after) - first_row)
            for i in range(0, plan.edge, TILE):
                stored[pl.ds(pl.multiple_of(gap + i, TILE if plan.sums % TILE == 0 else 8), TILE), :] = edge[i:i + TILE, :]
        end = 3 * (s + 1) * part if s < SPLIT - 1 else plan.window
        plan.sort(first_row, 3 * s * part, end, False, move)

    @pl.when(me == plan.p - 1)
    def _():
        base = plan.small_row - plan.starts[plan.p - 1]
        for row, kept, nj in plan.pairs():
            for layer in range(2):
                flat[pl.ds(base + row + layer * nj, nj), :] = stored[pl.ds(base + kept + layer, nj, stride=2), :]

    passed.wait_send()

    def sent(i):
        k, slot = lax.rem(i, 3), i
        swapped(slot).wait_send()
        swapped_late(slot).wait_send()
        hop(0, k, slot).wait_send()

        @pl.when(i < 2 * wave)
        def _():
            hop(1, k, slot).wait_send()

        @pl.when(i < wave)
        def _():
            hop(2, k, slot).wait_send()

    loop(early_n, sent)


def reduce_scatter(plan, xs):
    dma = pltpu.SemaphoreType.DMA
    wave = 3 * SPLIT
    slots = [4 * wave, 4 * wave + 1, 2 * wave, wave, DEEP, DEEP]
    used = (sum(slots) * plan.part * LANES * 4 >> 20) + 2
    g, _ = pl.pallas_call(
        functools.partial(rs_kernel, plan),
        out_shape=(
            pltpu.VMEM((plan.window, LANES), F32),
            jax.ShapeDtypeStruct((4 * wave, plan.part, LANES), F32),
        ),
        in_specs=[ANY] * len(xs),
        out_specs=(pl.BlockSpec(memory_space=pltpu.VMEM), ANY),
        scratch_shapes=[pltpu.VMEM((n, plan.part, LANES), F32) for n in slots]
        + [pltpu.VMEM((plan.small_rows, LANES), F32), pltpu.VMEM(xs[len(plan.big)].shape, F32)]
        + [pltpu.VMEM((plan.edge, LANES), F32)]
        + [dma((DEEP,)), dma((DEEP,))]
        + [dma((n * wave,)) for n in (8, 8, 4, 4, 2, 2, 1, 1)]
        + [dma((len(plan.pairs()),)), dma((2,))],
        compiler_params=pltpu.CompilerParams(
            collective_id=0, has_side_effects=True, vmem_limit_bytes=used << 20
        ),
        name="reduce_scatter",
    )(*xs)
    return g


def ag_kernel(plan, values, *refs):
    w_refs, (win, tiny, s_send, s_recv, d_send, d_recv) = refs[:3], refs[3:]
    part, unit = plan.piece, plan.unit
    place = Place()
    partner = place.partner()
    here = (0, 0, 0)
    me = place.owner(dims_of(0), here, place.core)
    arrive(place)

    first_row = plan.start(me)

    def move(nj, base):
        for j in range(0, nj, 2):
            pair = [values[pl.ds(base + j + h, 8, stride=nj), :] for h in range(2)]
            win[pl.ds(base + j * 8, TILE), :] = jnp.concatenate(pair, axis=0).astype(BF)

    @pl.when(me == plan.p - 1)
    def _():
        base = plan.small_row - plan.starts[plan.p - 1]
        tiny[...] = jnp.zeros_like(tiny)
        for row, kept, nj in plan.pairs():
            for layer in range(2):
                tiny[pl.ds(kept + layer, nj, stride=2), :] = values[pl.ds(base + row + layer * nj, nj), :]
        win[pl.ds(base, tiny.shape[0]), :] = tiny[...].astype(BF)

    def rows_of(k, e, s, core):
        row = place.owner(dims_of(k), e, core) * unit + s * part
        return w_refs[k].at[pl.ds(pl.multiple_of(row, TILE), part)]

    slot = {here: 0, (1, 0, 0): 1, (0, 1, 0): 2, (0, 0, 1): 3, (1, 1, 0): 4, (1, 0, 1): 5, (0, 1, 1): 6, (1, 1, 1): 7}

    def index(k, e, s):
        return (slot[e] * 3 + k) * HALVES + s

    def src(k, e, s):
        return win.at[pl.ds((3 * s + k) * part, part)] if e == here else rows_of(k, e, s, place.core)

    sent = []

    def send(k, e, s, n):
        there = list(e)
        there[n] = 1
        i = index(k, tuple(there), s)
        copy = remote(
            src(k, e, s), rows_of(k, e, s, place.core), s_send.at[i], s_recv.at[i], place.flipped(dims_of(k)[n])
        )
        copy.start()
        sent.append(copy)

    def share(k, e, s):
        i = index(k, e, s)
        copy = remote(src(k, e, s), rows_of(k, e, s, place.core), d_send.at[i], d_recv.at[i], partner)
        copy.start()
        sent.append(copy)

    def arrival(k, e, s):
        i, dst = index(k, e, s), rows_of(k, e, s, place.core)
        return remote(dst, dst, s_send.at[i], s_recv.at[i], partner)

    def shared(k, e, s):
        i, dst = index(k, e, s), rows_of(k, e, s, 1 - place.core)
        return remote(dst, dst, d_send.at[i], d_recv.at[i], partner)

    for s in range(HALVES):
        plan.sort(first_row, 3 * s * part, 3 * (s + 1) * part, True, move)
        if s == 0:
            meet(4)
        for n in range(3):
            for k in range(3):
                send(k, here, s, n)
    for s in range(HALVES):
        for k in range(3):
            share(k, here, s)
    rows = 3 * TILE
    for s in range(HALVES):
        for k in range(3):

            def keep(i, _, k=k, s=s):
                at = pl.multiple_of(i * rows, rows)
                to = pl.ds(pl.multiple_of(me * unit + s * part + at, TILE), rows)
                w_refs[k][to, :] = win[pl.ds((3 * s + k) * part + at, rows), :]
                return 0

            lax.fori_loop(0, part // rows, keep, 0)
    for e in list(slot)[1:]:
        for s in range(HALVES):
            for k in range(3):
                arrival(k, e, s).wait_recv()
                for n in range(1, 3):
                    if not any(e[n:]):
                        send(k, e, s, n)
                share(k, e, s)
    for e in slot:
        for s in range(HALVES):
            for k in range(3):
                shared(k, e, s).wait_recv()
    for copy in sent:
        copy.wait_send()

    for r in range(1, plan.p):
        size = plan.group(plan.starts[r])[1]
        nj, shape = size // 8, (size, LANES)
        row, lane = lax.broadcasted_iota(jnp.int32, shape, 0), lax.broadcasted_iota(jnp.int32, shape, 1)
        at = (lax.rem(row, 8) * nj + lax.div(row, 8)) * LANES + lane
        cut = r * plan.shard - plan.starts[r] * LANES
        gap = plan.starts[r] - plan.starts[r - 1] - plan.window
        before = w_refs[2][pl.ds(r * unit + gap, size), :]
        rows = pl.ds(r * unit, size)
        w_refs[0][rows, :] = jnp.where(at < cut, before.astype(F32), w_refs[0][rows, :].astype(F32)).astype(BF)


def all_gather(plan, win):
    dma = pltpu.SemaphoreType.DMA
    n = 8 * 3 * HALVES
    return pl.pallas_call(
        functools.partial(ag_kernel, plan),
        out_shape=[pltpu.VMEM((plan.p * plan.unit, LANES), BF)] * 3,
        in_specs=[pl.BlockSpec(memory_space=pltpu.VMEM)],
        out_specs=[pl.BlockSpec(memory_space=pltpu.VMEM)] * 3,
        scratch_shapes=[pltpu.VMEM((plan.window, LANES), BF), pltpu.VMEM((small_rows(plan), LANES), F32)]
        + [dma((n,))] * 4,
        compiler_params=pltpu.CompilerParams(collective_id=1, has_side_effects=True, vmem_limit_bytes=8 << 20),
        name="all_gather",
    )(win)


def small_rows(plan):
    return -(-plan.small_size // (LANES * TILE)) * TILE


def restore_kernel(plan, *refs):
    w_refs, outs, out_sem = refs[:3], refs[3:-1], refs[-1]
    p, part = plan.p, plan.piece
    copies = []

    def copy(r, x, y, dst):
        for n in range(x // part, -(-y // part)):
            lo, hi = max(x, n * part), min(y, (n + 1) * part)
            src = w_refs[n % 3].at[pl.ds(r * plan.unit + n // 3 * part + lo - n * part, hi - lo)]
            copies.append(pltpu.make_async_copy(src, dst(lo - x, hi - lo), out_sem.at[len(copies)]))

    for r in range(p):
        lo = plan.starts[r]
        hi = plan.starts[r + 1] if r + 1 < p else plan.small_row
        for t, (a, b) in enumerate(plan.spans()[:-1]):
            x, y = max(a, lo), min(b, hi)
            if x < y:
                copy(r, x - lo, y - lo, lambda at, size, t=t, x=x, a=a: outs[t].at[pl.ds(x - a + at, size)])
    base = plan.small_row - plan.starts[p - 1]
    for out, (_, kept, nj) in zip(outs[len(plan.big):], plan.pairs()):
        copy(p - 1, base + kept, base + kept + out.shape[0], lambda at, size, out=out: out.at[pl.ds(at, size)])
    for c in copies:
        c.start()
    for c in copies:
        c.wait()


def restore(plan, gathered, shapes):
    n = len(plan.big)
    dma = pltpu.SemaphoreType.DMA
    outs = pl.pallas_call(
        functools.partial(restore_kernel, plan),
        out_shape=[jax.ShapeDtypeStruct((rows, LANES), BF) for rows, _, _ in plan.big]
        + [jax.ShapeDtypeStruct((2 * nj if m else -(-2 * nj // TILE) * TILE, LANES), BF)
           for m, (_, _, nj) in enumerate(plan.pairs())],
        in_specs=[ANY] * 3,
        out_specs=[ANY] * len(shapes),
        scratch_shapes=[dma((3 * HALVES * plan.p + 3 * n,))],
        compiler_params=pltpu.CompilerParams(vmem_limit_bytes=1 << 20),
        name="restore",
    )(*gathered)
    result = [from_stored(x, nj, s) for x, (_, nj, _), s in zip(outs, plan.big, shapes)]
    for x, (_, _, nj), s in zip(outs[n:], plan.pairs(), shapes[n:]):
        result.append(x[:2 * nj].reshape(nj, 2, LANES).transpose(1, 0, 2).reshape(s))
    return tuple(result)


def adam_update(g, m, v, w, lr, beta1, beta2, eps, step):
    t = step.astype(jnp.float32)
    m_new = beta1 * m + (1.0 - beta1) * g
    v_new = beta2 * v + (1.0 - beta2) * (g * g)
    m_hat = m_new * (1.0 / (1.0 - beta1 ** t))
    v_hat = v_new * (1.0 / (1.0 - beta2 ** t))
    w_new = w - lr * m_hat / (jnp.sqrt(v_hat) + eps)
    return m_new, v_new, w_new


def solution(mesh):
    p = mesh.shape["outer"] * mesh.shape["inner"]

    def body(g_emb, g_qkv, g_o, g_w1, g_w2, g_bqkv, g_b1, g_dvec, m, v, w, lr, beta1, beta2, eps, step):
        grads = (g_emb, g_qkv, g_o, g_w1, g_w2, g_bqkv, g_b1, g_dvec)
        shapes = tuple(x.shape[1:] for x in grads)
        plan = Plan(shapes, p)
        n = len(plan.big)
        stored = [as_stored(x, nj) for x, (_, nj, _) in zip(grads, plan.big)]
        stored.append(grads[n].reshape(shapes[n]))
        stored += [x.reshape(2, -1, LANES).transpose(1, 0, 2).reshape(-1, LANES) for x in grads[n + 1:]]
        total = reduce_scatter(plan, stored).reshape(-1)
        r = lax.axis_index(AXES)
        offset = r * plan.shard - plan.start(r) * LANES
        g = lax.dynamic_slice(total, (offset,), (plan.shard,)) / p
        m_new, v_new, w_new = adam_update(g, m, v, w, lr, beta1, beta2, eps, step)
        front = max(i * plan.shard - plan.starts[i] * LANES for i in range(p))
        back = plan.window * LANES - plan.shard
        win = lax.dynamic_slice(jnp.pad(w_new, (front, back)), (front - offset,), (plan.window * LANES,))
        wb = all_gather(plan, win.reshape(plan.window, LANES))
        return (m_new, v_new, w_new) + restore(plan, wb, shapes)

    g3 = P(AXES, None, None)
    g4 = P(AXES, None, None, None)
    flat = P(AXES)
    rep = P()
    in_specs = (g3, g4, g4, g4, g4, g3, g3, g4, flat, flat, flat, rep, rep, rep, rep, rep)
    out_specs = (flat, flat, flat, rep, rep, rep, rep, rep, rep, rep, rep)
    return jax.shard_map(body, mesh=mesh, in_specs=in_specs, out_specs=out_specs, check_vma=False)
```

```python
import functools
import math

import jax
import jax.numpy as jnp
from jax import lax
from jax.experimental import pallas as pl
from jax.experimental.pallas import tpu as pltpu
from jax.sharding import PartitionSpec as P

AXES = ("outer", "inner")
MESH = pl.DeviceIdType.MESH
ANY = pl.BlockSpec(memory_space=pl.ANY)
LANES = 128
TILE = 16
SPLIT = 4
HALVES = 2
DEEP = 4
LEAD = 12
BF = jnp.bfloat16
F32 = jnp.float32


class Plan:
    def __init__(self, shapes, p):
        self.p = p
        self.sizes = [math.prod(s) for s in shapes]
        self.total = sum(self.sizes)
        self.shard = self.total // p
        self.big = []
        start = 0
        for s, n in zip(shapes, self.sizes):
            if s[-2] % TILE == 0:
                self.big.append((n // LANES, s[-1] // LANES, start // LANES))
                start += n
        self.small_row = start // LANES
        self.small_size = self.total - start
        self.starts, need = [], 0
        for r in range(p):
            self.starts.append(self.group(r * self.shard // LANES)[0])
            low, size = self.group(((r + 1) * self.shard - 1) // LANES)
            need = max(need, low + size - self.starts[r])
        step = 3 * HALVES * 3 * TILE
        self.window = -(-need // step) * step
        own = [b - a for a, b in zip(self.starts, self.starts[1:] + [self.total // LANES])]
        self.part = -(-max(own) // (3 * SPLIT * 8)) * 8
        self.sums = 3 * SPLIT * self.part
        self.piece = -(-max(own) // (3 * HALVES * TILE)) * TILE
        self.unit = HALVES * self.piece
        self.edge = max(8 * nj for _, nj, _ in self.big)
        self.small_rows = self.starts[p - 1] + self.sums - self.small_row

    def group(self, row):
        for n, nj, flat in self.big:
            if flat <= row < flat + n:
                size = 8 * nj
                return flat + (row - flat) // size * size, size
        return self.small_row + (row - self.small_row) // TILE * TILE, TILE

    def spans(self):
        spans = [(flat, flat + n) for n, _, flat in self.big]
        return spans + [(self.small_row, self.small_row + self.small_rows)]

    def crossing(self):
        out = {}
        for start in self.starts:
            for lo in range(start, start + self.sums, self.part):
                cuts = []
                for t, (x, y) in enumerate(self.spans()):
                    x, y = max(x, lo), min(y, lo + self.part)
                    if x < y:
                        cuts.append((t, x - self.spans()[t][0], y - x, x - lo))
                if len(cuts) > 1:
                    out[lo] = cuts
        return out

    def start(self, r):
        row = jnp.int32(self.starts[0])
        for i in range(1, self.p):
            row = jnp.where(r == i, jnp.int32(self.starts[i]), row)
        return row

    def segments(self, first):
        out = []
        for n, nj, flat in self.big:
            lo = jnp.maximum(first, flat)
            hi = jnp.minimum(first + self.window, flat + n)
            out.append((nj, lo - first, lax.div(jnp.maximum(hi - lo, 0), 8 * nj)))
        return out

    def sort(self, first, lo, hi, spill, move):
        for nj, row, groups in self.segments(first):
            size = 8 * nj
            more = size - 1 if spill else 0
            done, todo = [
                jnp.minimum(groups, lax.div(jnp.maximum(x - row, 0) + more, size)) if x else 0 for x in (lo, hi)
            ]

            def body(i, _, nj=nj, row=row, done=done, size=size):
                move(nj, pl.multiple_of(row + (done + i) * size, TILE))
                return 0

            lax.fori_loop(0, todo - done, body, 0)

    def pairs(self):
        flat, row, kept = [], 0, 0
        for n in self.sizes[len(self.big):]:
            flat.append((row, n // (2 * LANES)))
            row += n // LANES
        out = []
        for at, nj in flat[1:] + flat[:1]:
            out.append((at, kept, nj))
            kept += 2 * nj
        return out[-1:] + out[:-1]


def as_stored(x, nj):
    return x.reshape(-1, 8, nj, LANES).transpose(0, 2, 1, 3).reshape(-1, LANES)


def from_stored(x, nj, shape):
    return x.reshape(-1, nj, 8, LANES).transpose(0, 2, 1, 3).reshape(shape)


class Place:
    def __init__(self):
        o, i = lax.axis_index("outer"), lax.axis_index("inner")
        self.bits = [lax.div(o, 2), lax.rem(o, 2), lax.div(i, 2)]
        self.core = lax.rem(i, 2)

    def flipped(self, d):
        b = list(self.bits)
        b[d] = 1 - b[d]
        return (b[0] * 2 + b[1], b[2] * 2 + self.core)

    def partner(self):
        return (self.bits[0] * 2 + self.bits[1], self.bits[2] * 2 + 1 - self.core)

    def neighbour(self, k, n):
        d = lax.rem(k + n, 3)
        b = [jnp.where(d == i, 1 - x, x) for i, x in enumerate(self.bits)]
        return (b[0] * 2 + b[1], b[2] * 2 + self.core)

    def part(self, i):
        return lax.div(i, 3 * SPLIT), lax.rem(i, 3), lax.rem(i, 3 * SPLIT)

    def block(self, a, k, core):
        e = [1 - lax.div(a, 4), 1 - lax.rem(lax.div(a, 2), 2), 1 - lax.rem(a, 2)]
        r = core
        for d, weight in enumerate((8, 4, 2)):
            j = lax.rem(d - k + 3, 3)
            flip = jnp.where(j == 0, e[0], jnp.where(j == 1, e[1], e[2]))
            r = r + weight * (self.bits[d] + flip - 2 * self.bits[d] * flip)
        return r

    def owner(self, dims, e, core):
        b = list(self.bits)
        for d, flip in zip(dims, e):
            if flip:
                b[d] = 1 - b[d]
        return b[0] * 8 + b[1] * 4 + b[2] * 2 + core


def dims_of(k):
    return (k, (k + 1) % 3, (k + 2) % 3)


def arrive(place, others=()):
    barrier = pltpu.get_barrier_semaphore()
    for peer in [place.partner()] + [place.flipped(d) for d in range(3)] + list(others):
        pl.semaphore_signal(barrier, inc=1, device_id=peer, device_id_type=MESH)


def meet(peers):
    pl.semaphore_wait(pltpu.get_barrier_semaphore(), peers)


def remote(src, dst, send, recv, dev):
    return pltpu.make_async_remote_copy(
        src_ref=src, dst_ref=dst, send_sem=send, recv_sem=recv, device_id=dev, device_id_type=MESH
    )


def rs_kernel(plan, *refs):
    n_big = len(plan.big)
    n_in = n_big + len(plan.pairs())
    flat, late_ref = refs[n_in:n_in + 2]
    early, r1, r2, r3, own, oth, small, odd, edge = refs[n_in + 2:n_in + 11]
    own_sem, oth_sem, d_send, d_recv, s1_send, s1_recv, s2_send, s2_recv, s3_send, s3_recv, tiny_sem, edge_sem = refs[
        n_in + 11:
    ]
    xs = refs[:n_big] + (small,)
    part = plan.part
    wave = 3 * SPLIT
    early_n = 4 * wave
    place = Place()
    partner = place.partner()
    crossing = plan.crossing()

    def pick(i, core, issue):
        a, k, at = place.part(i)
        row = plan.start(place.block(a, k, core)) + at * part
        for t, (lo, hi) in enumerate(plan.spans()):

            @pl.when((row >= lo) & (row <= hi - part))
            def _(t=t, lo=lo):
                issue(xs[t].at[pl.ds(pl.multiple_of(row - lo, 8), part)], 0, part)

        for first, cuts in crossing.items():

            @pl.when(row == first)
            def _(cuts=cuts):
                for t, at, size, to in cuts:
                    issue(xs[t].at[pl.ds(at, size)], to, size)

    def swap(i):
        slot = i

        def issue(src, at, size):
            remote(src, early.at[slot, pl.ds(at, size)], d_send.at[slot], d_recv.at[slot], partner).start()

        pick(i, 1 - place.core, issue)

    def swap_late(i):
        slot = i

        def issue(src, at, size):
            remote(
                src, late_ref.at[slot, pl.ds(at, size)], d_send.at[early_n + slot], d_recv.at[early_n + slot], partner
            ).start()

        pick(early_n + i, 1 - place.core, issue)

    def swapped(slot):
        return remote(early.at[slot], early.at[slot], d_send.at[slot], d_recv.at[slot], partner)

    def swapped_late(slot):
        sems = d_send.at[early_n + slot], d_recv.at[early_n + slot]
        return remote(late_ref.at[slot], late_ref.at[slot], *sems, partner)

    def load(i):
        to = lax.rem(i, DEEP)

        def issue(src, at, size):
            pltpu.make_async_copy(src, own.at[to, pl.ds(at, size)], own_sem.at[to]).start()

        pick(i, place.core, issue)

    def loaded(i):
        to = lax.rem(i, DEEP)
        return pltpu.make_async_copy(late_ref.at[0], own.at[to], own_sem.at[to])

    def fetch(i):
        to = lax.rem(i, DEEP)
        return pltpu.make_async_copy(late_ref.at[i], oth.at[to], oth_sem.at[to])

    def hop(stage, k, slot):
        src, dst, send, recv, base = (
            (early, r1, s1_send, s1_recv, 0),
            (r1, r2, s2_send, s2_recv, 0),
            (r1, r3, s3_send, s3_recv, 2 * wave),
        )[stage]
        return remote(src.at[base + slot], dst.at[slot], send.at[slot], recv.at[slot], place.neighbour(k, stage))

    def add(dst, *srcs):
        step = 48

        def some(rows):
            total = dst[rows, :]
            for s in srcs:
                total = total + s[rows, :]
            dst[rows, :] = total

        def body(i, _):
            some(pl.ds(pl.multiple_of(i * step, 8), step))
            return 0

        lax.fori_loop(0, part // step, body, 0)
        if part % step:
            some(pl.ds(part - part % step, part % step))

    def loop(count, f):
        def body(i, _):
            f(i)
            return 0

        lax.fori_loop(0, count, body, 0)

    me = place.owner(dims_of(0), (0, 0, 0), place.core)
    after = lax.rem(me + 1, plan.p)
    arrive(place, [(lax.div(after, 4), lax.rem(after, 4))])
    copies = []
    for m, (x, (_, kept, nj)) in enumerate(zip(refs[n_big:n_in], plan.pairs())):
        dst = odd if m == 0 else small.at[pl.ds(kept, 2 * nj)]
        copies.append(pltpu.make_async_copy(x, dst, tiny_sem.at[m]))
        copies[-1].start()
    end = plan.small_size // LANES
    small[end:, :] = jnp.zeros((plan.small_rows - end, LANES), F32)
    for c in copies:
        c.wait()
    _, kept, nj = plan.pairs()[0]
    for j in range(nj):
        small[kept + 2 * j:kept + 2 * j + 2, :] = odd[:, j * LANES:(j + 1) * LANES]
    loop(DEEP, load)
    meet(5)
    loop(LEAD, swap)

    def first(i):
        k, slot = lax.rem(i, 3), i

        @pl.when(i + LEAD < early_n)
        def _():
            swap(i + LEAD)

        @pl.when(i + LEAD >= early_n)
        def _():
            swap_late(i + LEAD - early_n)

        loaded(i).wait()
        swapped(slot).wait_recv()
        add(early.at[slot], own.at[lax.rem(i, DEEP)])
        hop(0, k, slot).start()
        load(i + DEEP)

    loop(early_n, first)

    def prefetch(i):
        swapped_late(i).wait_recv()
        fetch(i).start()

    loop(DEEP, prefetch)

    def second(i):
        k, slot = lax.rem(i, 3), i

        @pl.when(i + LEAD < early_n)
        def _():
            swap_late(i + LEAD)

        to = lax.rem(i, DEEP)
        loaded(i).wait()
        fetch(i).wait()
        hop(0, k, slot).wait_recv()
        add(r1.at[slot], own.at[to], oth.at[to])

        @pl.when(i < 2 * wave)
        def _():
            hop(1, k, slot).start()

        @pl.when(i + DEEP < early_n)
        def _():
            load(early_n + i + DEEP)
            prefetch(i + DEEP)

    loop(early_n, second)

    def third(i):
        k, slot = lax.rem(i, 3), i
        hop(1, k, slot).wait_recv()
        add(r1.at[2 * wave + slot], r2.at[slot])

        @pl.when(i < wave)
        def _():
            hop(2, k, slot).start()

    loop(2 * wave, third)

    first_row = plan.start(me)
    stored = r1.at[pl.ds(3 * wave, wave + 1)].reshape((wave + 1) * part, LANES)
    before = lax.rem(me + plan.p - 1, plan.p)
    passed = remote(
        r1.at[3 * wave, pl.ds(0, plan.edge)], edge, edge_sem.at[0], edge_sem.at[1],
        (lax.div(before, 4), lax.rem(before, 4)),
    )

    def move(nj, base):
        for j in range(nj):
            flat[pl.ds(base + j, 8, stride=nj), :] = stored[pl.ds(base + j * 8, 8), :]

    for s in range(SPLIT):

        def fourth(j, s=s):
            slot = 3 * s + j
            hop(2, j, slot).wait_recv()
            add(r1.at[3 * wave + slot], r3.at[slot])

        loop(3, fourth)
        if s == 0:
            passed.start()
        if s == SPLIT - 1:
            passed.wait_recv()
            gap = jnp.where(me == plan.p - 1, plan.sums, plan.start(after) - first_row)
            for i in range(0, plan.edge, TILE):
                stored[pl.ds(pl.multiple_of(gap + i, TILE if plan.sums % TILE == 0 else 8), TILE), :] = edge[i:i + TILE, :]
        end = 3 * (s + 1) * part if s < SPLIT - 1 else plan.window
        plan.sort(first_row, 3 * s * part, end, False, move)

    @pl.when(me == plan.p - 1)
    def _():
        base = plan.small_row - plan.starts[plan.p - 1]
        for row, kept, nj in plan.pairs():
            for layer in range(2):
                flat[pl.ds(base + row + layer * nj, nj), :] = stored[pl.ds(base + kept + layer, nj, stride=2), :]

    passed.wait_send()

    def sent(i):
        k, slot = lax.rem(i, 3), i
        swapped(slot).wait_send()
        swapped_late(slot).wait_send()
        hop(0, k, slot).wait_send()

        @pl.when(i < 2 * wave)
        def _():
            hop(1, k, slot).wait_send()

        @pl.when(i < wave)
        def _():
            hop(2, k, slot).wait_send()

    loop(early_n, sent)


def reduce_scatter(plan, xs):
    dma = pltpu.SemaphoreType.DMA
    wave = 3 * SPLIT
    slots = [4 * wave, 4 * wave + 1, 2 * wave, wave, DEEP, DEEP]
    used = (sum(slots) * plan.part * LANES * 4 >> 20) + 2
    g, _ = pl.pallas_call(
        functools.partial(rs_kernel, plan),
        out_shape=(
            pltpu.VMEM((plan.window, LANES), F32),
            jax.ShapeDtypeStruct((4 * wave, plan.part, LANES), F32),
        ),
        in_specs=[ANY] * len(xs),
        out_specs=(pl.BlockSpec(memory_space=pltpu.VMEM), ANY),
        scratch_shapes=[pltpu.VMEM((n, plan.part, LANES), F32) for n in slots]
        + [pltpu.VMEM((plan.small_rows, LANES), F32), pltpu.VMEM(xs[len(plan.big)].shape, F32)]
        + [pltpu.VMEM((plan.edge, LANES), F32)]
        + [dma((DEEP,)), dma((DEEP,))]
        + [dma((n * wave,)) for n in (8, 8, 4, 4, 2, 2, 1, 1)]
        + [dma((len(plan.pairs()),)), dma((2,))],
        compiler_params=pltpu.CompilerParams(
            collective_id=0, has_side_effects=True, vmem_limit_bytes=used << 20
        ),
        name="reduce_scatter",
    )(*xs)
    return g


def ag_kernel(plan, values, *refs):
    w_refs, (win, tiny, edge, s_send, s_recv, d_send, d_recv, edge_sem) = refs[:3], refs[3:]
    part, unit = plan.piece, plan.unit
    place = Place()
    partner = place.partner()
    here = (0, 0, 0)
    me = place.owner(dims_of(0), here, place.core)
    after, before = lax.rem(me + 1, plan.p), lax.rem(me + plan.p - 1, plan.p)
    arrive(place, [(lax.div(before, 4), lax.rem(before, 4))])

    first_row = plan.start(me)

    def move(nj, base):
        for j in range(0, nj, 2):
            pair = [values[pl.ds(base + j + h, 8, stride=nj), :] for h in range(2)]
            win[pl.ds(base + j * 8, TILE), :] = jnp.concatenate(pair, axis=0).astype(BF)

    @pl.when(me == plan.p - 1)
    def _():
        base = plan.small_row - plan.starts[plan.p - 1]
        tiny[...] = jnp.zeros_like(tiny)
        for row, kept, nj in plan.pairs():
            for layer in range(2):
                tiny[pl.ds(kept + layer, nj, stride=2), :] = values[pl.ds(base + row + layer * nj, nj), :]
        win[pl.ds(base, tiny.shape[0]), :] = tiny[...].astype(BF)

    def rows_of(k, e, s, core):
        row = place.owner(dims_of(k), e, core) * unit + s * part
        return w_refs[k].at[pl.ds(pl.multiple_of(row, TILE), part)]

    slot = {here: 0, (1, 0, 0): 1, (0, 1, 0): 2, (0, 0, 1): 3, (1, 1, 0): 4, (1, 0, 1): 5, (0, 1, 1): 6, (1, 1, 1): 7}

    def index(k, e, s):
        return (slot[e] * 3 + k) * HALVES + s

    def src(k, e, s):
        return win.at[pl.ds((3 * s + k) * part, part)] if e == here else rows_of(k, e, s, place.core)

    sent = []

    def send(k, e, s, n):
        there = list(e)
        there[n] = 1
        i = index(k, tuple(there), s)
        copy = remote(
            src(k, e, s), rows_of(k, e, s, place.core), s_send.at[i], s_recv.at[i], place.flipped(dims_of(k)[n])
        )
        copy.start()
        sent.append(copy)

    def share(k, e, s):
        i = index(k, e, s)
        copy = remote(src(k, e, s), rows_of(k, e, s, place.core), d_send.at[i], d_recv.at[i], partner)
        copy.start()
        sent.append(copy)

    def arrival(k, e, s):
        i, dst = index(k, e, s), rows_of(k, e, s, place.core)
        return remote(dst, dst, s_send.at[i], s_recv.at[i], partner)

    def shared(k, e, s):
        i, dst = index(k, e, s), rows_of(k, e, s, 1 - place.core)
        return remote(dst, dst, d_send.at[i], d_recv.at[i], partner)

    gap = jnp.where(me == plan.p - 1, 3 * plan.unit, plan.start(after) - first_row)
    passed = remote(
        win.at[pl.ds(pl.multiple_of(gap, TILE), plan.edge)], edge, edge_sem.at[0], edge_sem.at[1],
        (lax.div(after, 4), lax.rem(after, 4)),
    )
    for s in reversed(range(HALVES)):
        end = 3 * (s + 1) * part if s < HALVES - 1 else plan.window
        plan.sort(first_row, 3 * s * part, end, False, move)
        if s == HALVES - 1:
            meet(5)
            passed.start()
        if s == 0:
            passed.wait_recv()
            for r in range(1, plan.p):

                @pl.when(me == r)
                def _(r=r):
                    size = plan.group(plan.starts[r])[1]
                    nj, shape = size // 8, (size, LANES)
                    row, lane = (lax.broadcasted_iota(jnp.int32, shape, d) for d in range(2))
                    at = (lax.rem(row, 8) * nj + lax.div(row, 8)) * LANES + lane
                    cut = r * plan.shard - plan.starts[r] * LANES
                    rows = pl.ds(0, size)
                    merged = jnp.where(at < cut, edge[rows, :].astype(F32), win[rows, :].astype(F32))
                    win[rows, :] = merged.astype(BF)

        for n in range(3):
            for k in range(3):
                send(k, here, s, n)
    for s in range(HALVES):
        for k in range(3):
            share(k, here, s)
    rows = TILE
    for s in range(HALVES):
        for k in range(3):

            def keep(i, _, k=k, s=s):
                at = pl.multiple_of(i * rows, rows)
                to = pl.ds(pl.multiple_of(me * unit + s * part + at, TILE), rows)
                w_refs[k][to, :] = win[pl.ds((3 * s + k) * part + at, rows), :]
                return 0

            lax.fori_loop(0, part // rows, keep, 0)
    for e in list(slot)[1:]:
        for s in reversed(range(HALVES)):
            for k in range(3):
                arrival(k, e, s).wait_recv()
                for n in range(1, 3):
                    if not any(e[n:]):
                        send(k, e, s, n)
                share(k, e, s)
    for e in slot:
        for s in range(HALVES):
            for k in range(3):
                shared(k, e, s).wait_recv()
    for copy in sent:
        copy.wait_send()

    passed.wait_send()


def all_gather(plan, win):
    dma = pltpu.SemaphoreType.DMA
    n = 8 * 3 * HALVES
    return pl.pallas_call(
        functools.partial(ag_kernel, plan),
        out_shape=[pltpu.VMEM((plan.p * plan.unit, LANES), BF)] * 3,
        in_specs=[pl.BlockSpec(memory_space=pltpu.VMEM)],
        out_specs=[pl.BlockSpec(memory_space=pltpu.VMEM)] * 3,
        scratch_shapes=[pltpu.VMEM((3 * plan.unit + plan.edge, LANES), BF), pltpu.VMEM((small_rows(plan), LANES), F32)]
        + [pltpu.VMEM((plan.edge, LANES), BF)]
        + [dma((n,))] * 4
        + [dma((2,))],
        compiler_params=pltpu.CompilerParams(collective_id=1, has_side_effects=True, vmem_limit_bytes=8 << 20),
        name="all_gather",
    )(win)


def small_rows(plan):
    return -(-plan.small_size // (LANES * TILE)) * TILE


def restore_kernel(plan, *refs):
    w_refs, outs, out_sem = refs[:3], refs[3:-1], refs[-1]
    p, part = plan.p, plan.piece
    copies = []

    def copy(r, x, y, dst):
        for n in range(x // part, -(-y // part)):
            lo, hi = max(x, n * part), min(y, (n + 1) * part)
            src = w_refs[n % 3].at[pl.ds(r * plan.unit + n // 3 * part + lo - n * part, hi - lo)]
            copies.append(pltpu.make_async_copy(src, dst(lo - x, hi - lo), out_sem.at[len(copies)]))

    for r in range(p):
        lo = plan.starts[r]
        hi = plan.starts[r + 1] if r + 1 < p else plan.small_row
        for t, (a, b) in enumerate(plan.spans()[:-1]):
            x, y = max(a, lo), min(b, hi)
            if x < y:
                copy(r, x - lo, y - lo, lambda at, size, t=t, x=x, a=a: outs[t].at[pl.ds(x - a + at, size)])
    base = plan.small_row - plan.starts[p - 1]
    for out, (_, kept, nj) in zip(outs[len(plan.big):], plan.pairs()):
        copy(p - 1, base + kept, base + kept + out.shape[0], lambda at, size, out=out: out.at[pl.ds(at, size)])
    for c in copies:
        c.start()
    for c in copies:
        c.wait()


def restore(plan, gathered, shapes):
    n = len(plan.big)
    dma = pltpu.SemaphoreType.DMA
    outs = pl.pallas_call(
        functools.partial(restore_kernel, plan),
        out_shape=[jax.ShapeDtypeStruct((rows, LANES), BF) for rows, _, _ in plan.big]
        + [jax.ShapeDtypeStruct((2 * nj if m else -(-2 * nj // TILE) * TILE, LANES), BF)
           for m, (_, _, nj) in enumerate(plan.pairs())],
        in_specs=[ANY] * 3,
        out_specs=[ANY] * len(shapes),
        scratch_shapes=[dma((3 * HALVES * plan.p + 3 * n,))],
        compiler_params=pltpu.CompilerParams(vmem_limit_bytes=1 << 20),
        name="restore",
    )(*gathered)
    result = [from_stored(x, nj, s) for x, (_, nj, _), s in zip(outs, plan.big, shapes)]
    for x, (_, _, nj), s in zip(outs[n:], plan.pairs(), shapes[n:]):
        result.append(x[:2 * nj].reshape(nj, 2, LANES).transpose(1, 0, 2).reshape(s))
    return tuple(result)


def adam_update(g, m, v, w, lr, beta1, beta2, eps, step):
    t = step.astype(jnp.float32)
    m_new = beta1 * m + (1.0 - beta1) * g
    v_new = beta2 * v + (1.0 - beta2) * (g * g)
    m_hat = m_new * (1.0 / (1.0 - beta1 ** t))
    v_hat = v_new * (1.0 / (1.0 - beta2 ** t))
    w_new = w - lr * m_hat / (jnp.sqrt(v_hat) + eps)
    return m_new, v_new, w_new


def solution(mesh):
    p = mesh.shape["outer"] * mesh.shape["inner"]

    def body(g_emb, g_qkv, g_o, g_w1, g_w2, g_bqkv, g_b1, g_dvec, m, v, w, lr, beta1, beta2, eps, step):
        grads = (g_emb, g_qkv, g_o, g_w1, g_w2, g_bqkv, g_b1, g_dvec)
        shapes = tuple(x.shape[1:] for x in grads)
        plan = Plan(shapes, p)
        n = len(plan.big)
        stored = [as_stored(x, nj) for x, (_, nj, _) in zip(grads, plan.big)]
        stored.append(grads[n].reshape(shapes[n]))
        stored += [x.reshape(2, -1, LANES).transpose(1, 0, 2).reshape(-1, LANES) for x in grads[n + 1:]]
        total = reduce_scatter(plan, stored).reshape(-1)
        r = lax.axis_index(AXES)
        offset = r * plan.shard - plan.start(r) * LANES
        g = lax.dynamic_slice(total, (offset,), (plan.shard,)) / p
        m_new, v_new, w_new = adam_update(g, m, v, w, lr, beta1, beta2, eps, step)
        front = max(i * plan.shard - plan.starts[i] * LANES for i in range(p))
        back = plan.window * LANES - plan.shard
        win = lax.dynamic_slice(jnp.pad(w_new, (front, back)), (front - offset,), (plan.window * LANES,))
        wb = all_gather(plan, win.reshape(plan.window, LANES))
        return (m_new, v_new, w_new) + restore(plan, wb, shapes)

    g3 = P(AXES, None, None)
    g4 = P(AXES, None, None, None)
    flat = P(AXES)
    rep = P()
    in_specs = (g3, g4, g4, g4, g4, g3, g3, g4, flat, flat, flat, rep, rep, rep, rep, rep)
    out_specs = (flat, flat, flat, rep, rep, rep, rep, rep, rep, rep, rep)
    return jax.shard_map(body, mesh=mesh, in_specs=in_specs, out_specs=out_specs, check_vma=False)
```

```python
import functools
import math

import jax
import jax.numpy as jnp
from jax import lax
from jax.experimental import pallas as pl
from jax.experimental.pallas import tpu as pltpu
from jax.sharding import PartitionSpec as P

AXES = ("outer", "inner")
MESH = pl.DeviceIdType.MESH
ANY = pl.BlockSpec(memory_space=pl.ANY)
LANES = 128
TILE = 16
SPLIT = 4
HALVES = 2
DEEP = 4
LEAD = 12
BF = jnp.bfloat16
F32 = jnp.float32


class Plan:
    def __init__(self, shapes, p):
        self.p = p
        self.sizes = [math.prod(s) for s in shapes]
        self.total = sum(self.sizes)
        self.shard = self.total // p
        self.big = []
        start = 0
        for s, n in zip(shapes, self.sizes):
            if s[-2] % TILE == 0:
                self.big.append((n // LANES, s[-1] // LANES, start // LANES))
                start += n
        self.small_row = start // LANES
        self.small_size = self.total - start
        self.starts, need = [], 0
        for r in range(p):
            self.starts.append(self.group(r * self.shard // LANES)[0])
            low, size = self.group(((r + 1) * self.shard - 1) // LANES)
            need = max(need, low + size - self.starts[r])
        step = 3 * HALVES * 3 * TILE
        self.window = -(-need // step) * step
        own = [b - a for a, b in zip(self.starts, self.starts[1:] + [self.total // LANES])]
        self.part = -(-max(own) // (3 * SPLIT * 8)) * 8
        self.sums = 3 * SPLIT * self.part
        self.piece = -(-max(own) // (3 * HALVES * TILE)) * TILE
        self.unit = HALVES * self.piece
        self.edge = max(8 * nj for _, nj, _ in self.big)
        self.small_rows = self.starts[p - 1] + self.sums - self.small_row

    def group(self, row):
        for n, nj, flat in self.big:
            if flat <= row < flat + n:
                size = 8 * nj
                return flat + (row - flat) // size * size, size
        return self.small_row + (row - self.small_row) // TILE * TILE, TILE

    def spans(self):
        spans = [(flat, flat + n) for n, _, flat in self.big]
        return spans + [(self.small_row, self.small_row + self.small_rows)]

    def crossing(self):
        out = {}
        for start in self.starts:
            for lo in range(start, start + self.sums, self.part):
                cuts = []
                for t, (x, y) in enumerate(self.spans()):
                    x, y = max(x, lo), min(y, lo + self.part)
                    if x < y:
                        cuts.append((t, x - self.spans()[t][0], y - x, x - lo))
                if len(cuts) > 1:
                    out[lo] = cuts
        return out

    def start(self, r):
        row = jnp.int32(self.starts[0])
        for i in range(1, self.p):
            row = jnp.where(r == i, jnp.int32(self.starts[i]), row)
        return row

    def segments(self, first):
        out = []
        for n, nj, flat in self.big:
            lo = jnp.maximum(first, flat)
            hi = jnp.minimum(first + self.window, flat + n)
            out.append((nj, lo - first, lax.div(jnp.maximum(hi - lo, 0), 8 * nj)))
        return out

    def sort(self, first, lo, hi, spill, move):
        for nj, row, groups in self.segments(first):
            size = 8 * nj
            more = size - 1 if spill else 0
            done, todo = [
                jnp.minimum(groups, lax.div(jnp.maximum(x - row, 0) + more, size)) if x else 0 for x in (lo, hi)
            ]

            def body(i, _, nj=nj, row=row, done=done, size=size):
                move(nj, pl.multiple_of(row + (done + i) * size, TILE))
                return 0

            lax.fori_loop(0, todo - done, body, 0)

    def pairs(self):
        flat, row, kept = [], 0, 0
        for n in self.sizes[len(self.big):]:
            flat.append((row, n // (2 * LANES)))
            row += n // LANES
        out = []
        for at, nj in flat[1:] + flat[:1]:
            out.append((at, kept, nj))
            kept += 2 * nj
        return out[-1:] + out[:-1]


def as_stored(x, nj):
    return x.reshape(-1, 8, nj, LANES).transpose(0, 2, 1, 3).reshape(-1, LANES)


def from_stored(x, nj, shape):
    return x.reshape(-1, nj, 8, LANES).transpose(0, 2, 1, 3).reshape(shape)


class Place:
    def __init__(self):
        o, i = lax.axis_index("outer"), lax.axis_index("inner")
        self.bits = [lax.div(o, 2), lax.rem(o, 2), lax.div(i, 2)]
        self.core = lax.rem(i, 2)

    def flipped(self, d):
        b = list(self.bits)
        b[d] = 1 - b[d]
        return (b[0] * 2 + b[1], b[2] * 2 + self.core)

    def partner(self):
        return (self.bits[0] * 2 + self.bits[1], self.bits[2] * 2 + 1 - self.core)

    def neighbour(self, k, n):
        d = lax.rem(k + n, 3)
        b = [jnp.where(d == i, 1 - x, x) for i, x in enumerate(self.bits)]
        return (b[0] * 2 + b[1], b[2] * 2 + self.core)

    def part(self, i):
        return lax.div(i, 3 * SPLIT), lax.rem(i, 3), lax.rem(i, 3 * SPLIT)

    def block(self, a, k, core):
        e = [1 - lax.div(a, 4), 1 - lax.rem(lax.div(a, 2), 2), 1 - lax.rem(a, 2)]
        r = core
        for d, weight in enumerate((8, 4, 2)):
            j = lax.rem(d - k + 3, 3)
            flip = jnp.where(j == 0, e[0], jnp.where(j == 1, e[1], e[2]))
            r = r + weight * (self.bits[d] + flip - 2 * self.bits[d] * flip)
        return r

    def owner(self, dims, e, core):
        b = list(self.bits)
        for d, flip in zip(dims, e):
            if flip:
                b[d] = 1 - b[d]
        return b[0] * 8 + b[1] * 4 + b[2] * 2 + core


def dims_of(k):
    return (k, (k + 1) % 3, (k + 2) % 3)


def arrive(place, others=()):
    barrier = pltpu.get_barrier_semaphore()
    for peer in [place.partner()] + [place.flipped(d) for d in range(3)] + list(others):
        pl.semaphore_signal(barrier, inc=1, device_id=peer, device_id_type=MESH)


def meet(peers):
    pl.semaphore_wait(pltpu.get_barrier_semaphore(), peers)


def remote(src, dst, send, recv, dev):
    return pltpu.make_async_remote_copy(
        src_ref=src, dst_ref=dst, send_sem=send, recv_sem=recv, device_id=dev, device_id_type=MESH
    )


def rs_kernel(plan, *refs):
    n_big = len(plan.big)
    n_in = n_big + len(plan.pairs())
    flat, late_ref = refs[n_in:n_in + 2]
    early, r1, r2, r3, own, oth, small, odd, edge = refs[n_in + 2:n_in + 11]
    own_sem, oth_sem, d_send, d_recv, s1_send, s1_recv, s2_send, s2_recv, s3_send, s3_recv, tiny_sem, edge_sem = refs[
        n_in + 11:
    ]
    xs = refs[:n_big] + (small,)
    part = plan.part
    wave = 3 * SPLIT
    early_n = 4 * wave
    place = Place()
    partner = place.partner()
    crossing = plan.crossing()

    def pick(i, core, issue):
        a, k, at = place.part(i)
        row = plan.start(place.block(a, k, core)) + at * part
        for t, (lo, hi) in enumerate(plan.spans()):

            @pl.when((row >= lo) & (row <= hi - part))
            def _(t=t, lo=lo):
                issue(xs[t].at[pl.ds(pl.multiple_of(row - lo, 8), part)], 0, part)

        for first, cuts in crossing.items():

            @pl.when(row == first)
            def _(cuts=cuts):
                for t, at, size, to in cuts:
                    issue(xs[t].at[pl.ds(at, size)], to, size)

    def swap(i):
        slot = i

        def issue(src, at, size):
            remote(src, early.at[slot, pl.ds(at, size)], d_send.at[slot], d_recv.at[slot], partner).start()

        pick(i, 1 - place.core, issue)

    def swap_late(i):
        slot = i

        def issue(src, at, size):
            remote(
                src, late_ref.at[slot, pl.ds(at, size)], d_send.at[early_n + slot], d_recv.at[early_n + slot], partner
            ).start()

        pick(early_n + i, 1 - place.core, issue)

    def swapped(slot):
        return remote(early.at[slot], early.at[slot], d_send.at[slot], d_recv.at[slot], partner)

    def swapped_late(slot):
        sems = d_send.at[early_n + slot], d_recv.at[early_n + slot]
        return remote(late_ref.at[slot], late_ref.at[slot], *sems, partner)

    def load(i):
        to = lax.rem(i, DEEP)

        def issue(src, at, size):
            pltpu.make_async_copy(src, own.at[to, pl.ds(at, size)], own_sem.at[to]).start()

        pick(i, place.core, issue)

    def loaded(i):
        to = lax.rem(i, DEEP)
        return pltpu.make_async_copy(late_ref.at[0], own.at[to], own_sem.at[to])

    def fetch(i):
        to = lax.rem(i, DEEP)
        return pltpu.make_async_copy(late_ref.at[i], oth.at[to], oth_sem.at[to])

    def hop(stage, k, slot):
        src, dst, send, recv, base = (
            (early, r1, s1_send, s1_recv, 0),
            (r1, r2, s2_send, s2_recv, 0),
            (r1, r3, s3_send, s3_recv, 2 * wave),
        )[stage]
        return remote(src.at[base + slot], dst.at[slot], send.at[slot], recv.at[slot], place.neighbour(k, stage))

    def add(dst, *srcs):
        step = 48

        def some(rows):
            total = dst[rows, :]
            for s in srcs:
                total = total + s[rows, :]
            dst[rows, :] = total

        def body(i, _):
            some(pl.ds(pl.multiple_of(i * step, 8), step))
            return 0

        lax.fori_loop(0, part // step, body, 0)
        if part % step:
            some(pl.ds(part - part % step, part % step))

    def loop(count, f):
        def body(i, _):
            f(i)
            return 0

        lax.fori_loop(0, count, body, 0)

    me = place.owner(dims_of(0), (0, 0, 0), place.core)
    after = lax.rem(me + 1, plan.p)
    arrive(place, [(lax.div(after, 4), lax.rem(after, 4))])
    copies = []
    for m, (x, (_, kept, nj)) in enumerate(zip(refs[n_big:n_in], plan.pairs())):
        dst = odd if m == 0 else small.at[pl.ds(kept, 2 * nj)]
        copies.append(pltpu.make_async_copy(x, dst, tiny_sem.at[m]))
        copies[-1].start()
    end = plan.small_size // LANES
    small[end:, :] = jnp.zeros((plan.small_rows - end, LANES), F32)
    for c in copies:
        c.wait()
    _, kept, nj = plan.pairs()[0]
    for j in range(nj):
        small[kept + 2 * j:kept + 2 * j + 2, :] = odd[:, j * LANES:(j + 1) * LANES]
    loop(DEEP, load)
    meet(5)
    loop(LEAD, swap)

    def first(i):
        k, slot = lax.rem(i, 3), i

        @pl.when(i + LEAD < early_n)
        def _():
            swap(i + LEAD)

        @pl.when(i + LEAD >= early_n)
        def _():
            swap_late(i + LEAD - early_n)

        loaded(i).wait()
        swapped(slot).wait_recv()
        add(early.at[slot], own.at[lax.rem(i, DEEP)])
        hop(0, k, slot).start()
        load(i + DEEP)

    loop(early_n, first)

    def prefetch(i):
        swapped_late(i).wait_recv()
        fetch(i).start()

    loop(DEEP, prefetch)

    def second(i):
        k, slot = lax.rem(i, 3), i

        @pl.when(i + LEAD < early_n)
        def _():
            swap_late(i + LEAD)

        to = lax.rem(i, DEEP)
        loaded(i).wait()
        fetch(i).wait()
        hop(0, k, slot).wait_recv()
        add(r1.at[slot], own.at[to], oth.at[to])

        @pl.when(i < 2 * wave)
        def _():
            hop(1, k, slot).start()

        @pl.when(i + DEEP < early_n)
        def _():
            load(early_n + i + DEEP)
            prefetch(i + DEEP)

    loop(early_n, second)

    def third(i):
        k, slot = lax.rem(i, 3), i
        hop(1, k, slot).wait_recv()
        add(r1.at[2 * wave + slot], r2.at[slot])

        @pl.when(i < wave)
        def _():
            hop(2, k, slot).start()

    loop(2 * wave, third)

    first_row = plan.start(me)
    stored = r1.at[pl.ds(3 * wave, wave + 1)].reshape((wave + 1) * part, LANES)
    before = lax.rem(me + plan.p - 1, plan.p)
    passed = remote(
        r1.at[3 * wave, pl.ds(0, plan.edge)], edge, edge_sem.at[0], edge_sem.at[1],
        (lax.div(before, 4), lax.rem(before, 4)),
    )

    def move(nj, base):
        for j in range(nj):
            flat[pl.ds(base + j, 8, stride=nj), :] = stored[pl.ds(base + j * 8, 8), :]

    for s in range(SPLIT):

        def fourth(j, s=s):
            slot = 3 * s + j
            hop(2, j, slot).wait_recv()
            add(r1.at[3 * wave + slot], r3.at[slot])

        loop(3, fourth)
        if s == 0:
            passed.start()
        if s == SPLIT - 1:
            passed.wait_recv()
            gap = jnp.where(me == plan.p - 1, plan.sums, plan.start(after) - first_row)
            for i in range(0, plan.edge, TILE):
                stored[pl.ds(pl.multiple_of(gap + i, TILE if plan.sums % TILE == 0 else 8), TILE), :] = edge[i:i + TILE, :]
        end = 3 * (s + 1) * part if s < SPLIT - 1 else plan.window
        plan.sort(first_row, 3 * s * part, end, False, move)

    @pl.when(me == plan.p - 1)
    def _():
        base = plan.small_row - plan.starts[plan.p - 1]
        for row, kept, nj in plan.pairs():
            for layer in range(2):
                flat[pl.ds(base + row + layer * nj, nj), :] = stored[pl.ds(base + kept + layer, nj, stride=2), :]

    passed.wait_send()

    def sent(i):
        k, slot = lax.rem(i, 3), i
        swapped(slot).wait_send()
        swapped_late(slot).wait_send()
        hop(0, k, slot).wait_send()

        @pl.when(i < 2 * wave)
        def _():
            hop(1, k, slot).wait_send()

        @pl.when(i < wave)
        def _():
            hop(2, k, slot).wait_send()

    loop(early_n, sent)


def reduce_scatter(plan, xs):
    dma = pltpu.SemaphoreType.DMA
    wave = 3 * SPLIT
    slots = [4 * wave, 4 * wave + 1, 2 * wave, wave, DEEP, DEEP]
    used = (sum(slots) * plan.part * LANES * 4 >> 20) + 2
    g, _ = pl.pallas_call(
        functools.partial(rs_kernel, plan),
        out_shape=(
            pltpu.VMEM((plan.window, LANES), F32),
            jax.ShapeDtypeStruct((4 * wave, plan.part, LANES), F32),
        ),
        in_specs=[ANY] * len(xs),
        out_specs=(pl.BlockSpec(memory_space=pltpu.VMEM), ANY),
        scratch_shapes=[pltpu.VMEM((n, plan.part, LANES), F32) for n in slots]
        + [pltpu.VMEM((plan.small_rows, LANES), F32), pltpu.VMEM(xs[len(plan.big)].shape, F32)]
        + [pltpu.VMEM((plan.edge, LANES), F32)]
        + [dma((DEEP,)), dma((DEEP,))]
        + [dma((n * wave,)) for n in (8, 8, 4, 4, 2, 2, 1, 1)]
        + [dma((len(plan.pairs()),)), dma((2,))],
        compiler_params=pltpu.CompilerParams(
            collective_id=0, has_side_effects=True, vmem_limit_bytes=used << 20
        ),
        name="reduce_scatter",
    )(*xs)
    return g


def ag_kernel(plan, values, *refs):
    w_refs, (win, tiny, edge, s_send, s_recv, d_send, d_recv, edge_sem) = refs[:3], refs[3:]
    part, unit = plan.piece, plan.unit
    place = Place()
    partner = place.partner()
    here = (0, 0, 0)
    me = place.owner(dims_of(0), here, place.core)
    after, before = lax.rem(me + 1, plan.p), lax.rem(me + plan.p - 1, plan.p)
    arrive(place, [(lax.div(before, 4), lax.rem(before, 4))])

    first_row = plan.start(me)

    def move(nj, base):
        for j in range(0, nj, 2):
            pair = [values[pl.ds(base + j + h, 8, stride=nj), :] for h in range(2)]
            win[pl.ds(base + j * 8, TILE), :] = jnp.concatenate(pair, axis=0).astype(BF)

    @pl.when(me == plan.p - 1)
    def _():
        base = plan.small_row - plan.starts[plan.p - 1]
        tiny[...] = jnp.zeros_like(tiny)
        for row, kept, nj in plan.pairs():
            for layer in range(2):
                tiny[pl.ds(kept + layer, nj, stride=2), :] = values[pl.ds(base + row + layer * nj, nj), :]
        win[pl.ds(base, tiny.shape[0]), :] = tiny[...].astype(BF)

    def rows_of(k, e, s, core):
        row = place.owner(dims_of(k), e, core) * unit + s * part
        return w_refs[k].at[pl.ds(pl.multiple_of(row, TILE), part)]

    slot = {here: 0, (1, 0, 0): 1, (0, 1, 0): 2, (0, 0, 1): 3, (1, 1, 0): 4, (1, 0, 1): 5, (0, 1, 1): 6, (1, 1, 1): 7}

    def index(k, e, s):
        return (slot[e] * 3 + k) * HALVES + s

    def src(k, e, s):
        return win.at[pl.ds((3 * s + k) * part, part)] if e == here else rows_of(k, e, s, place.core)

    sent = []

    def send(k, e, s, n):
        there = list(e)
        there[n] = 1
        i = index(k, tuple(there), s)
        copy = remote(
            src(k, e, s), rows_of(k, e, s, place.core), s_send.at[i], s_recv.at[i], place.flipped(dims_of(k)[n])
        )
        copy.start()
        sent.append(copy)

    def share(k, e, s):
        i = index(k, e, s)
        copy = remote(src(k, e, s), rows_of(k, e, s, place.core), d_send.at[i], d_recv.at[i], partner)
        copy.start()
        sent.append(copy)

    def arrival(k, e, s):
        i, dst = index(k, e, s), rows_of(k, e, s, place.core)
        return remote(dst, dst, s_send.at[i], s_recv.at[i], partner)

    def shared(k, e, s):
        i, dst = index(k, e, s), rows_of(k, e, s, 1 - place.core)
        return remote(dst, dst, d_send.at[i], d_recv.at[i], partner)

    gap = jnp.where(me == plan.p - 1, 3 * plan.unit, plan.start(after) - first_row)
    passed = remote(
        win.at[pl.ds(pl.multiple_of(gap, TILE), plan.edge)], edge, edge_sem.at[0], edge_sem.at[1],
        (lax.div(after, 4), lax.rem(after, 4)),
    )
    for s in reversed(range(HALVES)):
        end = 3 * (s + 1) * part if s < HALVES - 1 else plan.window
        plan.sort(first_row, 3 * s * part, end, False, move)
        if s == HALVES - 1:
            meet(5)
            passed.start()
        if s == 0:
            passed.wait_recv()
            for r in range(1, plan.p):

                @pl.when(me == r)
                def _(r=r):
                    size = plan.group(plan.starts[r])[1]
                    nj, shape = size // 8, (size, LANES)
                    row, lane = (lax.broadcasted_iota(jnp.int32, shape, d) for d in range(2))
                    at = (lax.rem(row, 8) * nj + lax.div(row, 8)) * LANES + lane
                    cut = r * plan.shard - plan.starts[r] * LANES
                    rows = pl.ds(0, size)
                    merged = jnp.where(at < cut, edge[rows, :].astype(F32), win[rows, :].astype(F32))
                    win[rows, :] = merged.astype(BF)

        for n in range(3):
            for k in range(3):
                send(k, here, s, n)
    for s in range(HALVES):
        for k in range(3):
            share(k, here, s)
    rows = TILE
    for s in range(HALVES):
        for k in range(3):

            def keep(i, _, k=k, s=s):
                at = pl.multiple_of(i * rows, rows)
                to = pl.ds(pl.multiple_of(me * unit + s * part + at, TILE), rows)
                w_refs[k][to, :] = win[pl.ds((3 * s + k) * part + at, rows), :]
                return 0

            lax.fori_loop(0, part // rows, keep, 0)
    for e in list(slot)[1:]:
        for s in reversed(range(HALVES)):
            for k in range(3):
                arrival(k, e, s).wait_recv()
                for n in range(1, 3):
                    if not any(e[n:]):
                        send(k, e, s, n)
                share(k, e, s)
    for e in slot:
        for s in range(HALVES):
            for k in range(3):
                shared(k, e, s).wait_recv()
    for copy in sent:
        copy.wait_send()

    passed.wait_send()


def all_gather(plan, win):
    dma = pltpu.SemaphoreType.DMA
    n = 8 * 3 * HALVES
    return pl.pallas_call(
        functools.partial(ag_kernel, plan),
        out_shape=[pltpu.VMEM((plan.p * plan.unit, LANES), BF)] * 3,
        in_specs=[pl.BlockSpec(memory_space=pltpu.VMEM)],
        out_specs=[pl.BlockSpec(memory_space=pltpu.VMEM)] * 3,
        scratch_shapes=[pltpu.VMEM((3 * plan.unit + plan.edge, LANES), BF), pltpu.VMEM((small_rows(plan), LANES), F32)]
        + [pltpu.VMEM((plan.edge, LANES), BF)]
        + [dma((n,))] * 4
        + [dma((2,))],
        compiler_params=pltpu.CompilerParams(collective_id=1, has_side_effects=True, vmem_limit_bytes=6 << 20),
        name="all_gather",
    )(win)


def small_rows(plan):
    return -(-plan.small_size // (LANES * TILE)) * TILE


def restore_kernel(plan, *refs):
    w_refs, outs, out_sem = refs[:3], refs[3:-1], refs[-1]
    p, part = plan.p, plan.piece
    copies = []

    def copy(r, x, y, dst):
        for n in range(x // part, -(-y // part)):
            lo, hi = max(x, n * part), min(y, (n + 1) * part)
            src = w_refs[n % 3].at[pl.ds(r * plan.unit + n // 3 * part + lo - n * part, hi - lo)]
            copies.append(pltpu.make_async_copy(src, dst(lo - x, hi - lo), out_sem.at[len(copies)]))

    for r in range(p):
        lo = plan.starts[r]
        hi = plan.starts[r + 1] if r + 1 < p else plan.small_row
        for t, (a, b) in enumerate(plan.spans()[:-1]):
            x, y = max(a, lo), min(b, hi)
            if x < y:
                copy(r, x - lo, y - lo, lambda at, size, t=t, x=x, a=a: outs[t].at[pl.ds(x - a + at, size)])
    base = plan.small_row - plan.starts[p - 1]
    for out, (_, kept, nj) in zip(outs[len(plan.big):], plan.pairs()):
        copy(p - 1, base + kept, base + kept + out.shape[0], lambda at, size, out=out: out.at[pl.ds(at, size)])
    for c in copies:
        c.start()
    for c in copies:
        c.wait()


def restore(plan, gathered, shapes):
    n = len(plan.big)
    dma = pltpu.SemaphoreType.DMA
    outs = pl.pallas_call(
        functools.partial(restore_kernel, plan),
        out_shape=[jax.ShapeDtypeStruct((rows, LANES), BF) for rows, _, _ in plan.big]
        + [jax.ShapeDtypeStruct((2 * nj if m else -(-2 * nj // TILE) * TILE, LANES), BF)
           for m, (_, _, nj) in enumerate(plan.pairs())],
        in_specs=[ANY] * 3,
        out_specs=[ANY] * len(shapes),
        scratch_shapes=[dma((3 * HALVES * plan.p + 3 * n,))],
        compiler_params=pltpu.CompilerParams(vmem_limit_bytes=1 << 20),
        name="restore",
    )(*gathered)
    result = [from_stored(x, nj, s) for x, (_, nj, _), s in zip(outs, plan.big, shapes)]
    for x, (_, _, nj), s in zip(outs[n:], plan.pairs(), shapes[n:]):
        result.append(x[:2 * nj].reshape(nj, 2, LANES).transpose(1, 0, 2).reshape(s))
    return tuple(result)


def adam_update(g, m, v, w, lr, beta1, beta2, eps, step):
    t = step.astype(jnp.float32)
    m_new = beta1 * m + (1.0 - beta1) * g
    v_new = beta2 * v + (1.0 - beta2) * (g * g)
    m_hat = m_new * (1.0 / (1.0 - beta1 ** t))
    v_hat = v_new * (1.0 / (1.0 - beta2 ** t))
    w_new = w - lr * m_hat / (jnp.sqrt(v_hat) + eps)
    return m_new, v_new, w_new


def solution(mesh):
    p = mesh.shape["outer"] * mesh.shape["inner"]

    def body(g_emb, g_qkv, g_o, g_w1, g_w2, g_bqkv, g_b1, g_dvec, m, v, w, lr, beta1, beta2, eps, step):
        grads = (g_emb, g_qkv, g_o, g_w1, g_w2, g_bqkv, g_b1, g_dvec)
        shapes = tuple(x.shape[1:] for x in grads)
        plan = Plan(shapes, p)
        n = len(plan.big)
        stored = [as_stored(x, nj) for x, (_, nj, _) in zip(grads, plan.big)]
        stored.append(grads[n].reshape(shapes[n]))
        stored += [x.reshape(2, -1, LANES).transpose(1, 0, 2).reshape(-1, LANES) for x in grads[n + 1:]]
        total = reduce_scatter(plan, stored).reshape(-1)
        r = lax.axis_index(AXES)
        offset = r * plan.shard - plan.start(r) * LANES
        g = lax.dynamic_slice(total, (offset,), (plan.shard,)) / p
        m_new, v_new, w_new = adam_update(g, m, v, w, lr, beta1, beta2, eps, step)
        front = max(i * plan.shard - plan.starts[i] * LANES for i in range(p))
        back = plan.window * LANES - plan.shard
        win = lax.dynamic_slice(jnp.pad(w_new, (front, back)), (front - offset,), (plan.window * LANES,))
        wb = all_gather(plan, win.reshape(plan.window, LANES))
        return (m_new, v_new, w_new) + restore(plan, wb, shapes)

    g3 = P(AXES, None, None)
    g4 = P(AXES, None, None, None)
    flat = P(AXES)
    rep = P()
    in_specs = (g3, g4, g4, g4, g4, g3, g3, g4, flat, flat, flat, rep, rep, rep, rep, rep)
    out_specs = (flat, flat, flat, rep, rep, rep, rep, rep, rep, rep, rep)
    return jax.shard_map(body, mesh=mesh, in_specs=in_specs, out_specs=out_specs, check_vma=False)
```
